32 devices in a mesh: dp: 8 (over y, x, core), head: 4 (over z).
Axes of the slice: x: 2, y: 2, z: 4, core: 2. Of those that a mesh axis runs over, the one named last changes fastest.
Arguments:
- tokens: bfloat16 [32768, 768], P(('dp', 'head')), may hold values from -6 to 6
- span_mask: int32 [32768], P(('dp', 'head')), may hold values from 0 to 1, as said below
- valid_mask: int32 [32768], P(('dp', 'head')), may hold values from 0 to 1, as said below
- mask_embedding: bfloat16 [768], replicated, may hold values from -6 to 6
- qkv_weight: bfloat16 [768, 3, 768], P(None, None, 'head'), may hold values from -0.3125 to 0.3125
- query_bias: bfloat16 [768], P('head'), may hold values from -3 to 3
- value_bias: bfloat16 [768], P('head'), may hold values from -3 to 3
- out_weight: bfloat16 [768, 768], replicated, may hold values from -0.875 to 0.875
- out_bias: float32 [768], replicated, may hold values from -3 to 3
- norm1_gain: float32 [768], replicated, may hold values from 0.5 to 1.5
- norm1_bias: float32 [768], replicated, may hold values from -3 to 3
- up_weight: bfloat16 [768, 3072], replicated, may hold values from -0.21875 to 0.21875
- up_bias: float32 [3072], replicated, may hold values from -3 to 3
- down_weight: bfloat16 [3072, 768], replicated, may hold values from -0.109375 to 0.109375
- down_bias: float32 [768], replicated, may hold values from -3 to 3
- norm2_gain: float32 [768], replicated, may hold values from 0.5 to 1.5
- norm2_bias: float32 [768], replicated, may hold values from -3 to 3
- out_grad: bfloat16 [32768, 768], P(('dp', 'head')), may hold values from -6 to 6
Outputs:
- output: bfloat16 [32768, 768], P(('dp', 'head'))
- tokens_grad: float32 [32768, 768], P(('dp', 'head'))
- mask_embedding_grad: float32 [768], replicated
- qkv_weight_grad: float32 [768, 3, 768], P(None, None, 'head')
- query_bias_grad: float32 [768], P('head')
- value_bias_grad: float32 [768], P('head')
- out_weight_grad: float32 [768, 768], replicated
- out_bias_grad: float32 [768], replicated
- norm1_gain_grad: float32 [768], replicated
- norm1_bias_grad: float32 [768], replicated
- up_weight_grad: float32 [768, 3072], replicated
- up_bias_grad: float32 [3072], replicated
- down_weight_grad: float32 [3072, 768], replicated
- down_bias_grad: float32 [768], replicated
- norm2_gain_grad: float32 [768], replicated
- norm2_bias_grad: float32 [768], replicated
- stream_rms: float32 [3], replicated
The draws below stay inside these ranges and needn't reach their ends.
Inputs may be any that keep to these rules, and one draw needn't show every extreme that they name: `span_mask`: 1 marks a token inside a masked span; spans lie within one row of 512 tokens. `valid_mask`: 1 marks a token whose output gradient counts.
All inputs are finite; a program needn't handle non-finite values.
Results may differ from the reference program's by a relative error of at most 0.017.
Values may be sent and summed in bfloat16 or wider, within the bound.
A program may use at most 192 MiB of HBM per device.

```python
import math
from functools import partial
import jax
import jax.numpy as jnp
import numpy as np
from jax import lax

D = 768
HEADS = 12
HEAD_DIM = 64
FF = 3072
LEN = 512
TOKENS = 32768


def draw_span_mask(key, part):
    start_key, length_key = jax.random.split(jax.random.fold_in(key, 17))
    starting = jax.random.randint(start_key, (TOKENS,), 0, 1000) < 42
    levels = jax.random.randint(length_key, (TOKENS,), 0, 1 << 20)
    bounds = jnp.asarray(np.array([int((0.8 ** offset - 0.8 ** 10) / (1.0 - 0.8 ** 10) * (1 << 20)) for offset in range(1, 10)], dtype=np.int32))
    lengths = 1 + jnp.sum((levels[:, None] < bounds[None, :]).astype(jnp.int32), axis=1)
    position = jnp.arange(TOKENS, dtype=jnp.int32) % LEN
    covered = jnp.zeros((TOKENS,), dtype=jnp.bool_)
    for offset in range(10):
        moved_start = jnp.concatenate([jnp.zeros((offset,), jnp.bool_), starting[:TOKENS - offset]])
        moved_length = jnp.concatenate([jnp.zeros((offset,), jnp.int32), lengths[:TOKENS - offset]])
        covered = covered | moved_start & (moved_length > offset) & (position >= offset)
    return covered.astype(jnp.int32)


def draw_valid_mask(key, part):
    levels = jax.random.randint(jax.random.fold_in(key, 23), (TOKENS,), 0, 4 * TOKENS)
    return (levels < TOKENS + 2 * jnp.arange(TOKENS, dtype=jnp.int32)).astype(jnp.int32)


def block_scale(own_key, shape, pieces, low, top_value):
    level = 1.0
    for axis_at, shards_of in pieces:
        steps = jax.random.uniform(jax.random.fold_in(jax.random.fold_in(own_key, 6), axis_at), (shards_of,), jnp.float32, low / len(pieces), top_value / len(pieces))
        level = level * jnp.repeat(jnp.exp(steps), shape[axis_at] // shards_of).reshape((-1,) + (1,) * (len(shape) - 1 - axis_at))
    return level


def gaussian(key, shape, deviation, bound, cuts=(), kind=jnp.bfloat16):
    values = jax.random.normal(key, shape, jnp.float32) * deviation
    if len(cuts) > 0:
        values = block_scale(key, shape, cuts, -0.22, 0.18) * values
    return jnp.clip(values, min=-bound, max=bound).astype(kind)


def setup_inputs(seed: int = 0) -> dict:
    key_list = jax.random.split(jax.random.key(seed), 19)
    return {
        "tokens": gaussian(key_list[0], (TOKENS, D), 1.0, 6.0, ((0, 32),)),
        "span_mask": draw_span_mask(jax.random.fold_in(key_list[18], 71), 0),
        "valid_mask": draw_valid_mask(jax.random.fold_in(key_list[18], 71), 0),
        "mask_embedding": gaussian(key_list[3], (D,), 1.0, 6.0),
        "qkv_weight": gaussian(key_list[4], (D, 3, D), (D // 2) ** -0.5, 0.3125, ((2, 4),)),
        "query_bias": gaussian(key_list[5], (D,), 0.5, 3.0, ((0, 4),)),
        "value_bias": gaussian(key_list[6], (D,), 0.5, 3.0, ((0, 4),)),
        "out_weight": gaussian(key_list[7], (D, D), (D // 16) ** -0.5, 0.875),
        "out_bias": gaussian(key_list[8], (D,), 0.5, 3.0, (), jnp.float32),
        "norm1_gain": jnp.clip(1.0 + 0.1 * jax.random.normal(key_list[9], (D,), jnp.float32), 0.5, 1.5),
        "norm1_bias": gaussian(key_list[10], (D,), 0.5, 3.0, (), jnp.float32),
        "up_weight": gaussian(key_list[11], (D, FF), D ** -0.5, 0.21875),
        "up_bias": gaussian(key_list[12], (FF,), 0.5, 3.0, (), jnp.float32),
        "down_weight": gaussian(key_list[13], (FF, D), FF ** -0.5, 0.109375),
        "down_bias": gaussian(key_list[14], (D,), 0.5, 3.0, (), jnp.float32),
        "norm2_gain": jnp.clip(1.0 + 0.1 * jax.random.normal(key_list[15], (D,), jnp.float32), 0.5, 1.5),
        "norm2_bias": gaussian(key_list[16], (D,), 0.5, 3.0, (), jnp.float32),
        "out_grad": gaussian(key_list[17], (TOKENS, D), 1.0, 6.0, ((0, 32),)),
    }


@jax.custom_vjp
def low(v):
    return lax.optimization_barrier(v.astype(jnp.bfloat16)).astype(jnp.float32)

@jax.custom_vjp
def low_back(v):
    return v

def low_keep(v):
    return (low(v), None)

def low_pass(kept, grad):
    return (grad,)

def back_keep(v):
    return (v, None)

def back_low(kept, grad):
    return (low(grad),)
low.defvjp(low_keep, low_pass)
low_back.defvjp(back_keep, back_low)
HIGHEST = lax.Precision.HIGHEST
eps_norm = 1e-12

def matmul(left, right):
    return jnp.dot(left, right, precision=HIGHEST, preferred_element_type=jnp.float32)

def layer_norm(hidden, gain, bias):
    center = hidden - lax.optimization_barrier(jnp.mean(hidden, axis=-1, keepdims=True))
    variance = lax.optimization_barrier(jnp.mean(center * center, axis=-1, keepdims=True))
    return center * lax.rsqrt(variance + eps_norm) * gain + bias

def attend_block(blocks):
    queries, keys_part, values = blocks
    scaling = 1.0 / math.sqrt(HEAD_DIM)
    scores = jnp.einsum('qhd,khd->hqk', queries, keys_part, precision=HIGHEST) * scaling
    scores = low_back(scores)
    probabilities = low(jax.nn.softmax(scores, axis=-1))
    return jnp.einsum('hqk,khd->qhd', probabilities, values, precision=HIGHEST)

def forward(span_mask, tokens, embedding, qkv_weight, query_bias, value_bias, out_weight, out_bias, gain_first, bias_first, up_weight, up_bias, down_weight, down_bias, gain_second, bias_second):
    inputs = jnp.where(span_mask[:, None] == 1, embedding[None, :], tokens)
    projected = matmul(inputs, qkv_weight.reshape(D, 3 * D))
    queries = low(low_back(projected[:, :D] + query_bias))
    keys_part = low(low_back(projected[:, D:2 * D]))
    values = low(low_back(projected[:, 2 * D:] + value_bias))
    blocked = (TOKENS // LEN, LEN, HEADS, HEAD_DIM)
    context = lax.map(jax.checkpoint(attend_block), (queries.reshape(blocked), keys_part.reshape(blocked), values.reshape(blocked)))
    context = low(low_back(context.reshape(TOKENS, D)))
    attended = low_back(matmul(context, out_weight) + out_bias)
    normed = layer_norm(inputs + attended, gain_first, bias_first)
    preact = low_back(matmul(low(normed), up_weight) + up_bias)
    activated = low(jax.nn.gelu(preact, approximate=False))
    feedout = low_back(matmul(activated, down_weight) + down_bias)
    result = layer_norm(normed + feedout, gain_second, bias_second)
    return (result, (inputs, attended, feedout))

def reference(tokens, span_mask, valid_mask, mask_embedding, qkv_weight, query_bias, value_bias, out_weight, out_bias, norm1_gain, norm1_bias, up_weight, up_bias, down_weight, down_bias, norm2_gain, norm2_bias, out_grad):
    primals = [argument.astype(jnp.float32) for argument in (tokens, mask_embedding, qkv_weight, query_bias, value_bias, out_weight, out_bias, norm1_gain, norm1_bias, up_weight, up_bias, down_weight, down_bias, norm2_gain, norm2_bias)]
    result, pullback, streams = jax.vjp(partial(forward, span_mask), *primals, has_aux=True)
    validity = valid_mask.astype(jnp.float32)
    grads = pullback(out_grad.astype(jnp.float32) * validity[:, None])
    count = jnp.maximum(jnp.sum(validity), 1.0)
    sums = [jnp.sum(validity[:, None] * stream * stream) for stream in streams]
    stream_rms = jnp.sqrt(jnp.stack(sums) / (count * D))
    return (result.astype(jnp.bfloat16), grads[0], grads[1], grads[2], grads[3], grads[4], grads[5], grads[6], grads[7], grads[8], grads[9], grads[10], grads[11], grads[12], grads[13], grads[14], stream_rms)
```

```python
import functools
import math

import jax
import jax.numpy as jnp
from jax import lax
from jax.experimental import pallas as pl
from jax.experimental.pallas import tpu as pltpu
from jax.sharding import PartitionSpec as P

HEAD_DIM = 64
LEN = 512
EPS = 1e-12
BF = jnp.bfloat16
F32 = jnp.float32


def dot_nn(left, right):
    return lax.dot_general(left, right, (((1,), (0,)), ((), ())), preferred_element_type=F32)


def dot_nt(left, right):
    return lax.dot_general(left, right, (((1,), (1,)), ((), ())), preferred_element_type=F32)


def dot_tn(left, right):
    return lax.dot_general(left, right, (((0,), (0,)), ((), ())), preferred_element_type=F32)


def head_lanes(width, head):
    lanes = lax.broadcasted_iota(jnp.int32, (1, width), 1)
    return (lanes >= head * HEAD_DIM) & (lanes < (head + 1) * HEAD_DIM)


def forward_kernel(
    x_ref, w_ref, qb_ref, vb_ref, ow_ref, acc_ref, q_ref, k_ref, v_ref, ctx_ref, lse_ref, out_ref
):
    x = x_ref[...]
    width = w_ref.shape[2]
    heads = width // HEAD_DIM
    q = (dot_nn(x, w_ref[0]) + qb_ref[...]).astype(BF)
    k = dot_nn(x, w_ref[1]).astype(BF)
    v32 = dot_nn(x, w_ref[2]) + vb_ref[...]
    v = v32.astype(BF)
    q_ref[...] = q
    k_ref[...] = k
    v_ref[...] = v
    v_t = v.T
    q_scaled = q * jnp.asarray(0.125, BF)
    pieces = []
    for head in range(heads):
        k_head = jnp.where(head_lanes(width, head), k, jnp.zeros_like(k))
        scores = dot_nt(k_head, q_scaled)
        highest = jnp.max(scores, axis=0, keepdims=True)
        exponent = jnp.exp(scores - highest)
        totals = jnp.sum(exponent, axis=0, keepdims=True)
        probs = (exponent * (1.0 / totals)).astype(BF)
        pieces.append(dot_nn(v_t[head * HEAD_DIM : (head + 1) * HEAD_DIM], probs))
        lse_ref[0, head : head + 1, :] = highest + jnp.log(totals)
    ctx = jnp.concatenate(pieces, axis=0).T.astype(BF)
    ctx_ref[...] = ctx
    out_ref[...] = acc_ref[...] + dot_nn(ctx, ow_ref[...])


def backward_kernel(
    x_ref,
    w_ref,
    ow_ref,
    q_ref,
    k_ref,
    v_ref,
    ctx_ref,
    lse_ref,
    ga_ref,
    acc_ref,
    wg_ref,
    owg_ref,
    qbg_ref,
    vbg_ref,
    out_ref,
    wg_acc,
    owg_acc,
):
    row = pl.program_id(0)
    last = pl.num_programs(0) - 1
    width = w_ref.shape[2]
    heads = width // HEAD_DIM
    x = x_ref[...]
    ga = ga_ref[...]
    dctx = dot_nt(ga, ow_ref[...]).astype(BF)
    q = q_ref[...]
    k = k_ref[...]
    v = v_ref[...]
    k_t = k.T
    q_scaled = q * jnp.asarray(0.125, BF)
    dq_t = []
    dk = jnp.zeros(q.shape, F32)
    dv = jnp.zeros(q.shape, F32)
    for head in range(heads):
        mask = head_lanes(width, head)
        scores = dot_nt(jnp.where(mask, k, jnp.zeros_like(k)), q_scaled)
        probs = jnp.exp(scores - lse_ref[0, head : head + 1, :])
        dprobs = dot_nt(jnp.where(mask, v, jnp.zeros_like(v)), dctx)
        delta = jnp.sum(probs * dprobs, axis=0, keepdims=True)
        dscores = (probs * (dprobs - delta)).astype(BF)
        dv = jnp.where(mask, dot_nn(probs.astype(BF), dctx), dv)
        dk = jnp.where(mask, dot_nn(dscores, q_scaled), dk)
        dq_t.append(dot_nn(k_t[head * HEAD_DIM : (head + 1) * HEAD_DIM], dscores))
    dq32 = (jnp.concatenate(dq_t, axis=0) * 0.125).T
    dq = dq32.astype(BF)
    dk = dk.astype(BF)
    dv = dv.astype(BF)
    out_ref[...] = (
        acc_ref[...] + dot_nt(dq, w_ref[0]) + dot_nt(dk, w_ref[1]) + dot_nt(dv, w_ref[2])
    )

    @pl.when(row == 0)
    def _():
        wg_acc[...] = jnp.zeros_like(wg_acc)
        owg_acc[...] = jnp.zeros_like(owg_acc)
        qbg_ref[...] = jnp.zeros_like(qbg_ref)
        vbg_ref[...] = jnp.zeros_like(vbg_ref)

    wg_acc[0] += dot_tn(x, dq)
    wg_acc[1] += dot_tn(x, dk)
    wg_acc[2] += dot_tn(x, dv)
    owg_acc[...] += dot_tn(ctx_ref[...], ga)
    qbg_ref[...] += jnp.sum(dq.astype(F32), axis=0, keepdims=True)
    vbg_ref[...] += jnp.sum(dv.astype(F32), axis=0, keepdims=True)

    @pl.when(row == last)
    def _():
        wg_ref[...] = wg_acc[...].astype(BF)
        owg_ref[...] = owg_acc[...].astype(BF)


def by_row(block):
    rank = len(block)
    return pl.BlockSpec(block, lambda r: (r,) + (0,) * (rank - 1))


def fixed(block):
    rank = len(block)
    return pl.BlockSpec(block, lambda r: (0,) * rank)


def attention_forward(x, w, qb, vb, ow, acc):
    tokens, features = x.shape
    width = w.shape[2]
    rows = tokens // LEN
    flops = 2 * tokens * features * width * 4 + 4 * tokens * LEN * width
    return pl.pallas_call(
        forward_kernel,
        grid=(rows,),
        in_specs=[
            by_row((LEN, features)),
            fixed(w.shape),
            fixed((1, width)),
            fixed((1, width)),
            fixed((width, features)),
            by_row((LEN, features)),
        ],
        out_specs=[
            by_row((LEN, width)),
            by_row((LEN, width)),
            by_row((LEN, width)),
            by_row((LEN, width)),
            by_row((1, 8, LEN)),
            by_row((LEN, features)),
        ],
        out_shape=[jax.ShapeDtypeStruct((tokens, width), BF)] * 4
        + [
            jax.ShapeDtypeStruct((rows, 8, LEN), F32),
            jax.ShapeDtypeStruct((tokens, features), F32),
        ],
        compiler_params=pltpu.CompilerParams(
            dimension_semantics=("arbitrary",), vmem_limit_bytes=48 << 20
        ),
        cost_estimate=pl.CostEstimate(
            flops=4 * flops, bytes_accessed=12 << 20, transcendentals=tokens * LEN * 3
        ),
        name="attention_forward",
    )(x, w, qb, vb, ow, acc)


def attention_backward(x, w, ow, q, k, v, ctx, lse, ga, acc):
    tokens, features = x.shape
    width = w.shape[2]
    rows = tokens // LEN
    flops = 2 * tokens * features * width * 8 + 10 * tokens * LEN * width
    return pl.pallas_call(
        backward_kernel,
        grid=(rows,),
        in_specs=[
            by_row((LEN, features)),
            fixed(w.shape),
            fixed((width, features)),
            by_row((LEN, width)),
            by_row((LEN, width)),
            by_row((LEN, width)),
            by_row((LEN, width)),
            by_row((1, 8, LEN)),
            by_row((LEN, features)),
            by_row((LEN, features)),
        ],
        out_specs=[
            fixed(w.shape),
            fixed((width, features)),
            fixed((1, width)),
            fixed((1, width)),
            by_row((LEN, features)),
        ],
        out_shape=[
            jax.ShapeDtypeStruct(w.shape, BF),
            jax.ShapeDtypeStruct((width, features), BF),
            jax.ShapeDtypeStruct((1, width), F32),
            jax.ShapeDtypeStruct((1, width), F32),
            jax.ShapeDtypeStruct((tokens, features), F32),
        ],
        scratch_shapes=[pltpu.VMEM(w.shape, F32), pltpu.VMEM((width, features), F32)],
        compiler_params=pltpu.CompilerParams(
            dimension_semantics=("arbitrary",), vmem_limit_bytes=48 << 20
        ),
        cost_estimate=pl.CostEstimate(
            flops=4 * flops, bytes_accessed=16 << 20, transcendentals=tokens * LEN * 3
        ),
        name="attention_backward",
    )(x, w, ow, q, k, v, ctx, lse, ga, acc)


def swap(value, axis, mask, size):
    return lax.ppermute(value, axis, [(i, i ^ mask) for i in range(size)])


def bit_of(axis, bit):
    return (lax.axis_index(axis) >> bit) & 1


def joined(mine, other, upper, dim, kind=None):
    low = jnp.where(upper == 1, other, mine)
    high = jnp.where(upper == 1, mine, other)
    if kind is not None:
        low, high = low.astype(kind), high.astype(kind)
    return jnp.concatenate([low, high], axis=dim)


def halve(value, bit, size, dim):
    half = value.shape[dim] // 2
    mine = bit_of("dp", bit)
    sent = lax.dynamic_slice_in_dim(value, (1 - mine) * half, half, dim)
    kept = lax.dynamic_slice_in_dim(value, mine * half, half, dim)
    received = swap(sent, "dp", 1 << bit, size)
    return (kept.astype(F32) + received.astype(F32)).astype(BF)


def double(value, bit, size, dim, kind=None):
    return joined(value, swap(value, "dp", 1 << bit, size), bit_of("dp", bit), dim, kind)


def plane_orders(size):
    bits = size.bit_length() - 1
    rest = list(range(1, bits))
    return rest, rest[::-1]


def reduce_plane(value, size, dim):
    value = halve(value, 0, size, dim)
    half = value.shape[dim] // 2
    parts = []
    for index, order in enumerate(plane_orders(size)):
        part = lax.slice_in_dim(value, index * half, (index + 1) * half, axis=dim)
        for bit in order:
            part = halve(part, bit, size, dim)
        parts.append(part)
    return parts


def gather_plane(parts, size, dim, kind=None):
    done = []
    for part, order in zip(parts, plane_orders(size)):
        for bit in order[::-1]:
            part = double(part, bit, size, dim)
        done.append(part)
    return double(jnp.concatenate(done, axis=dim), 0, size, dim, kind)


def reduce_head(pieces, size):
    total = pieces[0].astype(F32)
    for offset in range(1, size):
        total = total + swap(pieces[offset], "head", offset, size).astype(F32)
    return total


def gather_head(piece, size):
    return [piece] + [swap(piece, "head", offset, size) for offset in range(1, size)]


def absolute(pieces, dim):
    count = len(pieces)
    bit = 0
    while (1 << bit) < count:
        upper = bit_of("head", bit)
        step = 1 << bit
        pieces = [
            jnp.where(upper == 1, pieces[index ^ step], pieces[index]) for index in range(count)
        ]
        bit += 1
    return jnp.concatenate(pieces, axis=dim)


def own_pieces(value, size, dim):
    width = value.shape[dim] // size
    me = lax.axis_index("head")
    return [
        lax.dynamic_slice_in_dim(value, (me ^ offset) * width, width, dim)
        for offset in range(size)
    ]


def all_reduce_matrix(value, dp, head, head_dim):
    parts = []
    for part in reduce_plane(value, dp, 0):
        piece = reduce_head(own_pieces(part, head, head_dim), head).astype(BF)
        parts.append(absolute(gather_head(piece, head), head_dim))
    return gather_plane(parts, dp, 0, F32)


def all_reduce_small(vector, dp, head):
    bit = 1
    while bit < dp:
        vector = vector + swap(vector, "dp", bit, dp)
        bit *= 2
    bit = 1
    while bit < head:
        vector = vector + swap(vector, "head", bit, head)
        bit *= 2
    return vector


def norm_forward(hidden, gain, bias):
    center = hidden - jnp.mean(hidden, axis=-1, keepdims=True)
    inverse = lax.rsqrt(jnp.mean(center * center, axis=-1, keepdims=True) + EPS)
    normal = center * inverse
    return (normal * gain + bias, normal, inverse)


def norm_backward(upstream, normal, inverse, gain):
    gain_grad = jnp.sum(upstream * normal, axis=0)
    bias_grad = jnp.sum(upstream, axis=0)
    scaled = upstream * gain
    hidden_grad = inverse * (
        scaled
        - jnp.mean(scaled, axis=-1, keepdims=True)
        - normal * jnp.mean(scaled * normal, axis=-1, keepdims=True)
    )
    return (hidden_grad, gain_grad, bias_grad)


def phi(values):
    return 0.5 * (1.0 + jax.scipy.special.erf(values * (1.0 / math.sqrt(2.0))))


def body(
    dp,
    head,
    tokens,
    span_mask,
    valid_mask,
    mask_embedding,
    qkv_weight,
    query_bias,
    value_bias,
    out_weight,
    out_bias,
    norm1_gain,
    norm1_bias,
    up_weight,
    up_bias,
    down_weight,
    down_bias,
    norm2_gain,
    norm2_bias,
    out_grad,
):
    features = tokens.shape[1]
    width = qkv_weight.shape[2]
    masked = (span_mask == 1)[:, None]
    inputs = jnp.where(masked, mask_embedding[None, :], tokens)
    inputs_wide = inputs.astype(F32)
    validity = valid_mask.astype(F32)[:, None]

    own = jnp.transpose(qkv_weight, (1, 0, 2))
    core = bit_of("dp", 0)
    half = lax.dynamic_slice_in_dim(own, core * (features // 2), features // 2, 1)
    halves = [half]
    for bit in range(head.bit_length() - 1):
        halves = halves + [swap(part, "head", 1 << bit, head) for part in halves]
    weights = [own] + [double(part, 0, dp, 1) for part in halves[1:]]
    biases = jnp.stack([query_bias, value_bias]).astype(F32)
    bias_parts = [biases]
    for bit in range(head.bit_length() - 1):
        bias_parts = bias_parts + [swap(part, "head", 1 << bit, head) for part in bias_parts]
    out_parts = own_pieces(out_weight, head, 0)

    attended = jnp.broadcast_to(out_bias[None, :], tokens.shape)
    saved = []
    for group in range(head):
        q, k, v, ctx, lse, attended = attention_forward(
            inputs,
            weights[group],
            bias_parts[group][0:1],
            bias_parts[group][1:2],
            out_parts[group],
            attended,
        )
        saved.append((q, k, v, ctx, lse))

    normed, normal_first, inverse_first = norm_forward(
        inputs_wide + attended, norm1_gain, norm1_bias
    )
    normed_low = normed.astype(BF)
    preact = dot_nn(normed_low, up_weight) + up_bias
    activated = (preact * phi(preact)).astype(BF)
    feedout = dot_nn(activated, down_weight) + down_bias
    result, normal_second, inverse_second = norm_forward(normed + feedout, norm2_gain, norm2_bias)
    grad_output = out_grad.astype(F32) * validity
    grad_second, gain_second_grad, bias_second_grad = norm_backward(
        grad_output, normal_second, inverse_second, norm2_gain
    )
    grad_feed = grad_second.astype(BF)
    down_bias_grad = jnp.sum(grad_feed, axis=0, dtype=F32)
    down_local = dot_tn(activated, grad_feed).astype(BF)
    down_weight_grad = all_reduce_matrix(down_local, dp, head, 0)
    slope = phi(preact) + preact * jnp.exp(-0.5 * preact * preact) * (
        1.0 / math.sqrt(2.0 * math.pi)
    )
    grad_preact = (dot_nt(grad_feed, down_weight) * slope).astype(BF)
    up_bias_grad = jnp.sum(grad_preact, axis=0, dtype=F32)
    up_local = dot_tn(normed_low, grad_preact).astype(BF)
    up_weight_grad = all_reduce_matrix(up_local, dp, head, 1)
    grad_normed = dot_nt(grad_preact, up_weight) + grad_second
    grad_first, gain_first_grad, bias_first_grad = norm_backward(
        grad_normed, normal_first, inverse_first, norm1_gain
    )
    grad_attended = grad_first.astype(BF)
    out_bias_grad = jnp.sum(grad_attended, axis=0, dtype=F32)
    squares = jnp.stack(
        [
            jnp.sum(validity * inputs_wide * inputs_wide),
            jnp.sum(validity * attended * attended),
            jnp.sum(validity * feedout * feedout),
            jnp.sum(validity),
        ]
    )
    early = [
        down_bias_grad,
        gain_second_grad,
        bias_second_grad,
        gain_first_grad,
        bias_first_grad,
        out_bias_grad,
        up_bias_grad,
        squares,
    ]
    early_sum = all_reduce_small(jnp.concatenate(early), dp, head)

    grad_inputs = grad_first
    weight_pieces = []
    out_pieces = []
    query_parts = []
    value_parts = []
    for group in range(head):
        q, k, v, ctx, lse = saved[group]
        weight_piece, out_piece, query_part, value_part, grad_inputs = attention_backward(
            inputs,
            weights[group],
            out_parts[group],
            q,
            k,
            v,
            ctx,
            lse,
            grad_attended,
            grad_inputs,
        )
        weight_pieces.append(reduce_plane(weight_piece, dp, 1))
        out_pieces.append(out_piece)
        query_parts.append(query_part[0])
        value_parts.append(value_part[0])

    weight_grad = gather_plane(
        [
            reduce_head([weight_pieces[group][part] for group in range(head)], head).astype(BF)
            for part in range(2)
        ],
        dp,
        1,
        F32,
    )
    weight_grad = jnp.transpose(weight_grad, (1, 0, 2))

    out_reduced = jnp.stack(out_pieces)
    for bit in range(dp.bit_length() - 1):
        out_reduced = halve(out_reduced, bit, dp, 1)
    out_piece = reduce_head([out_reduced[group] for group in range(head)], head).astype(BF)
    for bit in range(dp.bit_length() - 2, -1, -1):
        out_piece = double(out_piece, bit, dp, 0)
    out_weight_grad = absolute(gather_head(out_piece, head), 0).astype(F32)

    tokens_grad = jnp.where(masked, 0.0, grad_inputs)
    embedding_grad = jnp.sum(jnp.where(masked, grad_inputs, 0.0), axis=0)
    late = jnp.concatenate([embedding_grad, absolute(query_parts, 0), absolute(value_parts, 0)])
    late_sum = all_reduce_small(late, dp, head)
    embedding_grad = late_sum[:features]
    me = lax.axis_index("head")
    first_grad = lax.dynamic_slice_in_dim(late_sum, features + me * width, width)
    third_grad = lax.dynamic_slice_in_dim(late_sum, 2 * features + me * width, width)

    pieces = []
    offset = 0
    for part in early:
        pieces.append(lax.slice_in_dim(early_sum, offset, offset + part.shape[0]))
        offset += part.shape[0]
    (
        down_bias_grad,
        gain_second_grad,
        bias_second_grad,
        gain_first_grad,
        bias_first_grad,
        out_bias_grad,
        up_bias_grad,
        squares,
    ) = pieces
    count = jnp.maximum(squares[3], 1.0)
    stream_rms = jnp.sqrt(squares[:3] / (count * features))
    return (
        result.astype(BF),
        tokens_grad,
        embedding_grad,
        weight_grad,
        first_grad,
        third_grad,
        out_weight_grad,
        out_bias_grad,
        gain_first_grad,
        bias_first_grad,
        up_weight_grad,
        up_bias_grad,
        down_weight_grad,
        down_bias_grad,
        gain_second_grad,
        bias_second_grad,
        stream_rms,
    )


def solution(mesh):
    split = P(("dp", "head"), None)
    flat = P(("dp", "head"))
    placed = (split, flat, flat, P(), P(None, None, "head"), P("head"), P("head")) + (P(),) * 10
    placed = placed + (split,)
    outs = (split, split, P(), P(None, None, "head"), P("head"), P("head")) + (P(),) * 11
    return jax.shard_map(
        functools.partial(body, mesh.shape["dp"], mesh.shape["head"]),
        mesh=mesh,
        in_specs=placed,
        out_specs=outs,
        check_vma=False,
    )
```

```python
import functools
import math

import jax
import jax.numpy as jnp
from jax import lax
from jax.experimental import pallas as pl
from jax.experimental.pallas import tpu as pltpu
from jax.sharding import PartitionSpec as P

HEAD_DIM = 64
LEN = 512
EPS = 1e-12
BF = jnp.bfloat16
F32 = jnp.float32


def dot_nn(left, right):
    return lax.dot_general(left, right, (((1,), (0,)), ((), ())), preferred_element_type=F32)


def dot_nt(left, right):
    return lax.dot_general(left, right, (((1,), (1,)), ((), ())), preferred_element_type=F32)


def dot_tn(left, right):
    return lax.dot_general(left, right, (((0,), (0,)), ((), ())), preferred_element_type=F32)


def head_lanes(width, head):
    lanes = lax.broadcasted_iota(jnp.int32, (1, width), 1)
    return (lanes >= head * HEAD_DIM) & (lanes < (head + 1) * HEAD_DIM)


def forward_kernel(
    x_ref, w_ref, qb_ref, vb_ref, ow_ref, acc_ref, q_ref, k_ref, v_ref, ctx_ref, lse_ref, out_ref
):
    x = x_ref[...]
    width = w_ref.shape[2]
    heads = width // HEAD_DIM
    q = (dot_nn(x, w_ref[0]) + qb_ref[...]).astype(BF)
    k = dot_nn(x, w_ref[1]).astype(BF)
    v32 = dot_nn(x, w_ref[2]) + vb_ref[...]
    v = v32.astype(BF)
    q_ref[...] = q
    k_ref[...] = k
    v_ref[...] = v
    v_t = v.T
    q_scaled = q * jnp.asarray(0.125, BF)
    pieces = []
    for head in range(heads):
        k_head = jnp.where(head_lanes(width, head), k, jnp.zeros_like(k))
        scores = dot_nt(k_head, q_scaled)
        highest = jnp.max(scores, axis=0, keepdims=True)
        exponent = jnp.exp(scores - highest)
        totals = jnp.sum(exponent, axis=0, keepdims=True)
        probs = (exponent * (1.0 / totals)).astype(BF)
        pieces.append(dot_nn(v_t[head * HEAD_DIM : (head + 1) * HEAD_DIM], probs))
        lse_ref[0, head : head + 1, :] = highest + jnp.log(totals)
    ctx = jnp.concatenate(pieces, axis=0).T.astype(BF)
    ctx_ref[...] = ctx
    out_ref[...] = acc_ref[...] + dot_nn(ctx, ow_ref[...])


def backward_kernel(
    x_ref,
    w_ref,
    ow_ref,
    q_ref,
    k_ref,
    v_ref,
    ctx_ref,
    lse_ref,
    ga_ref,
    acc_ref,
    wg_ref,
    owg_ref,
    qbg_ref,
    vbg_ref,
    out_ref,
    wg_acc,
    owg_acc,
):
    row = pl.program_id(0)
    last = pl.num_programs(0) - 1
    width = w_ref.shape[2]
    heads = width // HEAD_DIM
    x = x_ref[...]
    ga = ga_ref[...]
    dctx = dot_nt(ga, ow_ref[...]).astype(BF)
    q = q_ref[...]
    k = k_ref[...]
    v = v_ref[...]
    k_t = k.T
    q_scaled = q * jnp.asarray(0.125, BF)
    dq_t = []
    dk = jnp.zeros(q.shape, F32)
    dv = jnp.zeros(q.shape, F32)
    for head in range(heads):
        mask = head_lanes(width, head)
        scores = dot_nt(jnp.where(mask, k, jnp.zeros_like(k)), q_scaled)
        probs = jnp.exp(scores - lse_ref[0, head : head + 1, :])
        dprobs = dot_nt(jnp.where(mask, v, jnp.zeros_like(v)), dctx)
        delta = jnp.sum(probs * dprobs, axis=0, keepdims=True)
        dscores = (probs * (dprobs - delta)).astype(BF)
        dv = jnp.where(mask, dot_nn(probs.astype(BF), dctx), dv)
        dk = jnp.where(mask, dot_nn(dscores, q_scaled), dk)
        dq_t.append(dot_nn(k_t[head * HEAD_DIM : (head + 1) * HEAD_DIM], dscores))
    dq32 = (jnp.concatenate(dq_t, axis=0) * 0.125).T
    dq = dq32.astype(BF)
    dk = dk.astype(BF)
    dv = dv.astype(BF)
    out_ref[...] = (
        acc_ref[...] + dot_nt(dq, w_ref[0]) + dot_nt(dk, w_ref[1]) + dot_nt(dv, w_ref[2])
    )

    @pl.when(row == 0)
    def _():
        wg_acc[...] = jnp.zeros_like(wg_acc)
        owg_acc[...] = jnp.zeros_like(owg_acc)
        qbg_ref[...] = jnp.zeros_like(qbg_ref)
        vbg_ref[...] = jnp.zeros_like(vbg_ref)

    wg_acc[0] += dot_tn(x, dq)
    wg_acc[1] += dot_tn(x, dk)
    wg_acc[2] += dot_tn(x, dv)
    owg_acc[...] += dot_tn(ctx_ref[...], ga)
    qbg_ref[...] += jnp.sum(dq.astype(F32), axis=0, keepdims=True)
    vbg_ref[...] += jnp.sum(dv.astype(F32), axis=0, keepdims=True)

    @pl.when(row == last)
    def _():
        wg_ref[...] = wg_acc[...].astype(BF)
        owg_ref[...] = owg_acc[...].astype(BF)


def by_row(block):
    rank = len(block)
    return pl.BlockSpec(block, lambda r: (r,) + (0,) * (rank - 1))


def fixed(block):
    rank = len(block)
    return pl.BlockSpec(block, lambda r: (0,) * rank)


def attention_forward(x, w, qb, vb, ow, acc):
    tokens, features = x.shape
    width = w.shape[2]
    rows = tokens // LEN
    flops = 2 * tokens * features * width * 4 + 4 * tokens * LEN * width
    return pl.pallas_call(
        forward_kernel,
        grid=(rows,),
        in_specs=[
            by_row((LEN, features)),
            fixed(w.shape),
            fixed((1, width)),
            fixed((1, width)),
            fixed((width, features)),
            by_row((LEN, features)),
        ],
        out_specs=[
            by_row((LEN, width)),
            by_row((LEN, width)),
            by_row((LEN, width)),
            by_row((LEN, width)),
            by_row((1, 8, LEN)),
            by_row((LEN, features)),
        ],
        out_shape=[jax.ShapeDtypeStruct((tokens, width), BF)] * 4
        + [
            jax.ShapeDtypeStruct((rows, 8, LEN), F32),
            jax.ShapeDtypeStruct((tokens, features), F32),
        ],
        compiler_params=pltpu.CompilerParams(
            dimension_semantics=("arbitrary",), vmem_limit_bytes=48 << 20
        ),
        cost_estimate=pl.CostEstimate(
            flops=4 * flops, bytes_accessed=12 << 20, transcendentals=tokens * LEN * 3
        ),
        name="attention_forward",
    )(x, w, qb, vb, ow, acc)


def attention_backward(x, w, ow, q, k, v, ctx, lse, ga, acc):
    tokens, features = x.shape
    width = w.shape[2]
    rows = tokens // LEN
    flops = 2 * tokens * features * width * 8 + 10 * tokens * LEN * width
    return pl.pallas_call(
        backward_kernel,
        grid=(rows,),
        in_specs=[
            by_row((LEN, features)),
            fixed(w.shape),
            fixed((width, features)),
            by_row((LEN, width)),
            by_row((LEN, width)),
            by_row((LEN, width)),
            by_row((LEN, width)),
            by_row((1, 8, LEN)),
            by_row((LEN, features)),
            by_row((LEN, features)),
        ],
        out_specs=[
            fixed(w.shape),
            fixed((width, features)),
            fixed((1, width)),
            fixed((1, width)),
            by_row((LEN, features)),
        ],
        out_shape=[
            jax.ShapeDtypeStruct(w.shape, BF),
            jax.ShapeDtypeStruct((width, features), BF),
            jax.ShapeDtypeStruct((1, width), F32),
            jax.ShapeDtypeStruct((1, width), F32),
            jax.ShapeDtypeStruct((tokens, features), F32),
        ],
        scratch_shapes=[pltpu.VMEM(w.shape, F32), pltpu.VMEM((width, features), F32)],
        compiler_params=pltpu.CompilerParams(
            dimension_semantics=("arbitrary",), vmem_limit_bytes=48 << 20
        ),
        cost_estimate=pl.CostEstimate(
            flops=4 * flops, bytes_accessed=16 << 20, transcendentals=tokens * LEN * 3
        ),
        name="attention_backward",
    )(x, w, ow, q, k, v, ctx, lse, ga, acc)


MESH = pl.DeviceIdType.MESH


class Place:
    def __init__(self):
        self.dp = lax.axis_index("dp")
        self.h = lax.axis_index("head")
        self.c = self.dp & 1
        self.x = (self.dp >> 1) & 1
        self.y = (self.dp >> 2) & 1

    def core(self):
        return (self.dp ^ 1, self.h)

    def side(self, axis):
        return (self.dp ^ (2 if axis == "x" else 4), self.h)

    def up(self, offset):
        return (self.dp, self.h ^ offset)


def remote(src, dst, send, recv, where):
    return pltpu.make_async_remote_copy(
        src_ref=src,
        dst_ref=dst,
        send_sem=send,
        recv_sem=recv,
        device_id=where,
        device_id_type=MESH,
    )


def greet(friends):
    barrier = pltpu.get_barrier_semaphore()
    for friend in friends:
        pl.semaphore_signal(barrier, inc=1, device_id=friend, device_id_type=MESH)
    pl.semaphore_wait(barrier, len(friends))


def early_kernel(
    x_ref,
    own_ref,
    bias_ref,
    ow_ref,
    ob_ref,
    q_ref,
    k_ref,
    v_ref,
    ctx_ref,
    lse_ref,
    out_ref,
    w_out,
    w_all,
    b_all,
    send,
    recv,
    local,
):
    step = pl.program_id(0)
    group, row = step // 2, step % 2
    place = Place()
    features = w_all.shape[2]
    width = w_all.shape[3]
    heads = width // HEAD_DIM
    half = features // 2
    rows = pl.ds(pl.multiple_of(place.c * half, half), half)

    load = pltpu.make_async_copy(own_ref, w_all.at[0], local.at[0])

    def part(g):
        return w_all.at[g, :, rows, :]

    def direct(g):
        return remote(own_ref.at[:, rows, :], part(g), send.at[0, g], recv.at[0, g], place.up(g))

    relay = remote(part(2), part(3), send.at[0, 3], recv.at[0, 3], place.up(1))

    def cross(g):
        return remote(part(g), part(g), send.at[1, g], recv.at[1, g], place.core())

    def bias(g):
        return remote(bias_ref, b_all.at[g], send.at[2, g], recv.at[2, g], place.up(g))

    def store(g):
        return pltpu.make_async_copy(w_all.at[g], w_out.at[g], local.at[2 + g])

    @pl.when(step == 0)
    def _():
        greet([place.core()] + [place.up(o) for o in range(1, 4)])
        load.start()
        bias_load = pltpu.make_async_copy(bias_ref, b_all.at[0], local.at[1])
        bias_load.start()
        for g in range(1, 4):
            bias(g).start()
        direct(1).start()
        direct(2).start()
        load.wait()
        bias_load.wait()
        store(0).start()

    for g in range(1, 4):

        @pl.when(step == 2 * g)
        def _():
            cross(g).wait()
            bias(g).wait()
            store(g).start()

    x = x_ref[...]
    q = (dot_nn(x, w_all[group, 0]) + b_all[group, 0:1, :]).astype(BF)
    k = dot_nn(x, w_all[group, 1]).astype(BF)
    v = (dot_nn(x, w_all[group, 2]) + b_all[group, 1:2, :]).astype(BF)
    q_ref[0] = q
    k_ref[0] = k
    v_ref[0] = v
    v_t = v.T
    q_scaled = q * jnp.asarray(0.125, BF)
    pieces = []
    for head in range(heads):
        k_head = jnp.where(head_lanes(width, head), k, jnp.zeros_like(k))
        scores = dot_nt(k_head, q_scaled)
        highest = jnp.max(scores, axis=0, keepdims=True)
        exponent = jnp.exp(scores - highest)
        totals = jnp.sum(exponent, axis=0, keepdims=True)
        probs = (exponent * (1.0 / totals)).astype(BF)
        pieces.append(dot_nn(v_t[head * HEAD_DIM : (head + 1) * HEAD_DIM], probs))
        lse_ref[0, 0, head : head + 1, :] = highest + jnp.log(totals)
    ctx = jnp.concatenate(pieces, axis=0).T.astype(BF)
    ctx_ref[0] = ctx
    result = dot_nn(ctx, ow_ref[place.h ^ group])
    spot = pl.ds(pl.multiple_of(row * LEN, LEN), LEN)

    @pl.when(group == 0)
    def _():
        out_ref[spot, :] = result + ob_ref[...]

    @pl.when(group > 0)
    def _():
        out_ref[spot, :] = out_ref[spot, :] + result

    @pl.when(step == 1)
    def _():
        direct(1).wait()
        cross(1).start()

    @pl.when(step == 3)
    def _():
        direct(2).wait()
        cross(2).start()
        relay.start()

    @pl.when(step == 5)
    def _():
        relay.wait()
        cross(3).start()

    @pl.when(step == 7)
    def _():
        for g in range(4):
            store(g).wait()


def early_call(x, own, bias, ow, ob):
    tokens, features = x.shape
    width = own.shape[2]
    groups = features // width
    rows = tokens // LEN
    hbm = pl.BlockSpec(memory_space=pl.ANY)
    per_head = pl.BlockSpec((1, LEN, width), lambda s: (s // 2, s % 2, 0))
    stacked = jax.ShapeDtypeStruct((groups, tokens, width), BF)
    dma = pltpu.SemaphoreType.DMA
    return pl.pallas_call(
        early_kernel,
        grid=(groups * rows,),
        in_specs=[
            pl.BlockSpec((LEN, features), lambda s: (s % 2, 0)),
            hbm,
            hbm,
            pl.BlockSpec((groups, width, features), lambda s: (0, 0, 0)),
            pl.BlockSpec((1, features), lambda s: (0, 0)),
        ],
        out_specs=[
            per_head,
            per_head,
            per_head,
            per_head,
            pl.BlockSpec((1, 1, 8, LEN), lambda s: (s // 2, s % 2, 0, 0)),
            pl.BlockSpec((tokens, features), lambda s: (0, 0)),
            hbm,
        ],
        out_shape=[
            stacked,
            stacked,
            stacked,
            stacked,
            jax.ShapeDtypeStruct((groups, rows, 8, LEN), F32),
            jax.ShapeDtypeStruct((tokens, features), F32),
            jax.ShapeDtypeStruct((groups,) + own.shape, BF),
        ],
        scratch_shapes=[
            pltpu.VMEM((groups,) + own.shape, BF),
            pltpu.VMEM((groups, 8, width), F32),
            dma((3, 4)),
            dma((3, 4)),
            dma((6,)),
        ],
        compiler_params=pltpu.CompilerParams(
            dimension_semantics=("arbitrary",),
            vmem_limit_bytes=56 << 20,
            collective_id=0,
            has_side_effects=True,
        ),
        name="early_kernel",
    )(x, own, bias, ow, ob)


LANES = 384
CHUNK = 512
TICKS = 3
SPACING = 2


def add_into(target, source):
    target[...] = (target[...].astype(F32) + source[...].astype(F32)).astype(BF)


class MatrixSum:
    COPIES = 17

    def __init__(self, place, parts, keep, first, second, third, fourth, full, send, recv, local):
        self.place = place
        self.parts = parts
        self.keep, self.first, self.second = keep, first, second
        self.third, self.fourth, self.full = third, fourth, full
        self.send, self.recv, self.local = send, recv, local

    def copy(self, i, slot, src, dst, where):
        return remote(src, dst, self.send.at[i, slot], self.recv.at[i, slot], where)

    def fetches(self, i, source, index):
        p = self.place
        out = []
        for zl in range(2):
            lanes = pl.ds(zl * LANES, LANES)
            out.append(
                pltpu.make_async_copy(
                    source.at[index, p.c, :, :, :, :, :, lanes],
                    self.keep.at[i, :, :, :, :, zl],
                    self.local.at[i, zl],
                )
            )
        return out

    def copies(self, phase, i, source=None, index=None):
        p = self.place
        keep, full = self.keep, self.full
        if phase == 1:
            return [
                self.copy(
                    i,
                    zl,
                    source.at[index, 1 - p.c, :, :, :, :, :, pl.ds(zl * LANES, LANES)],
                    self.first.at[i, :, :, :, :, zl],
                    p.core(),
                )
                for zl in range(2)
            ]
        if phase == 2:
            out = [
                self.copy(i, 2, keep.at[i, 0, 1 - p.x], self.second.at[i, 0], p.side("x")),
                self.copy(i, 3, keep.at[i, 1, :, 1 - p.y], self.second.at[i, 1], p.side("y"))
                if self.parts == 2
                else None,
            ]
        if phase == 3:
            out = [
                self.copy(i, 4, keep.at[i, 0, p.x, 1 - p.y], self.third.at[i, 0], p.side("y")),
                self.copy(i, 5, keep.at[i, 1, 1 - p.x, p.y], self.third.at[i, 1], p.side("x"))
                if self.parts == 2
                else None,
            ]
        if phase == 4:
            out = []
            for o in range(1, 4):
                t = p.h ^ o
                out.append(
                    self.copy(
                        i,
                        5 + o,
                        keep.at[i, :, p.x, p.y, t >> 1, t & 1],
                        self.fourth.at[i, o - 1],
                        p.up(o),
                    )
                )
        if phase == 5:
            spot = full.at[i, p.c, :, p.x, p.y, p.h >> 1, p.h & 1]
            out = [self.copy(i, 8 + o, spot, spot, p.up(o)) for o in range(1, 4)]
        if phase == 6:
            spot = full.at[i, p.c, 0, p.x, p.y]
            out = [self.copy(i, 12, spot, spot, p.side("y"))]
            if self.parts == 2:
                spot = full.at[i, p.c, 1, p.x, p.y]
                out.append(self.copy(i, 13, spot, spot, p.side("x")))
        if phase == 7:
            spot = full.at[i, p.c, 0, p.x]
            out = [self.copy(i, 14, spot, spot, p.side("x"))]
            if self.parts == 2:
                spot = full.at[i, p.c, 1, :, p.y]
                out.append(self.copy(i, 15, spot, spot, p.side("y")))
        if phase == 8:
            spot = full.at[i, p.c]
            out = [self.copy(i, 16, spot, spot, p.core())]
        return [one for one in out if one is not None]

    def begin(self, i, source, index):
        for one in self.fetches(i, source, index) + self.copies(1, i, source, index):
            one.start()

    def advance(self, phase, i, source=None, index=None):
        p = self.place
        if phase == 2:
            for one in self.fetches(i, source, index):
                one.wait()
        for one in self.copies(phase - 1, i, source, index):
            one.wait()
        if phase == 2:
            add_into(self.keep.at[i], self.first.at[i])
        if phase == 3:
            add_into(self.keep.at[i, 0, p.x], self.second.at[i, 0])
            if self.parts == 2:
                add_into(self.keep.at[i, 1, :, p.y], self.second.at[i, 1])
        if phase == 4:
            for part in range(self.parts):
                add_into(self.keep.at[i, part, p.x, p.y], self.third.at[i, part])
        if phase == 5:
            total = self.keep[i, :, p.x, p.y, p.h >> 1, p.h & 1].astype(F32)
            for o in range(3):
                total = total + self.fourth[i, o].astype(F32)
            self.full[i, p.c, :, p.x, p.y, p.h >> 1, p.h & 1] = total.astype(BF)
        if phase <= 8:
            for one in self.copies(phase, i):
                one.start()


class GroupSum:
    def __init__(self, place, own, first, second, third, fourth, full, send, recv):
        self.place = place
        self.own, self.first, self.second = own, first, second
        self.third, self.fourth, self.full = third, fourth, full
        self.send, self.recv = send, recv

    def copy(self, g, slot, src, dst, where):
        return remote(src, dst, self.send.at[g, slot], self.recv.at[g, slot], where)

    def copies(self, phase, g):
        p, own, full = self.place, self.own, self.full
        if phase == 1:
            return [self.copy(g, 0, own.at[g, 1 - p.c], self.first.at[g], p.core())]
        even = g % 2 == 0
        if phase == 2:
            src = own.at[g, p.c, 1 - p.x] if even else own.at[g, p.c, :, 1 - p.y]
            return [self.copy(g, 1, src, self.second.at[g], p.side("x" if even else "y"))]
        if phase == 3:
            src = own.at[g, p.c, p.x, 1 - p.y] if even else own.at[g, p.c, 1 - p.x, p.y]
            return [self.copy(g, 2, src, self.third.at[g], p.side("y" if even else "x"))]
        if phase == 4:
            if g == 0:
                return []
            src = own.at[g, p.c, p.x, p.y]
            return [self.copy(g, 3, src, self.fourth.at[g - 1], p.up(g))]
        if phase == 6:
            spot = full.at[p.c, p.x, p.y]
            return [self.copy(0, 4, spot, spot, p.side("y"))]
        if phase == 7:
            spot = full.at[p.c, p.x]
            return [self.copy(0, 5, spot, spot, p.side("x"))]
        if phase == 8:
            spot = full.at[p.c]
            return [self.copy(0, 6, spot, spot, p.core())]
        return []

    def begin(self, g):
        for one in self.copies(1, g):
            one.start()

    def advance(self, phase, g):
        p, own = self.place, self.own
        if phase == 6:
            for group in range(own.shape[0]):
                for one in self.copies(4, group):
                    one.wait()
            total = own[0, p.c, p.x, p.y].astype(F32)
            for o in range(3):
                total = total + self.fourth[o].astype(F32)
            self.full[p.c, p.x, p.y] = total.astype(BF)
        else:
            for one in self.copies(phase - 1, g):
                one.wait()
        if phase == 2:
            add_into(own.at[g, p.c], self.first.at[g])
        if phase == 3:
            if g % 2 == 0:
                add_into(own.at[g, p.c, p.x], self.second.at[g])
            else:
                add_into(own.at[g, p.c, :, p.y], self.second.at[g])
        if phase == 4:
            add_into(own.at[g, p.c, p.x, p.y], self.third.at[g])
        for one in self.copies(phase, g):
            one.start()


def late_kernel(
    chunks,
    x_ref,
    w_ref,
    ow_ref,
    q_ref,
    k_ref,
    v_ref,
    lse_ref,
    ga_ref,
    gf_ref,
    mask_ref,
    early_0,
    early_1,
    early_2,
    early_3,
    early_4,
    early_5,
    early_up,
    early_squares,
    down_ref,
    up_ref,
    outw_ref,
    dx_ref,
    wg_ref,
    vec_ref,
    down_out,
    up_out,
    outw_out,
    wg_acc,
    k_t,
    dq_t,
    dk_acc,
    dv_acc,
    stage_up,
    vec,
    vec_in,
    ff_keep,
    ff_1,
    ff_2,
    ff_3,
    ff_4,
    ff_full,
    ow_keep,
    ow_1,
    ow_2,
    ow_3,
    ow_4,
    ow_full,
    qk_own,
    qk_1,
    qk_2,
    qk_3,
    qk_4,
    qk_full,
    ff_send,
    ff_recv,
    ff_local,
    ow_send,
    ow_recv,
    ow_local,
    qk_send,
    qk_recv,
    vec_send,
    vec_recv,
    store_sem,
):
    step = pl.program_id(0)
    group, row = step // 2, step % 2
    place = Place()
    half = chunks // 2
    count = qk_own.shape[0]
    feed = MatrixSum(
        place, 2, ff_keep, ff_1, ff_2, ff_3, ff_4, ff_full, ff_send, ff_recv, ff_local
    )
    outer = MatrixSum(
        place, 1, ow_keep, ow_1, ow_2, ow_3, ow_4, ow_full, ow_send, ow_recv, ow_local
    )
    groups = GroupSum(place, qk_own, qk_1, qk_2, qk_3, qk_4, qk_full, qk_send, qk_recv)
    tail = 2 * count * TICKS

    @pl.when(step == 0)
    def _():
        greet(
            [place.core(), place.side("x"), place.side("y")] + [place.up(o) for o in range(1, 4)]
        )
        vec[...] = jnp.zeros_like(vec)
        for index, ref in enumerate((early_0, early_1, early_2, early_3, early_4, early_5)):
            vec[0, index : index + 1, :] = ref[...]
        vec[0, 6:10, :] = early_up[...]
        vec[0, 10:11, :] = early_squares[...]

    def lanes(zl):
        return pl.ds(zl * LANES, LANES)

    def down_store(i):
        return [
            pltpu.make_async_copy(
                ff_full.at[i, :, :, :, :, :, zl],
                down_out.at[i, :, :, :, :, :, :, lanes(zl)],
                store_sem.at[i, zl],
            )
            for zl in range(2)
        ]

    def up_store(i):
        spot = pl.ds(pl.multiple_of(i * CHUNK, CHUNK), CHUNK)
        return pltpu.make_async_copy(
            stage_up.at[i % 2], up_out.at[:, spot], store_sem.at[half + i, 0]
        )

    def outw_store():
        return [
            pltpu.make_async_copy(
                ow_full.at[0, :, :, :, :, :, zl],
                outw_out.at[0, :, :, :, :, :, :, lanes(zl)],
                store_sem.at[chunks, zl],
            )
            for zl in range(2)
        ]

    def tick(t, start, stop):
        for phase in range(9, 1, -1):
            behind = SPACING * (phase - 1)
            if stop - behind <= 0 or start - behind > chunks:
                continue
            i = t - behind

            @pl.when((i >= 0) & (i < half))
            def _():
                feed.advance(phase, i, down_ref, i)
                if phase == 9:
                    for one in down_store(i):
                        one.start()

            @pl.when((i >= half) & (i < chunks))
            def _():
                feed.advance(phase, i, up_ref, i - half)
                if phase == 9:

                    @pl.when(i > half + 1)
                    def _():
                        up_store(i - half - 2).wait()

                    for zl in range(2):
                        block = ff_full[i, :, :, :, :, :, zl].reshape(CHUNK, LANES)
                        stage_up[(i - half) % 2, zl * LANES : (zl + 1) * LANES, :] = block.T
                    up_store(i - half).start()

            @pl.when(i == chunks)
            def _():
                outer.advance(phase, 0, outw_ref, 0)
                if phase == 9:
                    for one in outw_store():
                        one.start()

        if start <= chunks:

            @pl.when(t < half)
            def _():
                feed.begin(t, down_ref, t)

            @pl.when((t >= half) & (t < chunks))
            def _():
                feed.begin(t, up_ref, t - half)

            @pl.when(t == chunks)
            def _():
                outer.begin(0, outw_ref, 0)

        for g in range(count):
            base = 2 * TICKS * (g + 1)
            if base < start or base >= stop:
                continue
            phases = (9, 8, 7, 6, 4, 3, 2) if g == count - 1 else (4, 3, 2)
            for phase in phases:
                when = phase - 1 if phase < 5 else phase - 2

                @pl.when(t == base + when)
                def _():
                    groups.advance(phase, g)

            @pl.when(t == base)
            def _():
                groups.begin(g)

    width = q_ref.shape[2]
    heads = width // HEAD_DIM
    x = x_ref[...]
    ga = ga_ref[...]
    dctx = dot_nt(ga, ow_ref[place.h ^ group]).astype(BF)
    q = q_ref[0]
    k = k_ref[0]
    v = v_ref[0]
    k_t[...] = k.T
    q_scaled = q * jnp.asarray(0.125, BF)

    @pl.loop(0, heads)
    def _(head):
        tick(step * TICKS + head, 0, tail)
        mask = head_lanes(width, head)
        spot = pl.ds(pl.multiple_of(head * HEAD_DIM, HEAD_DIM), HEAD_DIM)
        scores = dot_nt(jnp.where(mask, k, jnp.zeros_like(k)), q_scaled)
        probs = jnp.exp(scores - lse_ref[0, 0, pl.ds(head, 1), :])
        dprobs = dot_nt(jnp.where(mask, v, jnp.zeros_like(v)), dctx)
        delta = jnp.sum(probs * dprobs, axis=0, keepdims=True)
        dscores = (probs * (dprobs - delta)).astype(BF)
        dv_acc[...] = jnp.where(mask, dot_nn(probs.astype(BF), dctx), dv_acc[...])
        dk_acc[...] = jnp.where(mask, dot_nn(dscores, q_scaled), dk_acc[...])
        dq_t[spot, :] = dot_nn(k_t[spot, :], dscores)

    dq = (dq_t[...] * 0.125).T.astype(BF)
    dk = dk_acc[...].astype(BF)
    dv = dv_acc[...].astype(BF)
    part = dot_nt(dq, w_ref[0, 0]) + dot_nt(dk, w_ref[0, 1]) + dot_nt(dv, w_ref[0, 2])
    mine = pl.ds(pl.multiple_of(row * LEN, LEN), LEN)

    @pl.when(group == 0)
    def _():
        dx_ref[mine, :] = gf_ref[...] + part

    @pl.when(group > 0)
    def _():
        dx_ref[mine, :] = dx_ref[mine, :] + part

    @pl.when(row == 0)
    def _():
        wg_acc[...] = jnp.zeros_like(wg_acc)

    for index, grad in enumerate((dq, dk, dv)):
        wg_acc[index * width : (index + 1) * width] += dot_tn(grad, x)
    spot = place.h ^ group
    vec[0, pl.ds(16 + spot, 1), 0:width] += jnp.sum(dq.astype(F32), axis=0, keepdims=True)
    vec[0, pl.ds(20 + spot, 1), 0:width] += jnp.sum(dv.astype(F32), axis=0, keepdims=True)

    @pl.when(row == 1)
    def _():
        shape = qk_own.shape[2:]
        for zl in range(2):
            block = wg_acc[:, zl * LANES : (zl + 1) * LANES].astype(BF)
            qk_own[group, zl] = block.reshape(shape)

    @pl.when(group == count - 1)
    def _():
        total = jnp.where(mask_ref[...] == 1.0, dx_ref[mine, :], 0.0)
        vec[0, 15:16, :] += jnp.sum(total, axis=0, keepdims=True)

    @pl.when(step == 2 * count - 1)
    def _():
        def vec_copy(k):
            if k < 3:
                where = (place.dp ^ (1 << k), place.h)
            else:
                where = (place.dp, place.h ^ (1 << (k - 3)))
            return remote(vec.at[k], vec_in.at[k], vec_send.at[k], vec_recv.at[k], where)

        @pl.loop(tail, tail + 8)
        def _(t):
            tick(t, tail, tail + 8)
            for k in range(6):

                @pl.when(t == tail + k)
                def _():
                    if k > 0:
                        vec_copy(k - 1).wait()
                        vec[k] = vec[k - 1] + vec_in[k - 1]
                    if k < 5:
                        vec_copy(k).start()

        vec_ref[...] = vec[5]
        for c in range(2):
            block = qk_full[c].reshape(wg_ref.shape[0], LANES)
            wg_ref[:, c * LANES : (c + 1) * LANES] = block.astype(F32)
        for i in range(half):
            for one in down_store(i):
                one.wait()
        for i in (half - 2, half - 1):
            up_store(i).wait()
        for one in outw_store():
            one.wait()


def late_call(x, w, ow, q, k, v, lse, ga, gf, mask, early, down, up, outw):
    tokens, features = x.shape
    count, _, _, width = w.shape
    ff = down.shape[0]
    chunks = 2 * ff // CHUNK
    chunked = (ff // CHUNK, 2, 2, 2, 2, 2, 16, features)
    squared = (1, 2, 1, 2, 2, 2, features // 16, features)
    hbm = pl.BlockSpec(memory_space=pl.ANY)

    def whole(shape):
        return pl.BlockSpec(shape, lambda s: (0,) * len(shape))

    per_head = pl.BlockSpec((1, LEN, width), lambda s: (s // 2, s % 2, 0))
    per_row = pl.BlockSpec((LEN, features), lambda s: (s % 2, 0))
    in_specs = [
        per_row,
        pl.BlockSpec((1, 3, features, width), lambda s: (s // 2, 0, 0, 0)),
        whole(ow.shape),
        per_head,
        per_head,
        per_head,
        pl.BlockSpec((1, 1, 8, LEN), lambda s: (s // 2, s % 2, 0, 0)),
        per_row,
        pl.BlockSpec((LEN, features), lambda s: (jnp.minimum(s, 1), 0)),
        pl.BlockSpec((LEN, 1), lambda s: (s % 2, 0)),
    ]
    in_specs += [whole(one.shape) for one in early]
    in_specs += [hbm, hbm, hbm]
    out_specs = [
        whole((tokens, features)),
        whole((3 * width, features)),
        whole((24, features)),
        hbm,
        hbm,
        hbm,
    ]
    out_shape = [
        jax.ShapeDtypeStruct((tokens, features), F32),
        jax.ShapeDtypeStruct((3 * width, features), F32),
        jax.ShapeDtypeStruct((24, features), F32),
        jax.ShapeDtypeStruct(chunked, BF),
        jax.ShapeDtypeStruct((features, ff), BF),
        jax.ShapeDtypeStruct(squared, BF),
    ]

    def sum_buffers(n, parts, rows):
        block = (rows, LANES)
        return [
            pltpu.VMEM((n, parts, 2, 2, 2, 2) + block, BF),
            pltpu.VMEM((n, parts, 2, 2, 2, 2) + block, BF),
            pltpu.VMEM((n, parts, 2, 2, 2) + block, BF),
            pltpu.VMEM((n, parts, 2, 2) + block, BF),
            pltpu.VMEM((n, 3, parts) + block, BF),
            pltpu.VMEM((n, 2, parts, 2, 2, 2, 2) + block, BF),
        ]

    qrows = 3 * width // 4
    scratch = [
        pltpu.VMEM((3 * width, features), F32),
        pltpu.VMEM((width, LEN), BF),
        pltpu.VMEM((width, LEN), F32),
        pltpu.VMEM((LEN, width), F32),
        pltpu.VMEM((LEN, width), F32),
        pltpu.VMEM((2, features, CHUNK), BF),
        pltpu.VMEM((6, 24, features), F32),
        pltpu.VMEM((5, 24, features), F32),
    ]
    scratch += sum_buffers(chunks, 2, 16)
    scratch += sum_buffers(1, 1, features // 16)
    scratch += [
        pltpu.VMEM((count, 2, 2, 2, qrows, LANES), BF),
        pltpu.VMEM((count, 2, 2, qrows, LANES), BF),
        pltpu.VMEM((count, 2, qrows, LANES), BF),
        pltpu.VMEM((count, qrows, LANES), BF),
        pltpu.VMEM((3, qrows, LANES), BF),
        pltpu.VMEM((2, 2, 2, qrows, LANES), BF),
    ]
    dma = pltpu.SemaphoreType.DMA
    scratch += [
        dma((chunks, MatrixSum.COPIES)),
        dma((chunks, MatrixSum.COPIES)),
        dma((chunks, 2)),
        dma((1, MatrixSum.COPIES)),
        dma((1, MatrixSum.COPIES)),
        dma((1, 2)),
        dma((count, 7)),
        dma((count, 7)),
        dma((5,)),
        dma((5,)),
        dma((chunks + 1, 2)),
    ]
    results = pl.pallas_call(
        functools.partial(late_kernel, chunks),
        grid=(2 * count,),
        in_specs=in_specs,
        out_specs=out_specs,
        out_shape=out_shape,
        scratch_shapes=scratch,
        compiler_params=pltpu.CompilerParams(
            dimension_semantics=("arbitrary",),
            vmem_limit_bytes=67043328,
            collective_id=1,
            has_side_effects=True,
        ),
        name="late_kernel",
    )(
        x,
        w,
        ow,
        q,
        k,
        v,
        lse,
        ga,
        gf,
        mask,
        *early,
        down.reshape(chunked),
        up.reshape(chunked),
        outw.reshape(squared),
    )
    dx, wg, sums, down_sum, up_sum, outw_sum = results
    return (
        dx,
        wg,
        sums,
        down_sum.reshape(ff, features),
        up_sum,
        outw_sum.reshape(features, features),
    )


def swap(value, axis, mask, size):
    return lax.ppermute(value, axis, [(i, i ^ mask) for i in range(size)])


def bit_of(axis, bit):
    return (lax.axis_index(axis) >> bit) & 1


def joined(mine, other, upper, dim, kind=None):
    low = jnp.where(upper == 1, other, mine)
    high = jnp.where(upper == 1, mine, other)
    if kind is not None:
        low, high = low.astype(kind), high.astype(kind)
    return jnp.concatenate([low, high], axis=dim)


def halve(value, bit, size, dim):
    half = value.shape[dim] // 2
    mine = bit_of("dp", bit)
    sent = lax.dynamic_slice_in_dim(value, (1 - mine) * half, half, dim)
    kept = lax.dynamic_slice_in_dim(value, mine * half, half, dim)
    received = swap(sent, "dp", 1 << bit, size)
    return (kept.astype(F32) + received.astype(F32)).astype(BF)


def double(value, bit, size, dim, kind=None):
    return joined(value, swap(value, "dp", 1 << bit, size), bit_of("dp", bit), dim, kind)


def plane_orders(size):
    bits = size.bit_length() - 1
    rest = list(range(1, bits))
    return rest, rest[::-1]


def reduce_plane(value, size, dim):
    value = halve(value, 0, size, dim)
    half = value.shape[dim] // 2
    parts = []
    for index, order in enumerate(plane_orders(size)):
        part = lax.slice_in_dim(value, index * half, (index + 1) * half, axis=dim)
        for bit in order:
            part = halve(part, bit, size, dim)
        parts.append(part)
    return parts


def gather_plane(parts, size, dim, kind=None):
    done = []
    for part, order in zip(parts, plane_orders(size)):
        for bit in order[::-1]:
            part = double(part, bit, size, dim)
        done.append(part)
    return double(jnp.concatenate(done, axis=dim), 0, size, dim, kind)


def reduce_head(pieces, size):
    total = pieces[0].astype(F32)
    for offset in range(1, size):
        total = total + swap(pieces[offset], "head", offset, size).astype(F32)
    return total


def gather_head(piece, size):
    return [piece] + [swap(piece, "head", offset, size) for offset in range(1, size)]


def absolute(pieces, dim):
    count = len(pieces)
    bit = 0
    while (1 << bit) < count:
        upper = bit_of("head", bit)
        step = 1 << bit
        pieces = [
            jnp.where(upper == 1, pieces[index ^ step], pieces[index]) for index in range(count)
        ]
        bit += 1
    return jnp.concatenate(pieces, axis=dim)


def own_pieces(value, size, dim):
    width = value.shape[dim] // size
    me = lax.axis_index("head")
    return [
        lax.dynamic_slice_in_dim(value, (me ^ offset) * width, width, dim)
        for offset in range(size)
    ]


def all_reduce_matrix(value, dp, head, head_dim):
    parts = []
    for part in reduce_plane(value, dp, 0):
        piece = reduce_head(own_pieces(part, head, head_dim), head).astype(BF)
        parts.append(absolute(gather_head(piece, head), head_dim))
    return gather_plane(parts, dp, 0, F32)


def all_reduce_small(vector, dp, head):
    bit = 1
    while bit < dp:
        vector = vector + swap(vector, "dp", bit, dp)
        bit *= 2
    bit = 1
    while bit < head:
        vector = vector + swap(vector, "head", bit, head)
        bit *= 2
    return vector


def norm_forward(hidden, gain, bias):
    center = hidden - jnp.mean(hidden, axis=-1, keepdims=True)
    inverse = lax.rsqrt(jnp.mean(center * center, axis=-1, keepdims=True) + EPS)
    normal = center * inverse
    return (normal * gain + bias, normal, inverse)


def norm_backward(upstream, normal, inverse, gain):
    gain_grad = jnp.sum(upstream * normal, axis=0)
    bias_grad = jnp.sum(upstream, axis=0)
    scaled = upstream * gain
    hidden_grad = inverse * (
        scaled
        - jnp.mean(scaled, axis=-1, keepdims=True)
        - normal * jnp.mean(scaled * normal, axis=-1, keepdims=True)
    )
    return (hidden_grad, gain_grad, bias_grad)


def phi(values):
    return 0.5 * (1.0 + jax.scipy.special.erf(values * (1.0 / math.sqrt(2.0))))


def body(
    dp,
    head,
    tokens,
    span_mask,
    valid_mask,
    mask_embedding,
    qkv_weight,
    query_bias,
    value_bias,
    out_weight,
    out_bias,
    norm1_gain,
    norm1_bias,
    up_weight,
    up_bias,
    down_weight,
    down_bias,
    norm2_gain,
    norm2_bias,
    out_grad,
):
    features = tokens.shape[1]
    width = qkv_weight.shape[2]
    masked = (span_mask == 1)[:, None]
    inputs = jnp.where(masked, mask_embedding[None, :], tokens)
    inputs_wide = inputs.astype(F32)
    validity = valid_mask.astype(F32)[:, None]

    direct = dp == 8 and head == 4 and features == 2 * LANES and tokens.shape[0] == 2 * LEN
    own = jnp.transpose(qkv_weight, (1, 0, 2))
    if direct:
        bias_block = jnp.pad(jnp.stack([query_bias, value_bias]).astype(F32), ((0, 6), (0, 0)))
        out_parts = out_weight.reshape(head, width, features)
        q, k, v, ctx, lse, attended, weights = early_call(
            inputs, own, bias_block, out_parts, out_bias[None, :]
        )
    else:
        core = bit_of("dp", 0)
        half = lax.dynamic_slice_in_dim(own, core * (features // 2), features // 2, 1)
        halves = [half]
        for bit in range(head.bit_length() - 1):
            halves = halves + [swap(part, "head", 1 << bit, head) for part in halves]
        weights = [own] + [double(part, 0, dp, 1) for part in halves[1:]]
        biases = jnp.stack([query_bias, value_bias]).astype(F32)
        bias_parts = [biases]
        for bit in range(head.bit_length() - 1):
            bias_parts = bias_parts + [swap(part, "head", 1 << bit, head) for part in bias_parts]
        out_parts = own_pieces(out_weight, head, 0)

        attended = jnp.broadcast_to(out_bias[None, :], tokens.shape)
        saved = []
        for group in range(head):
            q, k, v, ctx, lse, attended = attention_forward(
                inputs,
                weights[group],
                bias_parts[group][0:1],
                bias_parts[group][1:2],
                out_parts[group],
                attended,
            )
            saved.append((q, k, v, ctx, lse))

    normed, normal_first, inverse_first = norm_forward(
        inputs_wide + attended, norm1_gain, norm1_bias
    )
    normed_low = normed.astype(BF)
    preact = dot_nn(normed_low, up_weight) + up_bias
    activated = (preact * phi(preact)).astype(BF)
    feedout = dot_nn(activated, down_weight) + down_bias
    result, normal_second, inverse_second = norm_forward(normed + feedout, norm2_gain, norm2_bias)
    grad_output = out_grad.astype(F32) * validity
    grad_second, gain_second_grad, bias_second_grad = norm_backward(
        grad_output, normal_second, inverse_second, norm2_gain
    )
    grad_feed = grad_second.astype(BF)
    down_bias_grad = jnp.sum(grad_feed, axis=0, dtype=F32)
    down_local = dot_tn(activated, grad_feed).astype(BF)
    slope = phi(preact) + preact * jnp.exp(-0.5 * preact * preact) * (
        1.0 / math.sqrt(2.0 * math.pi)
    )
    grad_preact = (dot_nt(grad_feed, down_weight) * slope).astype(BF)
    up_bias_grad = jnp.sum(grad_preact, axis=0, dtype=F32)
    grad_normed = dot_nt(grad_preact, up_weight) + grad_second
    grad_first, gain_first_grad, bias_first_grad = norm_backward(
        grad_normed, normal_first, inverse_first, norm1_gain
    )
    grad_attended = grad_first.astype(BF)
    out_bias_grad = jnp.sum(grad_attended, axis=0, dtype=F32)
    squares = jnp.stack(
        [
            jnp.sum(validity * inputs_wide * inputs_wide),
            jnp.sum(validity * attended * attended),
            jnp.sum(validity * feedout * feedout),
            jnp.sum(validity),
        ]
    )
    early = [
        down_bias_grad,
        gain_second_grad,
        bias_second_grad,
        gain_first_grad,
        bias_first_grad,
        out_bias_grad,
        up_bias_grad,
        squares,
    ]
    if direct:
        up_local = dot_tn(grad_preact, normed_low).astype(BF)
        outw = lax.dot_general(
            ctx, grad_attended, (((1,), (0,)), ((), ())), preferred_element_type=F32
        ).astype(BF)
        outw_local = absolute([outw[g] for g in range(head)], 0)
        vectors = [one[None, :] for one in early[:6]]
        vectors.append(up_bias_grad.reshape(-1, features))
        vectors.append(jnp.pad(squares, (0, features - 4))[None, :])
        dx, weight_sum, sums, down_sum, up_sum, outw_sum = late_call(
            inputs,
            weights,
            out_parts,
            q,
            k,
            v,
            lse,
            grad_attended,
            grad_first,
            (span_mask == 1).astype(F32)[:, None],
            vectors,
            down_local,
            up_local,
            outw_local,
        )
        tokens_grad = jnp.where(masked, 0.0, dx)
        down_weight_grad = down_sum.astype(F32)
        up_weight_grad = up_sum.astype(F32)
        out_weight_grad = outw_sum.astype(F32)
        weight_grad = jnp.transpose(weight_sum.reshape(3, width, features), (2, 0, 1))
        me = lax.axis_index("head")
        first_grad = lax.dynamic_slice(sums, (16 + me, 0), (1, width))[0]
        third_grad = lax.dynamic_slice(sums, (20 + me, 0), (1, width))[0]
        squares = sums[10, :4]
        count = jnp.maximum(squares[3], 1.0)
        stream_rms = jnp.sqrt(squares[:3] / (count * features))
        return (
            result.astype(BF),
            tokens_grad,
            sums[15],
            weight_grad,
            first_grad,
            third_grad,
            out_weight_grad,
            sums[5],
            sums[3],
            sums[4],
            up_weight_grad,
            sums[6:10].reshape(-1),
            down_weight_grad,
            sums[0],
            sums[1],
            sums[2],
            stream_rms,
        )

    up_local = dot_tn(normed_low, grad_preact).astype(BF)
    down_weight_grad = all_reduce_matrix(down_local, dp, head, 0)
    up_weight_grad = all_reduce_matrix(up_local, dp, head, 1)
    early_sum = all_reduce_small(jnp.concatenate(early), dp, head)

    grad_inputs = grad_first
    weight_pieces = []
    out_pieces = []
    query_parts = []
    value_parts = []
    for group in range(head):
        q, k, v, ctx, lse = saved[group]
        weight_piece, out_piece, query_part, value_part, grad_inputs = attention_backward(
            inputs,
            weights[group],
            out_parts[group],
            q,
            k,
            v,
            ctx,
            lse,
            grad_attended,
            grad_inputs,
        )
        weight_pieces.append(reduce_plane(weight_piece, dp, 1))
        out_pieces.append(out_piece)
        query_parts.append(query_part[0])
        value_parts.append(value_part[0])

    weight_grad = gather_plane(
        [
            reduce_head([weight_pieces[group][part] for group in range(head)], head).astype(BF)
            for part in range(2)
        ],
        dp,
        1,
        F32,
    )
    weight_grad = jnp.transpose(weight_grad, (1, 0, 2))

    out_reduced = jnp.stack(out_pieces)
    for bit in range(dp.bit_length() - 1):
        out_reduced = halve(out_reduced, bit, dp, 1)
    out_piece = reduce_head([out_reduced[group] for group in range(head)], head).astype(BF)
    for bit in range(dp.bit_length() - 2, -1, -1):
        out_piece = double(out_piece, bit, dp, 0)
    out_weight_grad = absolute(gather_head(out_piece, head), 0).astype(F32)

    tokens_grad = jnp.where(masked, 0.0, grad_inputs)
    embedding_grad = jnp.sum(jnp.where(masked, grad_inputs, 0.0), axis=0)
    late = jnp.concatenate([embedding_grad, absolute(query_parts, 0), absolute(value_parts, 0)])
    late_sum = all_reduce_small(late, dp, head)
    embedding_grad = late_sum[:features]
    me = lax.axis_index("head")
    first_grad = lax.dynamic_slice_in_dim(late_sum, features + me * width, width)
    third_grad = lax.dynamic_slice_in_dim(late_sum, 2 * features + me * width, width)

    pieces = []
    offset = 0
    for part in early:
        pieces.append(lax.slice_in_dim(early_sum, offset, offset + part.shape[0]))
        offset += part.shape[0]
    (
        down_bias_grad,
        gain_second_grad,
        bias_second_grad,
        gain_first_grad,
        bias_first_grad,
        out_bias_grad,
        up_bias_grad,
        squares,
    ) = pieces
    count = jnp.maximum(squares[3], 1.0)
    stream_rms = jnp.sqrt(squares[:3] / (count * features))
    return (
        result.astype(BF),
        tokens_grad,
        embedding_grad,
        weight_grad,
        first_grad,
        third_grad,
        out_weight_grad,
        out_bias_grad,
        gain_first_grad,
        bias_first_grad,
        up_weight_grad,
        up_bias_grad,
        down_weight_grad,
        down_bias_grad,
        gain_second_grad,
        bias_second_grad,
        stream_rms,
    )


def solution(mesh):
    split = P(("dp", "head"), None)
    flat = P(("dp", "head"))
    placed = (split, flat, flat, P(), P(None, None, "head"), P("head"), P("head")) + (P(),) * 10
    placed = placed + (split,)
    outs = (split, split, P(), P(None, None, "head"), P("head"), P("head")) + (P(),) * 11
    return jax.shard_map(
        functools.partial(body, mesh.shape["dp"], mesh.shape["head"]),
        mesh=mesh,
        in_specs=placed,
        out_specs=outs,
        check_vma=False,
    )
```

```python
import functools
import math

import jax
import jax.numpy as jnp
from jax import lax
from jax.experimental import pallas as pl
from jax.experimental.pallas import tpu as pltpu
from jax.sharding import PartitionSpec as P

HEAD_DIM = 64
LEN = 512
EPS = 1e-12
BF = jnp.bfloat16
F32 = jnp.float32


def dot_nn(left, right):
    return lax.dot_general(left, right, (((1,), (0,)), ((), ())), preferred_element_type=F32)


def dot_nt(left, right):
    return lax.dot_general(left, right, (((1,), (1,)), ((), ())), preferred_element_type=F32)


def dot_tn(left, right):
    return lax.dot_general(left, right, (((0,), (0,)), ((), ())), preferred_element_type=F32)


def head_lanes(width, head):
    lanes = lax.broadcasted_iota(jnp.int32, (1, width), 1)
    return (lanes >= head * HEAD_DIM) & (lanes < (head + 1) * HEAD_DIM)


def forward_kernel(
    x_ref, w_ref, qb_ref, vb_ref, ow_ref, acc_ref, q_ref, k_ref, v_ref, ctx_ref, lse_ref, out_ref
):
    x = x_ref[...]
    width = w_ref.shape[2]
    heads = width // HEAD_DIM
    q = (dot_nn(x, w_ref[0]) + qb_ref[...]).astype(BF)
    k = dot_nn(x, w_ref[1]).astype(BF)
    v32 = dot_nn(x, w_ref[2]) + vb_ref[...]
    v = v32.astype(BF)
    q_ref[...] = q
    k_ref[...] = k
    v_ref[...] = v
    v_t = v.T
    q_scaled = q * jnp.asarray(0.125, BF)
    pieces = []
    for head in range(heads):
        k_head = jnp.where(head_lanes(width, head), k, jnp.zeros_like(k))
        scores = dot_nt(k_head, q_scaled)
        highest = jnp.max(scores, axis=0, keepdims=True)
        exponent = jnp.exp(scores - highest)
        totals = jnp.sum(exponent, axis=0, keepdims=True)
        probs = (exponent * (1.0 / totals)).astype(BF)
        pieces.append(dot_nn(v_t[head * HEAD_DIM : (head + 1) * HEAD_DIM], probs))
        lse_ref[0, head : head + 1, :] = highest + jnp.log(totals)
    ctx = jnp.concatenate(pieces, axis=0).T.astype(BF)
    ctx_ref[...] = ctx
    out_ref[...] = acc_ref[...] + dot_nn(ctx, ow_ref[...])


def backward_kernel(
    x_ref,
    w_ref,
    ow_ref,
    q_ref,
    k_ref,
    v_ref,
    ctx_ref,
    lse_ref,
    ga_ref,
    acc_ref,
    wg_ref,
    owg_ref,
    qbg_ref,
    vbg_ref,
    out_ref,
    wg_acc,
    owg_acc,
):
    row = pl.program_id(0)
    last = pl.num_programs(0) - 1
    width = w_ref.shape[2]
    heads = width // HEAD_DIM
    x = x_ref[...]
    ga = ga_ref[...]
    dctx = dot_nt(ga, ow_ref[...]).astype(BF)
    q = q_ref[...]
    k = k_ref[...]
    v = v_ref[...]
    k_t = k.T
    q_scaled = q * jnp.asarray(0.125, BF)
    dq_t = []
    dk = jnp.zeros(q.shape, F32)
    dv = jnp.zeros(q.shape, F32)
    for head in range(heads):
        mask = head_lanes(width, head)
        scores = dot_nt(jnp.where(mask, k, jnp.zeros_like(k)), q_scaled)
        probs = jnp.exp(scores - lse_ref[0, head : head + 1, :])
        dprobs = dot_nt(jnp.where(mask, v, jnp.zeros_like(v)), dctx)
        delta = jnp.sum(probs * dprobs, axis=0, keepdims=True)
        dscores = (probs * (dprobs - delta)).astype(BF)
        dv = jnp.where(mask, dot_nn(probs.astype(BF), dctx), dv)
        dk = jnp.where(mask, dot_nn(dscores, q_scaled), dk)
        dq_t.append(dot_nn(k_t[head * HEAD_DIM : (head + 1) * HEAD_DIM], dscores))
    dq32 = (jnp.concatenate(dq_t, axis=0) * 0.125).T
    dq = dq32.astype(BF)
    dk = dk.astype(BF)
    dv = dv.astype(BF)
    out_ref[...] = (
        acc_ref[...] + dot_nt(dq, w_ref[0]) + dot_nt(dk, w_ref[1]) + dot_nt(dv, w_ref[2])
    )

    @pl.when(row == 0)
    def _():
        wg_acc[...] = jnp.zeros_like(wg_acc)
        owg_acc[...] = jnp.zeros_like(owg_acc)
        qbg_ref[...] = jnp.zeros_like(qbg_ref)
        vbg_ref[...] = jnp.zeros_like(vbg_ref)

    wg_acc[0] += dot_tn(x, dq)
    wg_acc[1] += dot_tn(x, dk)
    wg_acc[2] += dot_tn(x, dv)
    owg_acc[...] += dot_tn(ctx_ref[...], ga)
    qbg_ref[...] += jnp.sum(dq.astype(F32), axis=0, keepdims=True)
    vbg_ref[...] += jnp.sum(dv.astype(F32), axis=0, keepdims=True)

    @pl.when(row == last)
    def _():
        wg_ref[...] = wg_acc[...].astype(BF)
        owg_ref[...] = owg_acc[...].astype(BF)


def by_row(block):
    rank = len(block)
    return pl.BlockSpec(block, lambda r: (r,) + (0,) * (rank - 1))


def fixed(block):
    rank = len(block)
    return pl.BlockSpec(block, lambda r: (0,) * rank)


def attention_forward(x, w, qb, vb, ow, acc):
    tokens, features = x.shape
    width = w.shape[2]
    rows = tokens // LEN
    flops = 2 * tokens * features * width * 4 + 4 * tokens * LEN * width
    return pl.pallas_call(
        forward_kernel,
        grid=(rows,),
        in_specs=[
            by_row((LEN, features)),
            fixed(w.shape),
            fixed((1, width)),
            fixed((1, width)),
            fixed((width, features)),
            by_row((LEN, features)),
        ],
        out_specs=[
            by_row((LEN, width)),
            by_row((LEN, width)),
            by_row((LEN, width)),
            by_row((LEN, width)),
            by_row((1, 8, LEN)),
            by_row((LEN, features)),
        ],
        out_shape=[jax.ShapeDtypeStruct((tokens, width), BF)] * 4
        + [
            jax.ShapeDtypeStruct((rows, 8, LEN), F32),
            jax.ShapeDtypeStruct((tokens, features), F32),
        ],
        compiler_params=pltpu.CompilerParams(
            dimension_semantics=("arbitrary",), vmem_limit_bytes=48 << 20
        ),
        cost_estimate=pl.CostEstimate(
            flops=4 * flops, bytes_accessed=12 << 20, transcendentals=tokens * LEN * 3
        ),
        name="attention_forward",
    )(x, w, qb, vb, ow, acc)


def attention_backward(x, w, ow, q, k, v, ctx, lse, ga, acc):
    tokens, features = x.shape
    width = w.shape[2]
    rows = tokens // LEN
    flops = 2 * tokens * features * width * 8 + 10 * tokens * LEN * width
    return pl.pallas_call(
        backward_kernel,
        grid=(rows,),
        in_specs=[
            by_row((LEN, features)),
            fixed(w.shape),
            fixed((width, features)),
            by_row((LEN, width)),
            by_row((LEN, width)),
            by_row((LEN, width)),
            by_row((LEN, width)),
            by_row((1, 8, LEN)),
            by_row((LEN, features)),
            by_row((LEN, features)),
        ],
        out_specs=[
            fixed(w.shape),
            fixed((width, features)),
            fixed((1, width)),
            fixed((1, width)),
            by_row((LEN, features)),
        ],
        out_shape=[
            jax.ShapeDtypeStruct(w.shape, BF),
            jax.ShapeDtypeStruct((width, features), BF),
            jax.ShapeDtypeStruct((1, width), F32),
            jax.ShapeDtypeStruct((1, width), F32),
            jax.ShapeDtypeStruct((tokens, features), F32),
        ],
        scratch_shapes=[pltpu.VMEM(w.shape, F32), pltpu.VMEM((width, features), F32)],
        compiler_params=pltpu.CompilerParams(
            dimension_semantics=("arbitrary",), vmem_limit_bytes=48 << 20
        ),
        cost_estimate=pl.CostEstimate(
            flops=4 * flops, bytes_accessed=16 << 20, transcendentals=tokens * LEN * 3
        ),
        name="attention_backward",
    )(x, w, ow, q, k, v, ctx, lse, ga, acc)


MESH = pl.DeviceIdType.MESH


class Place:
    def __init__(self):
        self.dp = lax.axis_index("dp")
        self.h = lax.axis_index("head")
        self.c = self.dp & 1
        self.x = (self.dp >> 1) & 1
        self.y = (self.dp >> 2) & 1

    def core(self):
        return (self.dp ^ 1, self.h)

    def side(self, axis):
        return (self.dp ^ (2 if axis == "x" else 4), self.h)

    def up(self, offset):
        return (self.dp, self.h ^ offset)


def remote(src, dst, send, recv, where):
    return pltpu.make_async_remote_copy(
        src_ref=src,
        dst_ref=dst,
        send_sem=send,
        recv_sem=recv,
        device_id=where,
        device_id_type=MESH,
    )


def greet(friends):
    barrier = pltpu.get_barrier_semaphore()
    for friend in friends:
        pl.semaphore_signal(barrier, inc=1, device_id=friend, device_id_type=MESH)
    pl.semaphore_wait(barrier, len(friends))


def early_kernel(
    tokens_ref,
    mask_ref,
    embed_ref,
    own_ref,
    bias_ref,
    ow_ref,
    ob_ref,
    q_ref,
    k_ref,
    v_ref,
    ctx_ref,
    lse_ref,
    out_ref,
    x_out,
    w_out,
    w_all,
    b_all,
    send,
    recv,
    local,
):
    step = pl.program_id(0)
    group, row = step // 2, step % 2
    place = Place()
    width = w_all.shape[2]
    heads = width // HEAD_DIM
    half, quarter = width // 2, width // 4

    def half_of(g):
        return w_all.at[g, :, pl.ds(pl.multiple_of(place.c * half, half), half), :]

    def quarter_rows(g):
        side = place.x if g == 1 else place.y
        return pl.ds(pl.multiple_of(place.c * half + side * quarter, quarter), quarter)

    def quarter_of(g):
        return w_all.at[g, :, quarter_rows(g), :]

    load = pltpu.make_async_copy(own_ref, w_all.at[0], local.at[0])

    def direct(g):
        src = own_ref.at[:, quarter_rows(g), :]
        return remote(src, quarter_of(g), send.at[0, g], recv.at[0, g], place.up(g))

    relay = remote(quarter_of(2), quarter_of(3), send.at[0, 3], recv.at[0, 3], place.up(1))

    def beside(g):
        where = place.side("x" if g == 1 else "y")
        return remote(quarter_of(g), quarter_of(g), send.at[3, g], recv.at[3, g], where)

    def cross(g):
        return remote(half_of(g), half_of(g), send.at[1, g], recv.at[1, g], place.core())

    def bias(g):
        return remote(bias_ref, b_all.at[g], send.at[2, g], recv.at[2, g], place.up(g))

    def store(g):
        return pltpu.make_async_copy(w_all.at[g], w_out.at[g], local.at[2 + g])

    @pl.when(step == 0)
    def _():
        greet(
            [place.core(), place.side("x"), place.side("y")] + [place.up(o) for o in range(1, 4)]
        )
        direct(1).start()
        direct(2).start()
        load.start()
        bias_load = pltpu.make_async_copy(bias_ref, b_all.at[0], local.at[1])
        bias_load.start()
        for g in range(1, 4):
            bias(g).start()
        load.wait()
        bias_load.wait()
        store(0).start()

    for g in range(1, 4):

        @pl.when(step == 2 * g)
        def _():
            cross(g).wait()
            bias(g).wait()
            store(g).start()

    x = jnp.where(mask_ref[...] == 1.0, embed_ref[...].astype(F32), tokens_ref[...].astype(F32))
    x = x.astype(BF)

    @pl.when(step < 2)
    def _():
        x_out[...] = x

    q = (dot_nt(x, w_all[group, 0]) + b_all[group, 0:1, :]).astype(BF)
    k = dot_nt(x, w_all[group, 1]).astype(BF)
    v = (dot_nt(x, w_all[group, 2]) + b_all[group, 1:2, :]).astype(BF)
    q_ref[0] = q
    k_ref[0] = k
    v_ref[0] = v
    v_t = v.T
    q_scaled = q * jnp.asarray(0.125, BF)
    pieces = []
    for head in range(heads):
        k_head = jnp.where(head_lanes(width, head), k, jnp.zeros_like(k))
        scores = dot_nt(k_head, q_scaled)
        highest = jnp.max(scores, axis=0, keepdims=True)
        exponent = jnp.exp(scores - highest)
        totals = jnp.sum(exponent, axis=0, keepdims=True)
        probs = (exponent * (1.0 / totals)).astype(BF)
        pieces.append(dot_nn(v_t[head * HEAD_DIM : (head + 1) * HEAD_DIM], probs))
        lse_ref[0, 0, head : head + 1, :] = highest + jnp.log(totals)
    ctx = jnp.concatenate(pieces, axis=0).T.astype(BF)
    ctx_ref[0] = ctx
    result = dot_nn(ctx, ow_ref[place.h ^ group])
    spot = pl.ds(pl.multiple_of(row * LEN, LEN), LEN)

    @pl.when(group == 0)
    def _():
        out_ref[spot, :] = result + ob_ref[...]

    @pl.when(group > 0)
    def _():
        out_ref[spot, :] = out_ref[spot, :] + result

    @pl.when(step == 1)
    def _():
        direct(1).wait()
        beside(1).start()
        direct(2).wait()
        relay.start()
        beside(2).start()
        beside(1).wait()
        cross(1).start()

    @pl.when(step == 2)
    def _():
        relay.wait()
        beside(3).start()
        beside(2).wait()
        cross(2).start()

    @pl.when(step == 4)
    def _():
        beside(3).wait()
        cross(3).start()

    @pl.when(step == 7)
    def _():
        for g in range(4):
            store(g).wait()


def early_call(x, mask, embed, own, bias, ow, ob):
    tokens, features = x.shape
    width = own.shape[1]
    groups = features // width
    rows = tokens // LEN
    hbm = pl.BlockSpec(memory_space=pl.ANY)
    per_head = pl.BlockSpec((1, LEN, width), lambda s: (s // 2, s % 2, 0))
    stacked = jax.ShapeDtypeStruct((groups, tokens, width), BF)
    dma = pltpu.SemaphoreType.DMA
    return pl.pallas_call(
        early_kernel,
        grid=(groups * rows,),
        in_specs=[
            pl.BlockSpec((LEN, features), lambda s: (s % 2, 0)),
            pl.BlockSpec((LEN, 1), lambda s: (s % 2, 0)),
            pl.BlockSpec((1, features), lambda s: (0, 0)),
            hbm,
            hbm,
            pl.BlockSpec((groups, width, features), lambda s: (0, 0, 0)),
            pl.BlockSpec((1, features), lambda s: (0, 0)),
        ],
        out_specs=[
            per_head,
            per_head,
            per_head,
            per_head,
            pl.BlockSpec((1, 1, 8, LEN), lambda s: (s // 2, s % 2, 0, 0)),
            pl.BlockSpec((tokens, features), lambda s: (0, 0)),
            pl.BlockSpec((LEN, features), lambda s: (jnp.minimum(s, 1), 0)),
            hbm,
        ],
        out_shape=[
            stacked,
            stacked,
            stacked,
            stacked,
            jax.ShapeDtypeStruct((groups, rows, 8, LEN), F32),
            jax.ShapeDtypeStruct((tokens, features), F32),
            jax.ShapeDtypeStruct((tokens, features), BF),
            jax.ShapeDtypeStruct((groups,) + own.shape, BF),
        ],
        scratch_shapes=[
            pltpu.VMEM((groups,) + own.shape, BF),
            pltpu.VMEM((groups, 8, width), F32),
            dma((4, 4)),
            dma((4, 4)),
            dma((6,)),
        ],
        compiler_params=pltpu.CompilerParams(
            dimension_semantics=("arbitrary",),
            vmem_limit_bytes=56 << 20,
            collective_id=0,
            has_side_effects=True,
        ),
        name="early_kernel",
    )(x, mask, embed, own, bias, ow, ob)


LANES = 384
CHUNK = 1024
PIECE = CHUNK // 64
SPACING = 3
DOWN_EVERY = 1
UP_EVERY = 4
UP_FIRST = 6
BLOCK = 256


def add_into(target, source):
    target[...] = (target[...].astype(F32) + source[...].astype(F32)).astype(BF)


class MatrixSum:
    COPIES = 16

    def __init__(self, place, parts, keep, first, second, third, fourth, full, send, recv, local):
        self.place = place
        self.parts = parts
        self.keep, self.first, self.second = keep, first, second
        self.third, self.fourth, self.full = third, fourth, full
        self.send, self.recv, self.local = send, recv, local

    def copy(self, i, slot, src, dst, where):
        return remote(src, dst, self.send.at[i, slot], self.recv.at[i, slot], where)

    def fetch(self, i, source, index):
        return pltpu.make_async_copy(
            source.at[index, self.place.c], self.keep.at[i], self.local.at[i]
        )

    def copies(self, phase, i, source=None, index=None):
        p = self.place
        keep, full = self.keep, self.full
        both = self.parts == 2
        out = []
        if phase == 1:
            out.append(self.copy(i, 0, source.at[index, 1 - p.c], self.first.at[i], p.core()))
        if phase == 2:
            src = keep.at[i, 0, 1 - p.x]
            out.append(self.copy(i, 1, src, self.second.at[i, 0], p.side("x")))
            if both:
                src = keep.at[i, 1, :, 1 - p.y]
                out.append(self.copy(i, 2, src, self.second.at[i, 1], p.side("y")))
        if phase == 3:
            src = keep.at[i, 0, p.x, 1 - p.y]
            out.append(self.copy(i, 3, src, self.third.at[i, 0], p.side("y")))
            if both:
                src = keep.at[i, 1, 1 - p.x, p.y]
                out.append(self.copy(i, 4, src, self.third.at[i, 1], p.side("x")))
        if phase == 4:
            for o in range(1, 4):
                src = keep.at[i, :, p.x, p.y, p.h ^ o]
                out.append(self.copy(i, 4 + o, src, self.fourth.at[i, o - 1], p.up(o)))
        if phase == 5:
            spot = full.at[i, p.c, :, p.x, p.y, p.h]
            for o in range(1, 4):
                out.append(self.copy(i, 7 + o, spot, spot, p.up(o)))
        if phase == 6:
            spot = full.at[i, p.c, 0, p.x, p.y]
            out.append(self.copy(i, 11, spot, spot, p.side("y")))
            if both:
                spot = full.at[i, p.c, 1, p.x, p.y]
                out.append(self.copy(i, 12, spot, spot, p.side("x")))
        if phase == 7:
            spot = full.at[i, p.c, 0, p.x]
            out.append(self.copy(i, 13, spot, spot, p.side("x")))
            if both:
                spot = full.at[i, p.c, 1, :, p.y]
                out.append(self.copy(i, 14, spot, spot, p.side("y")))
        if phase == 8:
            spot = full.at[i, p.c]
            out.append(self.copy(i, 15, spot, spot, p.core()))
        return out

    def begin(self, i, source, index):
        self.fetch(i, source, index).start()
        for one in self.copies(1, i, source, index):
            one.start()

    def advance(self, phase, i, source=None, index=None):
        p = self.place
        if phase == 2:
            self.fetch(i, source, index).wait()
        for one in self.copies(phase - 1, i, source, index):
            one.wait()
        if phase == 2:
            add_into(self.keep.at[i], self.first.at[i])
        if phase == 3:
            add_into(self.keep.at[i, 0, p.x], self.second.at[i, 0])
            if self.parts == 2:
                add_into(self.keep.at[i, 1, :, p.y], self.second.at[i, 1])
        if phase == 4:
            for part in range(self.parts):
                add_into(self.keep.at[i, part, p.x, p.y], self.third.at[i, part])
        if phase == 5:
            total = self.keep[i, :, p.x, p.y, p.h].astype(F32)
            for o in range(3):
                total = total + self.fourth[i, o].astype(F32)
            self.full[i, p.c, :, p.x, p.y, p.h] = total.astype(BF)
        if phase <= 8:
            for one in self.copies(phase, i):
                one.start()


class GroupSum:
    COPIES = 11

    def __init__(self, place, own, first, second, third, fourth, full, send, recv):
        self.place = place
        self.own, self.first, self.second = own, first, second
        self.third, self.fourth, self.full = third, fourth, full
        self.send, self.recv = send, recv

    def copy(self, g, slot, src, dst, where):
        return remote(src, dst, self.send.at[g, slot], self.recv.at[g, slot], where)

    def copies(self, phase, g):
        p, own, full = self.place, self.own, self.full
        x, y = p.side("x"), p.side("y")
        if phase == 1:
            return [self.copy(g, 0, own.at[g, 1 - p.c], self.first.at[g], p.core())]
        if phase == 2:
            return [
                self.copy(g, 1, own.at[g, p.c, 0, 1 - p.x], self.second.at[g, 0], x),
                self.copy(g, 2, own.at[g, p.c, 1, :, 1 - p.y], self.second.at[g, 1], y),
            ]
        if phase == 3:
            return [
                self.copy(g, 3, own.at[g, p.c, 0, p.x, 1 - p.y], self.third.at[g, 0], y),
                self.copy(g, 4, own.at[g, p.c, 1, 1 - p.x, p.y], self.third.at[g, 1], x),
            ]
        if phase == 4 and g > 0:
            return [
                self.copy(g, 5, own.at[g, p.c, :, p.x, p.y], self.fourth.at[g - 1], p.up(g))
            ]
        if phase == 6:
            spots = full.at[p.c, 0, p.x, p.y], full.at[p.c, 1, p.x, p.y]
            return [self.copy(0, 6, spots[0], spots[0], y), self.copy(0, 7, spots[1], spots[1], x)]
        if phase == 7:
            spots = full.at[p.c, 0, p.x], full.at[p.c, 1, :, p.y]
            return [self.copy(0, 8, spots[0], spots[0], x), self.copy(0, 9, spots[1], spots[1], y)]
        if phase == 8:
            spot = full.at[p.c]
            return [self.copy(0, 10, spot, spot, p.core())]
        return []

    def begin(self, g):
        for one in self.copies(1, g):
            one.start()

    def advance(self, phase, g):
        p, own = self.place, self.own
        if phase == 6:
            for group in range(own.shape[0]):
                for one in self.copies(4, group):
                    one.wait()
            total = own[0, p.c, :, p.x, p.y].astype(F32)
            for o in range(3):
                total = total + self.fourth[o].astype(F32)
            self.full[p.c, :, p.x, p.y] = total.astype(BF)
        else:
            for one in self.copies(phase - 1, g):
                one.wait()
        if phase == 2:
            add_into(own.at[g, p.c], self.first.at[g])
        if phase == 3:
            add_into(own.at[g, p.c, 0, p.x], self.second.at[g, 0])
            add_into(own.at[g, p.c, 1, :, p.y], self.second.at[g, 1])
        if phase == 4:
            add_into(own.at[g, p.c, 0, p.x, p.y], self.third.at[g, 0])
            add_into(own.at[g, p.c, 1, p.x, p.y], self.third.at[g, 1])
        for one in self.copies(phase, g):
            one.start()


class Stages:
    def __init__(self, tokens, ff, count, heads):
        rows = tokens // LEN
        self.blocks = ff // BLOCK
        self.norms = self.blocks + tokens // BLOCK
        self.outer = self.norms + count
        self.per_group = 2 * rows
        self.end = self.outer + count * self.per_group
        self.half = ff // CHUNK
        self.outw_first = self.outer + 1


def late_kernel(
    plan,
    gf_ref,
    nl_hbm,
    slope_ref,
    dw_ref,
    uw_ref,
    xh_ref,
    inv_ref,
    gs_ref,
    gain_ref,
    x_hbm,
    w_ref,
    ow_ref,
    ctx_ref,
    q_ref,
    k_ref,
    v_ref,
    lse_ref,
    mask_ref,
    early_0,
    early_1,
    early_2,
    early_squares,
    down_ref,
    vec_ref,
    dx_out,
    wg_out,
    down_out,
    up_out,
    outw_out,
    up_ref,
    outw_ref,
    dx,
    rows_ref,
    ga_all,
    dpre,
    stage_w,
    stage_o,
    wg_acc,
    dctx,
    k_t,
    dq_t,
    dk_acc,
    dv_acc,
    stage_up,
    vec,
    vec_in,
    ff_keep,
    ff_1,
    ff_2,
    ff_3,
    ff_4,
    ff_full,
    ow_keep,
    ow_1,
    ow_2,
    ow_3,
    ow_4,
    ow_full,
    qk_own,
    qk_1,
    qk_2,
    qk_3,
    qk_4,
    qk_full,
    ff_send,
    ff_recv,
    ff_local,
    ow_send,
    ow_recv,
    ow_local,
    qk_send,
    qk_recv,
    vec_send,
    vec_recv,
    store_sem,
    block_sem,
    outer_sem,
    last_sem,
    rows_sem,
):
    step = pl.program_id(0)
    place = Place()
    half = plan.half
    chunks = 2 * half
    count = qk_own.shape[0]
    width = q_ref.shape[2]
    heads = width // HEAD_DIM
    feed = MatrixSum(
        place, 2, ff_keep, ff_1, ff_2, ff_3, ff_4, ff_full, ff_send, ff_recv, ff_local
    )
    outer = MatrixSum(
        place, 1, ow_keep, ow_1, ow_2, ow_3, ow_4, ow_full, ow_send, ow_recv, ow_local
    )
    groups = GroupSum(place, qk_own, qk_1, qk_2, qk_3, qk_4, qk_full, qk_send, qk_recv)
    tail = plan.end
    end = max(
        tail + 8,
        plan.outw_first + 8 * SPACING + 1,
        UP_FIRST + UP_EVERY * (half - 1) + 8 * SPACING + 1,
    )

    nl_load = pltpu.make_async_copy(nl_hbm, rows_ref, rows_sem.at[0])
    x_load = pltpu.make_async_copy(x_hbm, rows_ref, rows_sem.at[1])

    @pl.when(step == 0)
    def _():
        nl_load.start()
        greet(
            [place.core(), place.side("x"), place.side("y")] + [place.up(o) for o in range(1, 4)]
        )
        nl_load.wait()
        vec[...] = jnp.zeros_like(vec)
        for index, ref in enumerate((early_0, early_1, early_2)):
            vec[0, index : index + 1, :] = ref[...]
        vec[0, 10:11, :] = early_squares[...]

    def down_store(i):
        return pltpu.make_async_copy(ff_full.at[i], down_out.at[i], store_sem.at[i, 0])

    def up_store(i, part):
        spot = pl.ds(pl.multiple_of((2 * i + part) * (CHUNK // 2), CHUNK // 2), CHUNK // 2)
        return pltpu.make_async_copy(stage_up, up_out.at[:, spot], store_sem.at[half + i, part])

    def outw_store():
        return pltpu.make_async_copy(ow_full.at[0], outw_out.at[0], store_sem.at[chunks, 0])

    def tick(t, start, stop):
        span = 8 * SPACING

        def window(first, last, run):
            if start <= last and stop > first:

                @pl.when((t >= first) & (t <= last))
                def _():
                    run()

        def each(first, every, number, run):
            for phase in range(9, 0, -1):
                behind = SPACING * (phase - 1)
                if stop - behind <= first or start - behind > first + every * (number - 1):
                    continue
                at = t - behind - first
                index = at // every

                @pl.when((at >= 0) & (index < number) & (at % every == 0))
                def _():
                    run(phase, index)

        def down_step(phase, i):
            if phase == 1:
                feed.begin(i, down_ref, i)
                return
            feed.advance(phase, i, down_ref, i)
            if phase == 9:
                down_store(i).start()

        def up_step(phase, i):
            if phase == 1:
                feed.begin(half + i, up_ref, i)
                return
            feed.advance(phase, half + i, up_ref, i)
            if phase == 9:

                @pl.when(i > 0)
                def _():
                    up_store(i - 1, 1).wait()

                for c in range(2):
                    if c == 1:
                        up_store(i, 0).wait()
                    block = ff_full[half + i, c].reshape(CHUNK // 2, 2 * LANES)
                    stage_up[...] = block.T
                    up_store(i, c).start()

        def outw_step(phase, i):
            if phase == 1:
                outer.begin(0, outw_ref, 0)
                return
            outer.advance(phase, 0, outw_ref, 0)
            if phase == 9:
                outw_store().start()

        def group_steps():
            for g in range(count):
                base = plan.outer + plan.per_group * (g + 1)
                if base < start or base >= stop:
                    continue
                phases = (9, 8, 7, 6, 4, 3, 2) if g == count - 1 else (4, 3, 2)
                for phase in phases:
                    when = phase - 1 if phase < 5 else phase - 2

                    @pl.when(t == base + when)
                    def _():
                        groups.advance(phase, g)

                @pl.when(t == base)
                def _():
                    groups.begin(g)

        first, last = 0, DOWN_EVERY * (half - 1) + span
        window(first, last, lambda: each(0, DOWN_EVERY, half, down_step))
        first, last = UP_FIRST, UP_FIRST + UP_EVERY * (half - 1) + span
        window(first, last, lambda: each(UP_FIRST, UP_EVERY, half, up_step))
        first, last = plan.outw_first, plan.outw_first + span
        window(first, last, lambda: each(plan.outw_first, 1, 1, outw_step))
        window(plan.outer + plan.per_group, tail + 8, group_steps)

    tick(step, 0, tail)


    def block_copy(b):
        per_chunk = CHUNK // BLOCK
        spot = up_ref.at[b // per_chunk, (b % per_chunk) // 2, b % 2]
        return pltpu.make_async_copy(stage_w.at[b % 2], spot, block_sem.at[b])

    @pl.when(step < plan.blocks)
    def _():
        grad = dot_nt(gf_ref[...], dw_ref[...]) * slope_ref[...]
        dpre[...] = grad.astype(BF)

        @pl.when(step > 1)
        def _():
            block_copy(step - 2).wait()

        part = dot_tn(dpre[...], rows_ref[...]).astype(BF)
        stage_w[step % 2] = part.reshape(stage_w.shape[1:])
        block_copy(step).start()
        per_row = rows_ref.shape[1] // BLOCK
        spot = pl.ds(pl.multiple_of((step % per_row) * BLOCK, BLOCK), BLOCK)
        vec[0, pl.ds(6 + step // per_row, 1), spot] = jnp.sum(
            dpre[...].astype(F32), axis=0, keepdims=True
        )
        for r in range(0, dx.shape[0], BLOCK):
            part = dot_nt(dpre[r : r + BLOCK], uw_ref[...])

            @pl.when(step == 0)
            def _():
                dx[r : r + BLOCK] = part

            @pl.when(step > 0)
            def _():
                dx[r : r + BLOCK] = dx[r : r + BLOCK] + part


    @pl.when((step >= plan.blocks) & (step < plan.norms))
    def _():
        @pl.when(step == plan.blocks)
        def _():
            block_copy(plan.blocks - 2).wait()
            block_copy(plan.blocks - 1).wait()
            x_load.start()

        rows = pl.ds(pl.multiple_of((step - plan.blocks) * BLOCK, BLOCK), BLOCK)
        upstream = dx[rows, :] + gs_ref[...]
        normal = xh_ref[...]
        scaled = upstream * gain_ref[...]
        mean = jnp.mean(scaled, axis=1, keepdims=True)
        along = jnp.mean(scaled * normal, axis=1, keepdims=True)
        hidden = inv_ref[...] * (scaled - mean - normal * along)
        low = hidden.astype(BF)
        dx[rows, :] = hidden
        ga_all[rows, :] = low
        vec[0, 3:4, :] += jnp.sum(upstream * normal, axis=0, keepdims=True)
        vec[0, 4:5, :] += jnp.sum(upstream, axis=0, keepdims=True)
        vec[0, 5:6, :] += jnp.sum(low.astype(F32), axis=0, keepdims=True)


    def outer_copy(g):
        spot = place.h ^ g
        return pltpu.make_async_copy(
            stage_o, outw_ref.at[0, spot >> 1, 0, spot & 1], outer_sem.at[g]
        )

    @pl.when((step >= plan.norms) & (step < plan.outer))
    def _():
        g = step - plan.norms

        @pl.when(g > 0)
        def _():
            outer_copy(g - 1).wait()

        part = dot_tn(ctx_ref[0], ga_all[...])
        stage_o[...] = part.astype(BF).reshape(stage_o.shape)
        outer_copy(g).start()

    @pl.when(step == plan.outer)
    def _():
        outer_copy(count - 1).wait()
        x_load.wait()


    def dx_copy(r):
        spot = pl.ds(pl.multiple_of(r * LEN, LEN), LEN)
        return pltpu.make_async_copy(dx.at[spot], dx_out.at[spot], last_sem.at[r])

    @pl.when(step >= plan.outer)
    def _():
        at = step - plan.outer
        part = at % 2
        row = (at // 2) % 2
        group = at // plan.per_group
        mine = pl.ds(pl.multiple_of(row * LEN, LEN), LEN)
        q = q_ref[0]
        k = k_ref[0]
        v = v_ref[0]

        @pl.when(part == 0)
        def _():
            dctx[...] = dot_nt(ga_all[mine, :], ow_ref[place.h ^ group]).astype(BF)
            k_t[...] = k.T

        q_scaled = q * jnp.asarray(0.125, BF)

        def one_head(head, carry):
            mask = head_lanes(width, head)
            spot = pl.ds(pl.multiple_of(head * HEAD_DIM, HEAD_DIM), HEAD_DIM)
            scores = dot_nt(jnp.where(mask, k, jnp.zeros_like(k)), q_scaled)
            probs = jnp.exp(scores - lse_ref[0, 0, pl.ds(head, 1), :])
            dprobs = dot_nt(jnp.where(mask, v, jnp.zeros_like(v)), dctx[...])
            delta = jnp.sum(probs * dprobs, axis=0, keepdims=True)
            dscores = (probs * (dprobs - delta)).astype(BF)
            dv_acc[...] = jnp.where(mask, dot_nn(probs.astype(BF), dctx[...]), dv_acc[...])
            dk_acc[...] = jnp.where(mask, dot_nn(dscores, q_scaled), dk_acc[...])
            dq_t[spot, :] = dot_nn(k_t[spot, :], dscores)
            return carry

        split = heads // 2 + 1
        lax.fori_loop(part * split, split + part * (heads - split), one_head, 0)

        @pl.when(part == 1)
        def _():
            x = rows_ref[mine, :]
            dq = (dq_t[...] * 0.125).T.astype(BF)
            dk = dk_acc[...].astype(BF)
            dv = dv_acc[...].astype(BF)
            delta = dot_nn(dq, w_ref[0, 0]) + dot_nn(dk, w_ref[0, 1]) + dot_nn(dv, w_ref[0, 2])
            dx[mine, :] = dx[mine, :] + delta

            @pl.when(row == 0)
            def _():
                wg_acc[...] = jnp.zeros_like(wg_acc)

            for index, grad in enumerate((dq, dk, dv)):
                wg_acc[index * width : (index + 1) * width] += dot_tn(grad, x)
            spot = place.h ^ group
            vec[0, pl.ds(16 + spot, 1), 0:width] += jnp.sum(
                dq.astype(F32), axis=0, keepdims=True
            )
            vec[0, pl.ds(20 + spot, 1), 0:width] += jnp.sum(
                dv.astype(F32), axis=0, keepdims=True
            )

            @pl.when(row == 1)
            def _():
                shape = qk_own.shape[2:]
                for zl in range(2):
                    block = wg_acc[:, zl * LANES : (zl + 1) * LANES].astype(BF)
                    qk_own[group, zl] = block.reshape(shape)

            @pl.when(group == count - 1)
            def _():
                total = jnp.where(mask_ref[...] == 1.0, dx[mine, :], 0.0)
                vec[0, 15:16, :] += jnp.sum(total, axis=0, keepdims=True)
                dx_copy(row).start()

    @pl.when(step == plan.end - 1)
    def _():
        def vec_copy(k):
            if k < 3:
                where = (place.dp ^ (1 << k), place.h)
            else:
                where = (place.dp, place.h ^ (1 << (k - 3)))
            return remote(vec.at[k], vec_in.at[k], vec_send.at[k], vec_recv.at[k], where)

        @pl.loop(tail, end)
        def _(t):
            tick(t, tail, end)
            for k in range(6):

                @pl.when(t == tail + k)
                def _():
                    if k > 0:
                        vec_copy(k - 1).wait()
                        vec[k] = vec[k - 1] + vec_in[k - 1]
                    if k < 5:
                        vec_copy(k).start()

        vec_ref[...] = vec[5]
        for c in range(2):
            block = qk_full[c].reshape(wg_acc.shape[0], LANES)
            wg_acc[:, c * LANES : (c + 1) * LANES] = block.astype(F32)
        wg_copy = pltpu.make_async_copy(wg_acc, wg_out, last_sem.at[2])
        wg_copy.start()
        for i in range(half):
            down_store(i).wait()
        up_store(half - 1, 1).wait()
        outw_store().wait()
        for r in range(2):
            dx_copy(r).wait()
        wg_copy.wait()


def late_call(
    gf, nl, slope, dw, uw, xh, inv, gs, gain, x, w, ow, ctx, q, k, v, lse, mask, early, down
):
    tokens, features = x.shape
    count, _, width, _ = w.shape
    ff = down.shape[0]
    heads = width // HEAD_DIM
    plan = Stages(tokens, ff, count, heads)
    chunks = 2 * plan.half
    chunked = (plan.half, 2, 2, 2, 2, 4, PIECE, features)
    squared = (1, 2, 1, 2, 2, 4, features // 32, features)
    hbm = pl.BlockSpec(memory_space=pl.ANY)
    once = pl.Buffered(1)

    def whole(shape):
        return pl.BlockSpec(shape, lambda s: (0,) * len(shape), pipeline_mode=once)

    def block_at(s):
        return jnp.minimum(s, plan.blocks - 1)

    def norm_at(s):
        return jnp.clip(s - plan.blocks, 0, tokens // BLOCK - 1)

    def head_at(s):
        at = jnp.clip(s - plan.outer, 0, plan.end - plan.outer - 1)
        return at // plan.per_group, (at // 2) % 2

    def per_head(s):
        group, row = head_at(s)
        return group, row, 0

    in_specs = [
        whole(gf.shape),
        hbm,
        pl.BlockSpec((tokens, BLOCK), lambda s: (0, block_at(s))),
        pl.BlockSpec((BLOCK, features), lambda s: (block_at(s), 0)),
        pl.BlockSpec((features, BLOCK), lambda s: (0, block_at(s))),
        pl.BlockSpec((BLOCK, features), lambda s: (norm_at(s), 0)),
        pl.BlockSpec((BLOCK, 1), lambda s: (norm_at(s), 0), pipeline_mode=once),
        pl.BlockSpec((BLOCK, features), lambda s: (norm_at(s), 0)),
        whole(gain.shape),
        hbm,
        pl.BlockSpec((1, 3, width, features), lambda s: (head_at(s)[0], 0, 0, 0)),
        whole(ow.shape),
        pl.BlockSpec(
            (1, tokens, width),
            lambda s: (jnp.clip(s - plan.norms, 0, count - 1), 0, 0),
            pipeline_mode=once,
        ),
        pl.BlockSpec((1, LEN, width), per_head),
        pl.BlockSpec((1, LEN, width), per_head),
        pl.BlockSpec((1, LEN, width), per_head),
        pl.BlockSpec((1, 1, 8, LEN), lambda s: head_at(s) + (0, 0)),
        pl.BlockSpec((LEN, 1), lambda s: (head_at(s)[1], 0)),
    ]
    in_specs += [whole(one.shape) for one in early]
    in_specs += [hbm]
    out_specs = [pl.BlockSpec((24, features), lambda s: (0, 0))] + [hbm] * 7
    out_shape = [
        jax.ShapeDtypeStruct((24, features), F32),
        jax.ShapeDtypeStruct((tokens, features), F32),
        jax.ShapeDtypeStruct((3 * width, features), F32),
        jax.ShapeDtypeStruct(chunked, BF),
        jax.ShapeDtypeStruct((features, ff), BF),
        jax.ShapeDtypeStruct(squared, BF),
        jax.ShapeDtypeStruct(chunked, BF),
        jax.ShapeDtypeStruct(squared, BF),
    ]

    def sum_buffers(n, parts, rows):
        block = (rows, features)
        return [
            pltpu.VMEM((n, parts, 2, 2, 4) + block, BF),
            pltpu.VMEM((n, parts, 2, 2, 4) + block, BF),
            pltpu.VMEM((n, parts, 2, 4) + block, BF),
            pltpu.VMEM((n, parts, 4) + block, BF),
            pltpu.VMEM((n, 3, parts) + block, BF),
            pltpu.VMEM((n, 2, parts, 2, 2, 4) + block, BF),
        ]

    qrows = 3 * width // 8
    quarter = (2, 2, 2, qrows, LANES)
    scratch = [
        pltpu.VMEM((tokens, features), F32),
        pltpu.VMEM((tokens, features), BF),
        pltpu.VMEM((tokens, features), BF),
        pltpu.VMEM((tokens, BLOCK), BF),
        pltpu.VMEM((2, 2, 2, 4, PIECE, features), BF),
        pltpu.VMEM((2, 4, width // 8, features), BF),
        pltpu.VMEM((3 * width, features), F32),
        pltpu.VMEM((LEN, width), BF),
        pltpu.VMEM((width, LEN), BF),
        pltpu.VMEM((width, LEN), F32),
        pltpu.VMEM((LEN, width), F32),
        pltpu.VMEM((LEN, width), F32),
        pltpu.VMEM((features, CHUNK // 2), BF),
        pltpu.VMEM((6, 24, features), F32),
        pltpu.VMEM((5, 24, features), F32),
    ]
    scratch += sum_buffers(chunks, 2, PIECE)
    scratch += sum_buffers(1, 1, features // 32)
    scratch += [
        pltpu.VMEM((count, 2) + quarter, BF),
        pltpu.VMEM((count,) + quarter, BF),
        pltpu.VMEM((count, 2, 2, qrows, LANES), BF),
        pltpu.VMEM((count, 2, qrows, LANES), BF),
        pltpu.VMEM((3, 2, qrows, LANES), BF),
        pltpu.VMEM((2,) + quarter, BF),
    ]
    dma = pltpu.SemaphoreType.DMA
    scratch += [
        dma((chunks, MatrixSum.COPIES)),
        dma((chunks, MatrixSum.COPIES)),
        dma((chunks,)),
        dma((1, MatrixSum.COPIES)),
        dma((1, MatrixSum.COPIES)),
        dma((1,)),
        dma((count, GroupSum.COPIES)),
        dma((count, GroupSum.COPIES)),
        dma((5,)),
        dma((5,)),
        dma((chunks + 1, 2)),
        dma((plan.blocks,)),
        dma((count,)),
        dma((3,)),
        dma((2,)),
    ]
    results = pl.pallas_call(
        functools.partial(late_kernel, plan),
        grid=(plan.end,),
        in_specs=in_specs,
        out_specs=out_specs,
        out_shape=out_shape,
        scratch_shapes=scratch,
        compiler_params=pltpu.CompilerParams(
            dimension_semantics=("arbitrary",),
            vmem_limit_bytes=67043328,
            collective_id=1,
            has_side_effects=True,
        ),
        name="late_kernel",
    )(
        gf,
        nl,
        slope,
        dw,
        uw,
        xh,
        inv,
        gs,
        gain,
        x,
        w,
        ow,
        ctx,
        q,
        k,
        v,
        lse,
        mask,
        *early,
        down.reshape(chunked),
    )
    sums, dx, wg, down_sum, up_sum, outw_sum = results[:6]
    return (
        dx,
        wg,
        sums,
        down_sum.reshape(ff, features),
        up_sum,
        outw_sum.reshape(features, features),
    )


def swap(value, axis, mask, size):
    return lax.ppermute(value, axis, [(i, i ^ mask) for i in range(size)])


def bit_of(axis, bit):
    return (lax.axis_index(axis) >> bit) & 1


def joined(mine, other, upper, dim, kind=None):
    low = jnp.where(upper == 1, other, mine)
    high = jnp.where(upper == 1, mine, other)
    if kind is not None:
        low, high = low.astype(kind), high.astype(kind)
    return jnp.concatenate([low, high], axis=dim)


def halve(value, bit, size, dim):
    half = value.shape[dim] // 2
    mine = bit_of("dp", bit)
    sent = lax.dynamic_slice_in_dim(value, (1 - mine) * half, half, dim)
    kept = lax.dynamic_slice_in_dim(value, mine * half, half, dim)
    received = swap(sent, "dp", 1 << bit, size)
    return (kept.astype(F32) + received.astype(F32)).astype(BF)


def double(value, bit, size, dim, kind=None):
    return joined(value, swap(value, "dp", 1 << bit, size), bit_of("dp", bit), dim, kind)


def plane_orders(size):
    bits = size.bit_length() - 1
    rest = list(range(1, bits))
    return rest, rest[::-1]


def reduce_plane(value, size, dim):
    value = halve(value, 0, size, dim)
    half = value.shape[dim] // 2
    parts = []
    for index, order in enumerate(plane_orders(size)):
        part = lax.slice_in_dim(value, index * half, (index + 1) * half, axis=dim)
        for bit in order:
            part = halve(part, bit, size, dim)
        parts.append(part)
    return parts


def gather_plane(parts, size, dim, kind=None):
    done = []
    for part, order in zip(parts, plane_orders(size)):
        for bit in order[::-1]:
            part = double(part, bit, size, dim)
        done.append(part)
    return double(jnp.concatenate(done, axis=dim), 0, size, dim, kind)


def reduce_head(pieces, size):
    total = pieces[0].astype(F32)
    for offset in range(1, size):
        total = total + swap(pieces[offset], "head", offset, size).astype(F32)
    return total


def gather_head(piece, size):
    return [piece] + [swap(piece, "head", offset, size) for offset in range(1, size)]


def absolute(pieces, dim):
    count = len(pieces)
    bit = 0
    while (1 << bit) < count:
        upper = bit_of("head", bit)
        step = 1 << bit
        pieces = [
            jnp.where(upper == 1, pieces[index ^ step], pieces[index]) for index in range(count)
        ]
        bit += 1
    return jnp.concatenate(pieces, axis=dim)


def own_pieces(value, size, dim):
    width = value.shape[dim] // size
    me = lax.axis_index("head")
    return [
        lax.dynamic_slice_in_dim(value, (me ^ offset) * width, width, dim)
        for offset in range(size)
    ]


def all_reduce_matrix(value, dp, head, head_dim):
    parts = []
    for part in reduce_plane(value, dp, 0):
        piece = reduce_head(own_pieces(part, head, head_dim), head).astype(BF)
        parts.append(absolute(gather_head(piece, head), head_dim))
    return gather_plane(parts, dp, 0, F32)


def all_reduce_small(vector, dp, head):
    bit = 1
    while bit < dp:
        vector = vector + swap(vector, "dp", bit, dp)
        bit *= 2
    bit = 1
    while bit < head:
        vector = vector + swap(vector, "head", bit, head)
        bit *= 2
    return vector


def norm_forward(hidden, gain, bias):
    center = hidden - jnp.mean(hidden, axis=-1, keepdims=True)
    inverse = lax.rsqrt(jnp.mean(center * center, axis=-1, keepdims=True) + EPS)
    normal = center * inverse
    return (normal * gain + bias, normal, inverse)


def norm_backward(upstream, normal, inverse, gain):
    gain_grad = jnp.sum(upstream * normal, axis=0)
    bias_grad = jnp.sum(upstream, axis=0)
    scaled = upstream * gain
    hidden_grad = inverse * (
        scaled
        - jnp.mean(scaled, axis=-1, keepdims=True)
        - normal * jnp.mean(scaled * normal, axis=-1, keepdims=True)
    )
    return (hidden_grad, gain_grad, bias_grad)


def phi(values):
    return 0.5 * (1.0 + jax.scipy.special.erf(values * (1.0 / math.sqrt(2.0))))


def body(
    dp,
    head,
    tokens,
    span_mask,
    valid_mask,
    mask_embedding,
    qkv_weight,
    query_bias,
    value_bias,
    out_weight,
    out_bias,
    norm1_gain,
    norm1_bias,
    up_weight,
    up_bias,
    down_weight,
    down_bias,
    norm2_gain,
    norm2_bias,
    out_grad,
):
    features = tokens.shape[1]
    width = qkv_weight.shape[2]
    masked = (span_mask == 1)[:, None]
    validity = valid_mask.astype(F32)[:, None]
    direct = dp == 8 and head == 4 and features == 2 * LANES and tokens.shape[0] == 2 * LEN
    if direct:
        mask_column = (span_mask == 1).astype(F32)[:, None]
        bias_block = jnp.pad(jnp.stack([query_bias, value_bias]).astype(F32), ((0, 6), (0, 0)))
        out_parts = out_weight.reshape(head, width, features)
        q, k, v, ctx, lse, attended, inputs, weights = early_call(
            tokens,
            mask_column,
            mask_embedding[None, :],
            jnp.transpose(qkv_weight, (1, 2, 0)),
            bias_block,
            out_parts,
            out_bias[None, :],
        )
    else:
        inputs = jnp.where(masked, mask_embedding[None, :], tokens)
        own = jnp.transpose(qkv_weight, (1, 0, 2))
        core = bit_of("dp", 0)
        half = lax.dynamic_slice_in_dim(own, core * (features // 2), features // 2, 1)
        halves = [half]
        for bit in range(head.bit_length() - 1):
            halves = halves + [swap(part, "head", 1 << bit, head) for part in halves]
        weights = [own] + [double(part, 0, dp, 1) for part in halves[1:]]
        biases = jnp.stack([query_bias, value_bias]).astype(F32)
        bias_parts = [biases]
        for bit in range(head.bit_length() - 1):
            bias_parts = bias_parts + [swap(part, "head", 1 << bit, head) for part in bias_parts]
        out_parts = own_pieces(out_weight, head, 0)

        attended = jnp.broadcast_to(out_bias[None, :], tokens.shape)
        saved = []
        for group in range(head):
            q, k, v, ctx, lse, attended = attention_forward(
                inputs,
                weights[group],
                bias_parts[group][0:1],
                bias_parts[group][1:2],
                out_parts[group],
                attended,
            )
            saved.append((q, k, v, ctx, lse))

    inputs_wide = inputs.astype(F32)
    normed, normal_first, inverse_first = norm_forward(
        inputs_wide + attended, norm1_gain, norm1_bias
    )
    normed_low = normed.astype(BF)
    preact = dot_nn(normed_low, up_weight) + up_bias
    share = phi(preact)
    activated = (preact * share).astype(BF)
    slope = share + preact * jnp.exp(-0.5 * preact * preact) * (1.0 / math.sqrt(2.0 * math.pi))
    feedout = dot_nn(activated, down_weight) + down_bias
    result, normal_second, inverse_second = norm_forward(normed + feedout, norm2_gain, norm2_bias)
    grad_output = out_grad.astype(F32) * validity
    grad_second, gain_second_grad, bias_second_grad = norm_backward(
        grad_output, normal_second, inverse_second, norm2_gain
    )
    grad_feed = grad_second.astype(BF)
    down_bias_grad = jnp.sum(grad_feed, axis=0, dtype=F32)
    down_local = dot_tn(activated, grad_feed).astype(BF)
    squares = jnp.stack(
        [
            jnp.sum(validity * inputs_wide * inputs_wide),
            jnp.sum(validity * attended * attended),
            jnp.sum(validity * feedout * feedout),
            jnp.sum(validity),
        ]
    )
    if direct:
        vectors = [one[None, :] for one in (down_bias_grad, gain_second_grad, bias_second_grad)]
        vectors.append(jnp.pad(squares, (0, features - 4))[None, :])
        dx, weight_sum, sums, down_sum, up_sum, outw_sum = late_call(
            grad_feed,
            normed_low,
            slope,
            down_weight,
            up_weight,
            normal_first,
            inverse_first,
            grad_second,
            norm1_gain[None, :],
            inputs,
            weights,
            out_parts,
            ctx,
            q,
            k,
            v,
            lse,
            mask_column,
            vectors,
            down_local,
        )
        tokens_grad = jnp.where(masked, 0.0, dx)
        down_weight_grad = down_sum.astype(F32)
        up_weight_grad = up_sum.astype(F32)
        out_weight_grad = outw_sum.astype(F32)
        weight_grad = jnp.transpose(weight_sum.reshape(3, width, features), (2, 0, 1))
        me = lax.axis_index("head")
        first_grad = lax.dynamic_slice(sums, (16 + me, 0), (1, width))[0]
        third_grad = lax.dynamic_slice(sums, (20 + me, 0), (1, width))[0]
        squares = sums[10, :4]
        count = jnp.maximum(squares[3], 1.0)
        stream_rms = jnp.sqrt(squares[:3] / (count * features))
        return (
            result.astype(BF),
            tokens_grad,
            sums[15],
            weight_grad,
            first_grad,
            third_grad,
            out_weight_grad,
            sums[5],
            sums[3],
            sums[4],
            up_weight_grad,
            sums[6:10].reshape(-1),
            down_weight_grad,
            sums[0],
            sums[1],
            sums[2],
            stream_rms,
        )

    grad_preact = (dot_nt(grad_feed, down_weight) * slope).astype(BF)
    up_bias_grad = jnp.sum(grad_preact, axis=0, dtype=F32)
    up_local = dot_tn(normed_low, grad_preact).astype(BF)
    grad_normed = dot_nt(grad_preact, up_weight) + grad_second
    grad_first, gain_first_grad, bias_first_grad = norm_backward(
        grad_normed, normal_first, inverse_first, norm1_gain
    )
    grad_attended = grad_first.astype(BF)
    out_bias_grad = jnp.sum(grad_attended, axis=0, dtype=F32)
    early = [
        down_bias_grad,
        gain_second_grad,
        bias_second_grad,
        gain_first_grad,
        bias_first_grad,
        out_bias_grad,
        up_bias_grad,
        squares,
    ]
    down_weight_grad = all_reduce_matrix(down_local, dp, head, 0)
    up_weight_grad = all_reduce_matrix(up_local, dp, head, 1)
    early_sum = all_reduce_small(jnp.concatenate(early), dp, head)

    grad_inputs = grad_first
    weight_pieces = []
    out_pieces = []
    query_parts = []
    value_parts = []
    for group in range(head):
        q, k, v, ctx, lse = saved[group]
        weight_piece, out_piece, query_part, value_part, grad_inputs = attention_backward(
            inputs,
            weights[group],
            out_parts[group],
            q,
            k,
            v,
            ctx,
            lse,
            grad_attended,
            grad_inputs,
        )
        weight_pieces.append(reduce_plane(weight_piece, dp, 1))
        out_pieces.append(out_piece)
        query_parts.append(query_part[0])
        value_parts.append(value_part[0])

    weight_grad = gather_plane(
        [
            reduce_head([weight_pieces[group][part] for group in range(head)], head).astype(BF)
            for part in range(2)
        ],
        dp,
        1,
        F32,
    )
    weight_grad = jnp.transpose(weight_grad, (1, 0, 2))

    out_reduced = jnp.stack(out_pieces)
    for bit in range(dp.bit_length() - 1):
        out_reduced = halve(out_reduced, bit, dp, 1)
    out_piece = reduce_head([out_reduced[group] for group in range(head)], head).astype(BF)
    for bit in range(dp.bit_length() - 2, -1, -1):
        out_piece = double(out_piece, bit, dp, 0)
    out_weight_grad = absolute(gather_head(out_piece, head), 0).astype(F32)

    tokens_grad = jnp.where(masked, 0.0, grad_inputs)
    embedding_grad = jnp.sum(jnp.where(masked, grad_inputs, 0.0), axis=0)
    late = jnp.concatenate([embedding_grad, absolute(query_parts, 0), absolute(value_parts, 0)])
    late_sum = all_reduce_small(late, dp, head)
    embedding_grad = late_sum[:features]
    me = lax.axis_index("head")
    first_grad = lax.dynamic_slice_in_dim(late_sum, features + me * width, width)
    third_grad = lax.dynamic_slice_in_dim(late_sum, 2 * features + me * width, width)

    pieces = []
    offset = 0
    for part in early:
        pieces.append(lax.slice_in_dim(early_sum, offset, offset + part.shape[0]))
        offset += part.shape[0]
    (
        down_bias_grad,
        gain_second_grad,
        bias_second_grad,
        gain_first_grad,
        bias_first_grad,
        out_bias_grad,
        up_bias_grad,
        squares,
    ) = pieces
    count = jnp.maximum(squares[3], 1.0)
    stream_rms = jnp.sqrt(squares[:3] / (count * features))
    return (
        result.astype(BF),
        tokens_grad,
        embedding_grad,
        weight_grad,
        first_grad,
        third_grad,
        out_weight_grad,
        out_bias_grad,
        gain_first_grad,
        bias_first_grad,
        up_weight_grad,
        up_bias_grad,
        down_weight_grad,
        down_bias_grad,
        gain_second_grad,
        bias_second_grad,
        stream_rms,
    )


def solution(mesh):
    split = P(("dp", "head"), None)
    flat = P(("dp", "head"))
    placed = (split, flat, flat, P(), P(None, None, "head"), P("head"), P("head")) + (P(),) * 10
    placed = placed + (split,)
    outs = (split, split, P(), P(None, None, "head"), P("head"), P("head")) + (P(),) * 11
    return jax.shard_map(
        functools.partial(body, mesh.shape["dp"], mesh.shape["head"]),
        mesh=mesh,
        in_specs=placed,
        out_specs=outs,
        check_vma=False,
    )
```

```python
import functools
import math

import jax
import jax.numpy as jnp
from jax import lax
from jax.experimental import pallas as pl
from jax.experimental.pallas import tpu as pltpu
from jax.sharding import PartitionSpec as P

HEAD_DIM = 64
LEN = 512
EPS = 1e-12
BF = jnp.bfloat16
F32 = jnp.float32


def dot_nn(left, right):
    return lax.dot_general(left, right, (((1,), (0,)), ((), ())), preferred_element_type=F32)


def dot_nt(left, right):
    return lax.dot_general(left, right, (((1,), (1,)), ((), ())), preferred_element_type=F32)


def dot_tn(left, right):
    return lax.dot_general(left, right, (((0,), (0,)), ((), ())), preferred_element_type=F32)


def head_lanes(width, head):
    lanes = lax.broadcasted_iota(jnp.int32, (1, width), 1)
    return (lanes >= head * HEAD_DIM) & (lanes < (head + 1) * HEAD_DIM)


def forward_kernel(
    x_ref, w_ref, qb_ref, vb_ref, ow_ref, acc_ref, q_ref, k_ref, v_ref, ctx_ref, lse_ref, out_ref
):
    x = x_ref[...]
    width = w_ref.shape[2]
    heads = width // HEAD_DIM
    q = (dot_nn(x, w_ref[0]) + qb_ref[...]).astype(BF)
    k = dot_nn(x, w_ref[1]).astype(BF)
    v32 = dot_nn(x, w_ref[2]) + vb_ref[...]
    v = v32.astype(BF)
    q_ref[...] = q
    k_ref[...] = k
    v_ref[...] = v
    v_t = v.T
    q_scaled = q * jnp.asarray(0.125, BF)
    pieces = []
    for head in range(heads):
        k_head = jnp.where(head_lanes(width, head), k, jnp.zeros_like(k))
        scores = dot_nt(k_head, q_scaled)
        highest = jnp.max(scores, axis=0, keepdims=True)
        exponent = jnp.exp(scores - highest)
        totals = jnp.sum(exponent, axis=0, keepdims=True)
        probs = (exponent * (1.0 / totals)).astype(BF)
        pieces.append(dot_nn(v_t[head * HEAD_DIM : (head + 1) * HEAD_DIM], probs))
        lse_ref[0, head : head + 1, :] = highest + jnp.log(totals)
    ctx = jnp.concatenate(pieces, axis=0).T.astype(BF)
    ctx_ref[...] = ctx
    out_ref[...] = acc_ref[...] + dot_nn(ctx, ow_ref[...])


def backward_kernel(
    x_ref,
    w_ref,
    ow_ref,
    q_ref,
    k_ref,
    v_ref,
    ctx_ref,
    lse_ref,
    ga_ref,
    acc_ref,
    wg_ref,
    owg_ref,
    qbg_ref,
    vbg_ref,
    out_ref,
    wg_acc,
    owg_acc,
):
    row = pl.program_id(0)
    last = pl.num_programs(0) - 1
    width = w_ref.shape[2]
    heads = width // HEAD_DIM
    x = x_ref[...]
    ga = ga_ref[...]
    dctx = dot_nt(ga, ow_ref[...]).astype(BF)
    q = q_ref[...]
    k = k_ref[...]
    v = v_ref[...]
    k_t = k.T
    q_scaled = q * jnp.asarray(0.125, BF)
    dq_t = []
    dk = jnp.zeros(q.shape, F32)
    dv = jnp.zeros(q.shape, F32)
    for head in range(heads):
        mask = head_lanes(width, head)
        scores = dot_nt(jnp.where(mask, k, jnp.zeros_like(k)), q_scaled)
        probs = jnp.exp(scores - lse_ref[0, head : head + 1, :])
        dprobs = dot_nt(jnp.where(mask, v, jnp.zeros_like(v)), dctx)
        delta = jnp.sum(probs * dprobs, axis=0, keepdims=True)
        dscores = (probs * (dprobs - delta)).astype(BF)
        dv = jnp.where(mask, dot_nn(probs.astype(BF), dctx), dv)
        dk = jnp.where(mask, dot_nn(dscores, q_scaled), dk)
        dq_t.append(dot_nn(k_t[head * HEAD_DIM : (head + 1) * HEAD_DIM], dscores))
    dq32 = (jnp.concatenate(dq_t, axis=0) * 0.125).T
    dq = dq32.astype(BF)
    dk = dk.astype(BF)
    dv = dv.astype(BF)
    out_ref[...] = (
        acc_ref[...] + dot_nt(dq, w_ref[0]) + dot_nt(dk, w_ref[1]) + dot_nt(dv, w_ref[2])
    )

    @pl.when(row == 0)
    def _():
        wg_acc[...] = jnp.zeros_like(wg_acc)
        owg_acc[...] = jnp.zeros_like(owg_acc)
        qbg_ref[...] = jnp.zeros_like(qbg_ref)
        vbg_ref[...] = jnp.zeros_like(vbg_ref)

    wg_acc[0] += dot_tn(x, dq)
    wg_acc[1] += dot_tn(x, dk)
    wg_acc[2] += dot_tn(x, dv)
    owg_acc[...] += dot_tn(ctx_ref[...], ga)
    qbg_ref[...] += jnp.sum(dq.astype(F32), axis=0, keepdims=True)
    vbg_ref[...] += jnp.sum(dv.astype(F32), axis=0, keepdims=True)

    @pl.when(row == last)
    def _():
        wg_ref[...] = wg_acc[...].astype(BF)
        owg_ref[...] = owg_acc[...].astype(BF)


def by_row(block):
    rank = len(block)
    return pl.BlockSpec(block, lambda r: (r,) + (0,) * (rank - 1))


def fixed(block):
    rank = len(block)
    return pl.BlockSpec(block, lambda r: (0,) * rank)


def attention_forward(x, w, qb, vb, ow, acc):
    tokens, features = x.shape
    width = w.shape[2]
    rows = tokens // LEN
    flops = 2 * tokens * features * width * 4 + 4 * tokens * LEN * width
    return pl.pallas_call(
        forward_kernel,
        grid=(rows,),
        in_specs=[
            by_row((LEN, features)),
            fixed(w.shape),
            fixed((1, width)),
            fixed((1, width)),
            fixed((width, features)),
            by_row((LEN, features)),
        ],
        out_specs=[
            by_row((LEN, width)),
            by_row((LEN, width)),
            by_row((LEN, width)),
            by_row((LEN, width)),
            by_row((1, 8, LEN)),
            by_row((LEN, features)),
        ],
        out_shape=[jax.ShapeDtypeStruct((tokens, width), BF)] * 4
        + [
            jax.ShapeDtypeStruct((rows, 8, LEN), F32),
            jax.ShapeDtypeStruct((tokens, features), F32),
        ],
        compiler_params=pltpu.CompilerParams(
            dimension_semantics=("arbitrary",), vmem_limit_bytes=48 << 20
        ),
        cost_estimate=pl.CostEstimate(
            flops=4 * flops, bytes_accessed=12 << 20, transcendentals=tokens * LEN * 3
        ),
        name="attention_forward",
    )(x, w, qb, vb, ow, acc)


def attention_backward(x, w, ow, q, k, v, ctx, lse, ga, acc):
    tokens, features = x.shape
    width = w.shape[2]
    rows = tokens // LEN
    flops = 2 * tokens * features * width * 8 + 10 * tokens * LEN * width
    return pl.pallas_call(
        backward_kernel,
        grid=(rows,),
        in_specs=[
            by_row((LEN, features)),
            fixed(w.shape),
            fixed((width, features)),
            by_row((LEN, width)),
            by_row((LEN, width)),
            by_row((LEN, width)),
            by_row((LEN, width)),
            by_row((1, 8, LEN)),
            by_row((LEN, features)),
            by_row((LEN, features)),
        ],
        out_specs=[
            fixed(w.shape),
            fixed((width, features)),
            fixed((1, width)),
            fixed((1, width)),
            by_row((LEN, features)),
        ],
        out_shape=[
            jax.ShapeDtypeStruct(w.shape, BF),
            jax.ShapeDtypeStruct((width, features), BF),
            jax.ShapeDtypeStruct((1, width), F32),
            jax.ShapeDtypeStruct((1, width), F32),
            jax.ShapeDtypeStruct((tokens, features), F32),
        ],
        scratch_shapes=[pltpu.VMEM(w.shape, F32), pltpu.VMEM((width, features), F32)],
        compiler_params=pltpu.CompilerParams(
            dimension_semantics=("arbitrary",), vmem_limit_bytes=48 << 20
        ),
        cost_estimate=pl.CostEstimate(
            flops=4 * flops, bytes_accessed=16 << 20, transcendentals=tokens * LEN * 3
        ),
        name="attention_backward",
    )(x, w, ow, q, k, v, ctx, lse, ga, acc)


MESH = pl.DeviceIdType.MESH


class Place:
    def __init__(self):
        self.dp = lax.axis_index("dp")
        self.h = lax.axis_index("head")
        self.c = self.dp & 1
        self.x = (self.dp >> 1) & 1
        self.y = (self.dp >> 2) & 1

    def core(self):
        return (self.dp ^ 1, self.h)

    def side(self, axis):
        return (self.dp ^ (2 if axis == "x" else 4), self.h)

    def up(self, offset):
        return (self.dp, self.h ^ offset)


def remote(src, dst, send, recv, where):
    return pltpu.make_async_remote_copy(
        src_ref=src,
        dst_ref=dst,
        send_sem=send,
        recv_sem=recv,
        device_id=where,
        device_id_type=MESH,
    )


def greet(friends):
    barrier = pltpu.get_barrier_semaphore()
    for friend in friends:
        pl.semaphore_signal(barrier, inc=1, device_id=friend, device_id_type=MESH)
    pl.semaphore_wait(barrier, len(friends))


def early_kernel(
    tokens_ref,
    mask_ref,
    embed_ref,
    own_ref,
    qb_ref,
    vb_ref,
    ow_ref,
    ob_ref,
    q_ref,
    k_ref,
    v_ref,
    ctx_ref,
    lse_ref,
    out_ref,
    x_out,
    w_out,
    w_all,
    b_all,
    send,
    recv,
    local,
):
    step = pl.program_id(0)
    group, row = step // 2, step % 2
    place = Place()
    width = w_all.shape[2]
    heads = width // HEAD_DIM
    half, quarter = width // 2, width // 4

    def half_of(g):
        return w_all.at[g, :, pl.ds(pl.multiple_of(place.c * half, half), half), :]

    def quarter_rows(g):
        side = place.x if g == 1 else place.y
        return pl.ds(pl.multiple_of(place.c * half + side * quarter, quarter), quarter)

    def quarter_of(g):
        return w_all.at[g, :, quarter_rows(g), :]

    load = pltpu.make_async_copy(own_ref, w_all.at[0], local.at[0])

    def direct(g):
        src = own_ref.at[:, quarter_rows(g), :]
        return remote(src, quarter_of(g), send.at[0, g], recv.at[0, g], place.up(g))

    relay = remote(quarter_of(2), quarter_of(3), send.at[0, 3], recv.at[0, 3], place.up(1))

    def beside(g):
        where = place.side("x" if g == 1 else "y")
        return remote(quarter_of(g), quarter_of(g), send.at[3, g], recv.at[3, g], where)

    def cross(g):
        return remote(half_of(g), half_of(g), send.at[1, g], recv.at[1, g], place.core())

    def bias(g):
        return remote(b_all.at[0], b_all.at[g], send.at[2, g], recv.at[2, g], place.up(g))

    def store(g):
        return pltpu.make_async_copy(w_all.at[g], w_out.at[g], local.at[2 + g])

    @pl.when(step == 0)
    def _():
        greet(
            [place.core(), place.side("x"), place.side("y")] + [place.up(o) for o in range(1, 4)]
        )
        direct(1).start()
        direct(2).start()
        load.start()
        b_all[0] = jnp.zeros(b_all.shape[1:], F32)
        b_all[0, 0:1, :] = qb_ref[...].astype(F32).reshape(1, width)
        b_all[0, 1:2, :] = vb_ref[...].astype(F32).reshape(1, width)
        load.wait()
        store(0).start()

    @pl.when(step == 1)
    def _():
        for g in range(1, 4):
            bias(g).start()

    for g in range(1, 4):

        @pl.when(step == 2 * g)
        def _():
            cross(g).wait()
            bias(g).wait()
            store(g).start()

    embed = embed_ref[...].astype(F32).reshape(1, tokens_ref.shape[1])
    x = jnp.where(mask_ref[...] == 1.0, embed, tokens_ref[...].astype(F32))
    x = x.astype(BF)

    @pl.when(step < 2)
    def _():
        x_out[...] = x

    q = (dot_nt(x, w_all[group, 0]) + b_all[group, 0:1, :]).astype(BF)
    k = dot_nt(x, w_all[group, 1]).astype(BF)
    v = (dot_nt(x, w_all[group, 2]) + b_all[group, 1:2, :]).astype(BF)
    q_ref[0] = q
    k_ref[0] = k
    v_ref[0] = v
    v_t = v.T
    q_scaled = q * jnp.asarray(0.125, BF)
    pieces = []
    for head in range(heads):
        k_head = jnp.where(head_lanes(width, head), k, jnp.zeros_like(k))
        scores = dot_nt(k_head, q_scaled)
        highest = jnp.max(scores, axis=0, keepdims=True)
        exponent = jnp.exp(scores - highest)
        totals = jnp.sum(exponent, axis=0, keepdims=True)
        probs = (exponent * (1.0 / totals)).astype(BF)
        pieces.append(dot_nn(v_t[head * HEAD_DIM : (head + 1) * HEAD_DIM], probs))
        lse_ref[0, 0, head : head + 1, :] = highest + jnp.log(totals)
    ctx = jnp.concatenate(pieces, axis=0).T.astype(BF)
    ctx_ref[0] = ctx
    result = dot_nn(ctx, ow_ref[place.h ^ group])
    spot = pl.ds(pl.multiple_of(row * LEN, LEN), LEN)

    @pl.when(group == 0)
    def _():
        out_ref[spot, :] = result + ob_ref[...].reshape(1, result.shape[1])

    @pl.when(group > 0)
    def _():
        out_ref[spot, :] = out_ref[spot, :] + result

    @pl.when(step == 1)
    def _():
        direct(1).wait()
        beside(1).start()
        direct(2).wait()
        relay.start()
        beside(2).start()
        beside(1).wait()
        cross(1).start()

    @pl.when(step == 2)
    def _():
        relay.wait()
        beside(3).start()
        beside(2).wait()
        cross(2).start()

    @pl.when(step == 4)
    def _():
        beside(3).wait()
        cross(3).start()

    @pl.when(step == 7)
    def _():
        for g in range(4):
            store(g).wait()


def early_call(x, mask, embed, own, qb, vb, ow, ob):
    tokens, features = x.shape
    width = own.shape[1]
    groups = features // width
    rows = tokens // LEN
    hbm = pl.BlockSpec(memory_space=pl.ANY)
    per_head = pl.BlockSpec((1, LEN, width), lambda s: (s // 2, s % 2, 0))
    stacked = jax.ShapeDtypeStruct((groups, tokens, width), BF)
    dma = pltpu.SemaphoreType.DMA
    return pl.pallas_call(
        early_kernel,
        grid=(groups * rows,),
        in_specs=[
            pl.BlockSpec((LEN, features), lambda s: (s % 2, 0)),
            pl.BlockSpec((LEN, 1), lambda s: (s % 2, 0)),
            pl.BlockSpec((features,), lambda s: (0,)),
            hbm,
            pl.BlockSpec((width,), lambda s: (0,)),
            pl.BlockSpec((width,), lambda s: (0,)),
            pl.BlockSpec((groups, width, features), lambda s: (0, 0, 0)),
            pl.BlockSpec((features,), lambda s: (0,)),
        ],
        out_specs=[
            per_head,
            per_head,
            per_head,
            per_head,
            pl.BlockSpec((1, 1, 8, LEN), lambda s: (s // 2, s % 2, 0, 0)),
            pl.BlockSpec((tokens, features), lambda s: (0, 0)),
            pl.BlockSpec((LEN, features), lambda s: (jnp.minimum(s, 1), 0)),
            hbm,
        ],
        out_shape=[
            stacked,
            stacked,
            stacked,
            stacked,
            jax.ShapeDtypeStruct((groups, rows, 8, LEN), F32),
            jax.ShapeDtypeStruct((tokens, features), F32),
            jax.ShapeDtypeStruct((tokens, features), BF),
            jax.ShapeDtypeStruct((groups,) + own.shape, BF),
        ],
        scratch_shapes=[
            pltpu.VMEM((groups,) + own.shape, BF),
            pltpu.VMEM((groups, 8, width), F32),
            dma((4, 4)),
            dma((4, 4)),
            dma((6,)),
        ],
        compiler_params=pltpu.CompilerParams(
            dimension_semantics=("arbitrary",),
            vmem_limit_bytes=56 << 20,
            collective_id=0,
            has_side_effects=True,
        ),
        name="early_kernel",
    )(x, mask, embed, own, qb, vb, ow, ob)


LANES = 384
CHUNK = 1024
PIECE = CHUNK // 64
SPACING = 3
DOWN_EVERY = 1
UP_EVERY = 4
UP_FIRST = 6
BLOCK = 256


def add_into(target, source):
    target[...] = (target[...].astype(F32) + source[...].astype(F32)).astype(BF)


class MatrixSum:
    COPIES = 16

    def __init__(self, place, parts, keep, first, second, third, fourth, full, send, recv, local):
        self.place = place
        self.parts = parts
        self.keep, self.first, self.second = keep, first, second
        self.third, self.fourth, self.full = third, fourth, full
        self.send, self.recv, self.local = send, recv, local

    def copy(self, i, slot, src, dst, where):
        return remote(src, dst, self.send.at[i, slot], self.recv.at[i, slot], where)

    def fetch(self, i, source, index):
        return pltpu.make_async_copy(
            source.at[index, self.place.c], self.keep.at[i], self.local.at[i]
        )

    def copies(self, phase, i, source=None, index=None):
        p = self.place
        keep, full = self.keep, self.full
        both = self.parts == 2
        out = []
        if phase == 1:
            out.append(self.copy(i, 0, source.at[index, 1 - p.c], self.first.at[i], p.core()))
        if phase == 2:
            src = keep.at[i, 0, 1 - p.x]
            out.append(self.copy(i, 1, src, self.second.at[i, 0], p.side("x")))
            if both:
                src = keep.at[i, 1, :, 1 - p.y]
                out.append(self.copy(i, 2, src, self.second.at[i, 1], p.side("y")))
        if phase == 3:
            src = keep.at[i, 0, p.x, 1 - p.y]
            out.append(self.copy(i, 3, src, self.third.at[i, 0], p.side("y")))
            if both:
                src = keep.at[i, 1, 1 - p.x, p.y]
                out.append(self.copy(i, 4, src, self.third.at[i, 1], p.side("x")))
        if phase == 4:
            for o in range(1, 4):
                src = keep.at[i, :, p.x, p.y, p.h ^ o]
                out.append(self.copy(i, 4 + o, src, self.fourth.at[i, o - 1], p.up(o)))
        if phase == 5:
            spot = full.at[i, p.c, :, p.x, p.y, p.h]
            for o in range(1, 4):
                out.append(self.copy(i, 7 + o, spot, spot, p.up(o)))
        if phase == 6:
            spot = full.at[i, p.c, 0, p.x, p.y]
            out.append(self.copy(i, 11, spot, spot, p.side("y")))
            if both:
                spot = full.at[i, p.c, 1, p.x, p.y]
                out.append(self.copy(i, 12, spot, spot, p.side("x")))
        if phase == 7:
            spot = full.at[i, p.c, 0, p.x]
            out.append(self.copy(i, 13, spot, spot, p.side("x")))
            if both:
                spot = full.at[i, p.c, 1, :, p.y]
                out.append(self.copy(i, 14, spot, spot, p.side("y")))
        if phase == 8:
            spot = full.at[i, p.c]
            out.append(self.copy(i, 15, spot, spot, p.core()))
        return out

    def begin(self, i, source, index):
        self.fetch(i, source, index).start()
        for one in self.copies(1, i, source, index):
            one.start()

    def advance(self, phase, i, source=None, index=None):
        p = self.place
        if phase == 2:
            self.fetch(i, source, index).wait()
        for one in self.copies(phase - 1, i, source, index):
            one.wait()
        if phase == 2:
            add_into(self.keep.at[i], self.first.at[i])
        if phase == 3:
            add_into(self.keep.at[i, 0, p.x], self.second.at[i, 0])
            if self.parts == 2:
                add_into(self.keep.at[i, 1, :, p.y], self.second.at[i, 1])
        if phase == 4:
            for part in range(self.parts):
                add_into(self.keep.at[i, part, p.x, p.y], self.third.at[i, part])
        if phase == 5:
            total = self.keep[i, :, p.x, p.y, p.h].astype(F32)
            for o in range(3):
                total = total + self.fourth[i, o].astype(F32)
            self.full[i, p.c, :, p.x, p.y, p.h] = total.astype(BF)
        if phase <= 8:
            for one in self.copies(phase, i):
                one.start()


class GroupSum:
    COPIES = 11

    def __init__(self, place, own, first, second, third, fourth, full, send, recv):
        self.place = place
        self.own, self.first, self.second = own, first, second
        self.third, self.fourth, self.full = third, fourth, full
        self.send, self.recv = send, recv

    def copy(self, g, slot, src, dst, where):
        return remote(src, dst, self.send.at[g, slot], self.recv.at[g, slot], where)

    def copies(self, phase, g):
        p, own, full = self.place, self.own, self.full
        x, y = p.side("x"), p.side("y")
        if phase == 1:
            return [self.copy(g, 0, own.at[g, 1 - p.c], self.first.at[g], p.core())]
        if phase == 2:
            return [
                self.copy(g, 1, own.at[g, p.c, 0, 1 - p.x], self.second.at[g, 0], x),
                self.copy(g, 2, own.at[g, p.c, 1, :, 1 - p.y], self.second.at[g, 1], y),
            ]
        if phase == 3:
            return [
                self.copy(g, 3, own.at[g, p.c, 0, p.x, 1 - p.y], self.third.at[g, 0], y),
                self.copy(g, 4, own.at[g, p.c, 1, 1 - p.x, p.y], self.third.at[g, 1], x),
            ]
        if phase == 4 and g > 0:
            return [
                self.copy(g, 5, own.at[g, p.c, :, p.x, p.y], self.fourth.at[g - 1], p.up(g))
            ]
        if phase == 6:
            spots = full.at[p.c, 0, p.x, p.y], full.at[p.c, 1, p.x, p.y]
            return [self.copy(0, 6, spots[0], spots[0], y), self.copy(0, 7, spots[1], spots[1], x)]
        if phase == 7:
            spots = full.at[p.c, 0, p.x], full.at[p.c, 1, :, p.y]
            return [self.copy(0, 8, spots[0], spots[0], x), self.copy(0, 9, spots[1], spots[1], y)]
        if phase == 8:
            spot = full.at[p.c]
            return [self.copy(0, 10, spot, spot, p.core())]
        return []

    def begin(self, g):
        for one in self.copies(1, g):
            one.start()

    def advance(self, phase, g):
        p, own = self.place, self.own
        if phase == 6:
            for group in range(own.shape[0]):
                for one in self.copies(4, group):
                    one.wait()
            total = own[0, p.c, :, p.x, p.y].astype(F32)
            for o in range(3):
                total = total + self.fourth[o].astype(F32)
            self.full[p.c, :, p.x, p.y] = total.astype(BF)
        else:
            for one in self.copies(phase - 1, g):
                one.wait()
        if phase == 2:
            add_into(own.at[g, p.c], self.first.at[g])
        if phase == 3:
            add_into(own.at[g, p.c, 0, p.x], self.second.at[g, 0])
            add_into(own.at[g, p.c, 1, :, p.y], self.second.at[g, 1])
        if phase == 4:
            add_into(own.at[g, p.c, 0, p.x, p.y], self.third.at[g, 0])
            add_into(own.at[g, p.c, 1, p.x, p.y], self.third.at[g, 1])
        for one in self.copies(phase, g):
            one.start()


class Stages:
    def __init__(self, tokens, ff, count, heads):
        rows = tokens // LEN
        self.blocks = ff // BLOCK
        self.norms = self.blocks + tokens // BLOCK
        self.outer = self.norms + count
        self.per_group = 2 * rows
        self.end = self.outer + count * self.per_group
        self.half = ff // CHUNK
        self.outw_first = self.outer + 1


def late_kernel(
    plan,
    gf_ref,
    nl_hbm,
    slope_ref,
    dw_ref,
    uw_ref,
    xh_ref,
    inv_ref,
    gs_ref,
    gain_ref,
    x_hbm,
    w_ref,
    ow_ref,
    ctx_ref,
    q_ref,
    k_ref,
    v_ref,
    lse_ref,
    mask_ref,
    early_0,
    early_1,
    early_2,
    early_3,
    early_4,
    early_5,
    early_6,
    down_ref,
    vec_ref,
    dx_out,
    wg_out,
    down_out,
    up_out,
    outw_out,
    up_ref,
    outw_ref,
    dx,
    rows_ref,
    ga_all,
    dpre,
    stage_w,
    stage_o,
    wg_acc,
    dctx,
    k_t,
    dq_t,
    dk_acc,
    dv_acc,
    stage_up,
    vec,
    vec_in,
    ff_keep,
    ff_1,
    ff_2,
    ff_3,
    ff_4,
    ff_full,
    ow_keep,
    ow_1,
    ow_2,
    ow_3,
    ow_4,
    ow_full,
    qk_own,
    qk_1,
    qk_2,
    qk_3,
    qk_4,
    qk_full,
    ff_send,
    ff_recv,
    ff_local,
    ow_send,
    ow_recv,
    ow_local,
    qk_send,
    qk_recv,
    vec_send,
    vec_recv,
    store_sem,
    block_sem,
    outer_sem,
    last_sem,
    rows_sem,
):
    step = pl.program_id(0)
    place = Place()
    half = plan.half
    chunks = 2 * half
    count = qk_own.shape[0]
    width = q_ref.shape[2]
    heads = width // HEAD_DIM
    feed = MatrixSum(
        place, 2, ff_keep, ff_1, ff_2, ff_3, ff_4, ff_full, ff_send, ff_recv, ff_local
    )
    outer = MatrixSum(
        place, 1, ow_keep, ow_1, ow_2, ow_3, ow_4, ow_full, ow_send, ow_recv, ow_local
    )
    groups = GroupSum(place, qk_own, qk_1, qk_2, qk_3, qk_4, qk_full, qk_send, qk_recv)
    tail = plan.end
    end = max(
        tail + 8,
        plan.outw_first + 8 * SPACING + 1,
        UP_FIRST + UP_EVERY * (half - 1) + 8 * SPACING + 1,
    )

    nl_load = pltpu.make_async_copy(nl_hbm, rows_ref, rows_sem.at[0])
    x_load = pltpu.make_async_copy(x_hbm, rows_ref, rows_sem.at[1])

    @pl.when(step == 0)
    def _():
        nl_load.start()
        greet(
            [place.core(), place.side("x"), place.side("y")] + [place.up(o) for o in range(1, 4)]
        )
        nl_load.wait()
        vec[...] = jnp.zeros_like(vec)
        rows = (early_0, 0), (early_1, 1), (early_2, 2)
        rows += (early_3, 10), (early_4, 11), (early_5, 12), (early_6, 13)
        for ref, index in rows:
            vec[0, index : index + 1, :] = ref[...].reshape(1, vec.shape[2])

    def down_store(i):
        return pltpu.make_async_copy(ff_full.at[i], down_out.at[i], store_sem.at[i, 0])

    def up_store(i, part):
        spot = pl.ds(pl.multiple_of((2 * i + part) * (CHUNK // 2), CHUNK // 2), CHUNK // 2)
        return pltpu.make_async_copy(stage_up, up_out.at[:, spot], store_sem.at[half + i, part])

    def outw_store():
        return pltpu.make_async_copy(ow_full.at[0], outw_out.at[0], store_sem.at[chunks, 0])

    def tick(t, start, stop):
        span = 8 * SPACING

        def window(first, last, run):
            if start <= last and stop > first:

                @pl.when((t >= first) & (t <= last))
                def _():
                    run()

        def each(first, every, number, run):
            for phase in range(9, 0, -1):
                behind = SPACING * (phase - 1)
                if stop - behind <= first or start - behind > first + every * (number - 1):
                    continue
                at = t - behind - first
                index = at // every

                @pl.when((at >= 0) & (index < number) & (at % every == 0))
                def _():
                    run(phase, index)

        def down_step(phase, i):
            if phase == 1:
                feed.begin(i, down_ref, i)
                return
            feed.advance(phase, i, down_ref, i)
            if phase == 9:
                down_store(i).start()

        def up_step(phase, i):
            if phase == 1:
                feed.begin(half + i, up_ref, i)
                return
            feed.advance(phase, half + i, up_ref, i)
            if phase == 9:

                @pl.when(i > 0)
                def _():
                    up_store(i - 1, 1).wait()

                for c in range(2):
                    if c == 1:
                        up_store(i, 0).wait()
                    block = ff_full[half + i, c].reshape(CHUNK // 2, 2 * LANES)
                    stage_up[...] = block.T
                    up_store(i, c).start()

        def outw_step(phase, i):
            if phase == 1:
                outer.begin(0, outw_ref, 0)
                return
            outer.advance(phase, 0, outw_ref, 0)
            if phase == 9:
                outw_store().start()

        def group_steps():
            for g in range(count):
                base = plan.outer + plan.per_group * (g + 1)
                if base < start or base >= stop:
                    continue
                phases = (9, 8, 7, 6, 4, 3, 2) if g == count - 1 else (4, 3, 2)
                for phase in phases:
                    when = phase - 1 if phase < 5 else phase - 2

                    @pl.when(t == base + when)
                    def _():
                        groups.advance(phase, g)

                @pl.when(t == base)
                def _():
                    groups.begin(g)

        first, last = 0, DOWN_EVERY * (half - 1) + span
        window(first, last, lambda: each(0, DOWN_EVERY, half, down_step))
        first, last = UP_FIRST, UP_FIRST + UP_EVERY * (half - 1) + span
        window(first, last, lambda: each(UP_FIRST, UP_EVERY, half, up_step))
        first, last = plan.outw_first, plan.outw_first + span
        window(first, last, lambda: each(plan.outw_first, 1, 1, outw_step))
        window(plan.outer + plan.per_group, tail + 8, group_steps)

    tick(step, 0, tail)


    def block_copy(b):
        per_chunk = CHUNK // BLOCK
        spot = up_ref.at[b // per_chunk, (b % per_chunk) // 2, b % 2]
        return pltpu.make_async_copy(stage_w.at[b % 2], spot, block_sem.at[b])

    @pl.when(step < plan.blocks)
    def _():
        grad = dot_nt(gf_ref[...], dw_ref[...]) * slope_ref[...]
        dpre[...] = grad.astype(BF)

        @pl.when(step > 1)
        def _():
            block_copy(step - 2).wait()

        part = dot_tn(dpre[...], rows_ref[...]).astype(BF)
        stage_w[step % 2] = part.reshape(stage_w.shape[1:])
        block_copy(step).start()
        per_row = rows_ref.shape[1] // BLOCK
        spot = pl.ds(pl.multiple_of((step % per_row) * BLOCK, BLOCK), BLOCK)
        vec[0, pl.ds(6 + step // per_row, 1), spot] = jnp.sum(
            dpre[...].astype(F32), axis=0, keepdims=True
        )
        for r in range(0, dx.shape[0], BLOCK):
            part = dot_nt(dpre[r : r + BLOCK], uw_ref[...])

            @pl.when(step == 0)
            def _():
                dx[r : r + BLOCK] = part

            @pl.when(step > 0)
            def _():
                dx[r : r + BLOCK] = dx[r : r + BLOCK] + part


    @pl.when((step >= plan.blocks) & (step < plan.norms))
    def _():
        @pl.when(step == plan.blocks)
        def _():
            block_copy(plan.blocks - 2).wait()
            block_copy(plan.blocks - 1).wait()
            x_load.start()

        rows = pl.ds(pl.multiple_of((step - plan.blocks) * BLOCK, BLOCK), BLOCK)
        upstream = dx[rows, :] + gs_ref[...]
        normal = xh_ref[...]
        scaled = upstream * gain_ref[...].reshape(1, upstream.shape[1])
        mean = jnp.mean(scaled, axis=1, keepdims=True)
        along = jnp.mean(scaled * normal, axis=1, keepdims=True)
        hidden = inv_ref[...] * (scaled - mean - normal * along)
        low = hidden.astype(BF)
        dx[rows, :] = hidden
        ga_all[rows, :] = low
        vec[0, 3:4, :] += jnp.sum(upstream * normal, axis=0, keepdims=True)
        vec[0, 4:5, :] += jnp.sum(upstream, axis=0, keepdims=True)
        vec[0, 5:6, :] += jnp.sum(low.astype(F32), axis=0, keepdims=True)


    def outer_copy(g):
        spot = place.h ^ g
        return pltpu.make_async_copy(
            stage_o, outw_ref.at[0, spot >> 1, 0, spot & 1], outer_sem.at[g]
        )

    @pl.when((step >= plan.norms) & (step < plan.outer))
    def _():
        g = step - plan.norms

        @pl.when(g > 0)
        def _():
            outer_copy(g - 1).wait()

        part = dot_tn(ctx_ref[0], ga_all[...])
        stage_o[...] = part.astype(BF).reshape(stage_o.shape)
        outer_copy(g).start()

    @pl.when(step == plan.outer)
    def _():
        outer_copy(count - 1).wait()
        x_load.wait()


    def dx_copy(r):
        spot = pl.ds(pl.multiple_of(r * LEN, LEN), LEN)
        return pltpu.make_async_copy(dx.at[spot], dx_out.at[spot], last_sem.at[r])

    @pl.when(step >= plan.outer)
    def _():
        at = step - plan.outer
        part = at % 2
        row = (at // 2) % 2
        group = at // plan.per_group
        mine = pl.ds(pl.multiple_of(row * LEN, LEN), LEN)
        q = q_ref[0]
        k = k_ref[0]
        v = v_ref[0]

        @pl.when(part == 0)
        def _():
            dctx[...] = dot_nt(ga_all[mine, :], ow_ref[place.h ^ group]).astype(BF)
            k_t[...] = k.T

        q_scaled = q * jnp.asarray(0.125, BF)

        def one_head(head, carry):
            mask = head_lanes(width, head)
            spot = pl.ds(pl.multiple_of(head * HEAD_DIM, HEAD_DIM), HEAD_DIM)
            scores = dot_nt(jnp.where(mask, k, jnp.zeros_like(k)), q_scaled)
            probs = jnp.exp(scores - lse_ref[0, 0, pl.ds(head, 1), :])
            dprobs = dot_nt(jnp.where(mask, v, jnp.zeros_like(v)), dctx[...])
            delta = jnp.sum(probs * dprobs, axis=0, keepdims=True)
            dscores = (probs * (dprobs - delta)).astype(BF)
            dv_acc[...] = jnp.where(mask, dot_nn(probs.astype(BF), dctx[...]), dv_acc[...])
            dk_acc[...] = jnp.where(mask, dot_nn(dscores, q_scaled), dk_acc[...])
            dq_t[spot, :] = dot_nn(k_t[spot, :], dscores)
            return carry

        split = heads // 2 + 1
        lax.fori_loop(part * split, split + part * (heads - split), one_head, 0)

        @pl.when(part == 1)
        def _():
            x = rows_ref[mine, :]
            dq = (dq_t[...] * 0.125).T.astype(BF)
            dk = dk_acc[...].astype(BF)
            dv = dv_acc[...].astype(BF)
            delta = dot_nn(dq, w_ref[0, 0]) + dot_nn(dk, w_ref[0, 1]) + dot_nn(dv, w_ref[0, 2])
            dx[mine, :] = dx[mine, :] + delta

            @pl.when(row == 0)
            def _():
                wg_acc[...] = jnp.zeros_like(wg_acc)

            for index, grad in enumerate((dq, dk, dv)):
                wg_acc[index * width : (index + 1) * width] += dot_tn(grad, x)
            spot = place.h ^ group
            vec[0, pl.ds(16 + spot, 1), 0:width] += jnp.sum(
                dq.astype(F32), axis=0, keepdims=True
            )
            vec[0, pl.ds(20 + spot, 1), 0:width] += jnp.sum(
                dv.astype(F32), axis=0, keepdims=True
            )

            @pl.when(row == 1)
            def _():
                shape = qk_own.shape[2:]
                for zl in range(2):
                    block = wg_acc[:, zl * LANES : (zl + 1) * LANES].astype(BF)
                    qk_own[group, zl] = block.reshape(shape)

            @pl.when(group == count - 1)
            def _():
                total = jnp.where(mask_ref[...] == 1.0, dx[mine, :], 0.0)
                vec[0, 15:16, :] += jnp.sum(total, axis=0, keepdims=True)
                dx_copy(row).start()

    @pl.when(step == plan.end - 1)
    def _():
        def vec_copy(k):
            if k < 3:
                where = (place.dp ^ (1 << k), place.h)
            else:
                where = (place.dp, place.h ^ (1 << (k - 3)))
            return remote(vec.at[k], vec_in.at[k], vec_send.at[k], vec_recv.at[k], where)

        @pl.loop(tail, end)
        def _(t):
            tick(t, tail, end)
            for k in range(6):

                @pl.when(t == tail + k)
                def _():
                    if k > 0:
                        vec_copy(k - 1).wait()
                        vec[k] = vec[k - 1] + vec_in[k - 1]
                    if k < 5:
                        vec_copy(k).start()

        vec_ref[...] = vec[5]
        for c in range(2):
            block = qk_full[c].reshape(wg_acc.shape[0], LANES)
            wg_acc[:, c * LANES : (c + 1) * LANES] = block.astype(F32)
        wg_copy = pltpu.make_async_copy(wg_acc, wg_out, last_sem.at[2])
        wg_copy.start()
        for i in range(half):
            down_store(i).wait()
        up_store(half - 1, 1).wait()
        outw_store().wait()
        for r in range(2):
            dx_copy(r).wait()
        wg_copy.wait()


def late_call(
    gf, nl, slope, dw, uw, xh, inv, gs, gain, x, w, ow, ctx, q, k, v, lse, mask, early, down
):
    tokens, features = x.shape
    count, _, width, _ = w.shape
    ff = down.shape[0]
    heads = width // HEAD_DIM
    plan = Stages(tokens, ff, count, heads)
    chunks = 2 * plan.half
    chunked = (plan.half, 2, 2, 2, 2, 4, PIECE, features)
    squared = (1, 2, 1, 2, 2, 4, features // 32, features)
    hbm = pl.BlockSpec(memory_space=pl.ANY)
    once = pl.Buffered(1)

    def whole(shape):
        return pl.BlockSpec(shape, lambda s: (0,) * len(shape), pipeline_mode=once)

    def block_at(s):
        return jnp.minimum(s, plan.blocks - 1)

    def norm_at(s):
        return jnp.clip(s - plan.blocks, 0, tokens // BLOCK - 1)

    def head_at(s):
        at = jnp.clip(s - plan.outer, 0, plan.end - plan.outer - 1)
        return at // plan.per_group, (at // 2) % 2

    def per_head(s):
        group, row = head_at(s)
        return group, row, 0

    in_specs = [
        whole(gf.shape),
        hbm,
        pl.BlockSpec((tokens, BLOCK), lambda s: (0, block_at(s))),
        pl.BlockSpec((BLOCK, features), lambda s: (block_at(s), 0)),
        pl.BlockSpec((features, BLOCK), lambda s: (0, block_at(s))),
        pl.BlockSpec((BLOCK, features), lambda s: (norm_at(s), 0)),
        pl.BlockSpec((BLOCK, 1), lambda s: (norm_at(s), 0), pipeline_mode=once),
        pl.BlockSpec((BLOCK, features), lambda s: (norm_at(s), 0)),
        whole(gain.shape),
        hbm,
        pl.BlockSpec((1, 3, width, features), lambda s: (head_at(s)[0], 0, 0, 0)),
        whole(ow.shape),
        pl.BlockSpec(
            (1, tokens, width),
            lambda s: (jnp.clip(s - plan.norms, 0, count - 1), 0, 0),
            pipeline_mode=once,
        ),
        pl.BlockSpec((1, LEN, width), per_head),
        pl.BlockSpec((1, LEN, width), per_head),
        pl.BlockSpec((1, LEN, width), per_head),
        pl.BlockSpec((1, 1, 8, LEN), lambda s: head_at(s) + (0, 0)),
        pl.BlockSpec((LEN, 1), lambda s: (head_at(s)[1], 0)),
    ]
    in_specs += [whole(one.shape) for one in early]
    in_specs += [hbm]
    out_specs = [pl.BlockSpec((24, features), lambda s: (0, 0))] + [hbm] * 7
    out_shape = [
        jax.ShapeDtypeStruct((24, features), F32),
        jax.ShapeDtypeStruct((tokens, features), F32),
        jax.ShapeDtypeStruct((3 * width, features), F32),
        jax.ShapeDtypeStruct(chunked, BF),
        jax.ShapeDtypeStruct((features, ff), BF),
        jax.ShapeDtypeStruct(squared, BF),
        jax.ShapeDtypeStruct(chunked, BF),
        jax.ShapeDtypeStruct(squared, BF),
    ]

    def sum_buffers(n, parts, rows):
        block = (rows, features)
        return [
            pltpu.VMEM((n, parts, 2, 2, 4) + block, BF),
            pltpu.VMEM((n, parts, 2, 2, 4) + block, BF),
            pltpu.VMEM((n, parts, 2, 4) + block, BF),
            pltpu.VMEM((n, parts, 4) + block, BF),
            pltpu.VMEM((n, 3, parts) + block, BF),
            pltpu.VMEM((n, 2, parts, 2, 2, 4) + block, BF),
        ]

    qrows = 3 * width // 8
    quarter = (2, 2, 2, qrows, LANES)
    scratch = [
        pltpu.VMEM((tokens, features), F32),
        pltpu.VMEM((tokens, features), BF),
        pltpu.VMEM((tokens, features), BF),
        pltpu.VMEM((tokens, BLOCK), BF),
        pltpu.VMEM((2, 2, 2, 4, PIECE, features), BF),
        pltpu.VMEM((2, 4, width // 8, features), BF),
        pltpu.VMEM((3 * width, features), F32),
        pltpu.VMEM((LEN, width), BF),
        pltpu.VMEM((width, LEN), BF),
        pltpu.VMEM((width, LEN), F32),
        pltpu.VMEM((LEN, width), F32),
        pltpu.VMEM((LEN, width), F32),
        pltpu.VMEM((features, CHUNK // 2), BF),
        pltpu.VMEM((6, 24, features), F32),
        pltpu.VMEM((5, 24, features), F32),
    ]
    scratch += sum_buffers(chunks, 2, PIECE)
    scratch += sum_buffers(1, 1, features // 32)
    scratch += [
        pltpu.VMEM((count, 2) + quarter, BF),
        pltpu.VMEM((count,) + quarter, BF),
        pltpu.VMEM((count, 2, 2, qrows, LANES), BF),
        pltpu.VMEM((count, 2, qrows, LANES), BF),
        pltpu.VMEM((3, 2, qrows, LANES), BF),
        pltpu.VMEM((2,) + quarter, BF),
    ]
    dma = pltpu.SemaphoreType.DMA
    scratch += [
        dma((chunks, MatrixSum.COPIES)),
        dma((chunks, MatrixSum.COPIES)),
        dma((chunks,)),
        dma((1, MatrixSum.COPIES)),
        dma((1, MatrixSum.COPIES)),
        dma((1,)),
        dma((count, GroupSum.COPIES)),
        dma((count, GroupSum.COPIES)),
        dma((5,)),
        dma((5,)),
        dma((chunks + 1, 2)),
        dma((plan.blocks,)),
        dma((count,)),
        dma((3,)),
        dma((2,)),
    ]
    results = pl.pallas_call(
        functools.partial(late_kernel, plan),
        grid=(plan.end,),
        in_specs=in_specs,
        out_specs=out_specs,
        out_shape=out_shape,
        scratch_shapes=scratch,
        compiler_params=pltpu.CompilerParams(
            dimension_semantics=("arbitrary",),
            vmem_limit_bytes=67043328,
            collective_id=1,
            has_side_effects=True,
        ),
        name="late_kernel",
    )(
        gf,
        nl,
        slope,
        dw,
        uw,
        xh,
        inv,
        gs,
        gain,
        x,
        w,
        ow,
        ctx,
        q,
        k,
        v,
        lse,
        mask,
        *early,
        down.reshape(chunked),
    )
    sums, dx, wg, down_sum, up_sum, outw_sum = results[:6]
    return (
        dx,
        wg,
        sums,
        down_sum.reshape(ff, features),
        up_sum,
        outw_sum.reshape(features, features),
    )


def final_kernel(down_ref, up_ref, outw_ref, dx_ref, mask_ref, down_out, up_out, outw_out, dx_out):
    down_out[...] = down_ref[...].astype(F32)
    up_out[...] = up_ref[...].astype(F32)
    outw_out[...] = outw_ref[...].astype(F32)
    dx_out[...] = jnp.where(mask_ref[...] == 1.0, 0.0, dx_ref[...])


def final_call(down, up, outw, dx, mask):
    steps = 8
    arrays = (down, up, outw, dx)

    def spec(shape):
        return pl.BlockSpec((shape[0] // steps, shape[1]), lambda s: (s, 0))

    return pl.pallas_call(
        final_kernel,
        grid=(steps,),
        in_specs=[spec(one.shape) for one in arrays + (mask,)],
        out_specs=[spec(one.shape) for one in arrays],
        out_shape=[jax.ShapeDtypeStruct(one.shape, F32) for one in arrays],
        compiler_params=pltpu.CompilerParams(
            dimension_semantics=("arbitrary",), vmem_limit_bytes=63 << 20
        ),
        name="final_kernel",
    )(down, up, outw, dx, mask)


def swap(value, axis, mask, size):
    return lax.ppermute(value, axis, [(i, i ^ mask) for i in range(size)])


def bit_of(axis, bit):
    return (lax.axis_index(axis) >> bit) & 1


def joined(mine, other, upper, dim, kind=None):
    low = jnp.where(upper == 1, other, mine)
    high = jnp.where(upper == 1, mine, other)
    if kind is not None:
        low, high = low.astype(kind), high.astype(kind)
    return jnp.concatenate([low, high], axis=dim)


def halve(value, bit, size, dim):
    half = value.shape[dim] // 2
    mine = bit_of("dp", bit)
    sent = lax.dynamic_slice_in_dim(value, (1 - mine) * half, half, dim)
    kept = lax.dynamic_slice_in_dim(value, mine * half, half, dim)
    received = swap(sent, "dp", 1 << bit, size)
    return (kept.astype(F32) + received.astype(F32)).astype(BF)


def double(value, bit, size, dim, kind=None):
    return joined(value, swap(value, "dp", 1 << bit, size), bit_of("dp", bit), dim, kind)


def plane_orders(size):
    bits = size.bit_length() - 1
    rest = list(range(1, bits))
    return rest, rest[::-1]


def reduce_plane(value, size, dim):
    value = halve(value, 0, size, dim)
    half = value.shape[dim] // 2
    parts = []
    for index, order in enumerate(plane_orders(size)):
        part = lax.slice_in_dim(value, index * half, (index + 1) * half, axis=dim)
        for bit in order:
            part = halve(part, bit, size, dim)
        parts.append(part)
    return parts


def gather_plane(parts, size, dim, kind=None):
    done = []
    for part, order in zip(parts, plane_orders(size)):
        for bit in order[::-1]:
            part = double(part, bit, size, dim)
        done.append(part)
    return double(jnp.concatenate(done, axis=dim), 0, size, dim, kind)


def reduce_head(pieces, size):
    total = pieces[0].astype(F32)
    for offset in range(1, size):
        total = total + swap(pieces[offset], "head", offset, size).astype(F32)
    return total


def gather_head(piece, size):
    return [piece] + [swap(piece, "head", offset, size) for offset in range(1, size)]


def absolute(pieces, dim):
    count = len(pieces)
    bit = 0
    while (1 << bit) < count:
        upper = bit_of("head", bit)
        step = 1 << bit
        pieces = [
            jnp.where(upper == 1, pieces[index ^ step], pieces[index]) for index in range(count)
        ]
        bit += 1
    return jnp.concatenate(pieces, axis=dim)


def own_pieces(value, size, dim):
    width = value.shape[dim] // size
    me = lax.axis_index("head")
    return [
        lax.dynamic_slice_in_dim(value, (me ^ offset) * width, width, dim)
        for offset in range(size)
    ]


def all_reduce_matrix(value, dp, head, head_dim):
    parts = []
    for part in reduce_plane(value, dp, 0):
        piece = reduce_head(own_pieces(part, head, head_dim), head).astype(BF)
        parts.append(absolute(gather_head(piece, head), head_dim))
    return gather_plane(parts, dp, 0, F32)


def all_reduce_small(vector, dp, head):
    bit = 1
    while bit < dp:
        vector = vector + swap(vector, "dp", bit, dp)
        bit *= 2
    bit = 1
    while bit < head:
        vector = vector + swap(vector, "head", bit, head)
        bit *= 2
    return vector


def norm_forward(hidden, gain, bias):
    center = hidden - jnp.mean(hidden, axis=-1, keepdims=True)
    inverse = lax.rsqrt(jnp.mean(center * center, axis=-1, keepdims=True) + EPS)
    normal = center * inverse
    return (normal * gain + bias, normal, inverse)


def norm_backward(upstream, normal, inverse, gain):
    gain_grad = jnp.sum(upstream * normal, axis=0)
    bias_grad = jnp.sum(upstream, axis=0)
    scaled = upstream * gain
    hidden_grad = inverse * (
        scaled
        - jnp.mean(scaled, axis=-1, keepdims=True)
        - normal * jnp.mean(scaled * normal, axis=-1, keepdims=True)
    )
    return (hidden_grad, gain_grad, bias_grad)


def phi(values):
    return 0.5 * (1.0 + jax.scipy.special.erf(values * (1.0 / math.sqrt(2.0))))


def body(
    dp,
    head,
    tokens,
    span_mask,
    valid_mask,
    mask_embedding,
    qkv_weight,
    query_bias,
    value_bias,
    out_weight,
    out_bias,
    norm1_gain,
    norm1_bias,
    up_weight,
    up_bias,
    down_weight,
    down_bias,
    norm2_gain,
    norm2_bias,
    out_grad,
):
    features = tokens.shape[1]
    width = qkv_weight.shape[2]
    masked = (span_mask == 1)[:, None]
    validity = valid_mask.astype(F32)[:, None]
    direct = dp == 8 and head == 4 and features == 2 * LANES and tokens.shape[0] == 2 * LEN
    if direct:
        mask_column = (span_mask == 1).astype(F32)[:, None]
        out_parts = out_weight.reshape(head, width, features)
        q, k, v, ctx, lse, attended, inputs, weights = early_call(
            tokens,
            mask_column,
            mask_embedding,
            jnp.transpose(qkv_weight, (1, 2, 0)),
            query_bias,
            value_bias,
            out_parts,
            out_bias,
        )
    else:
        inputs = jnp.where(masked, mask_embedding[None, :], tokens)
        own = jnp.transpose(qkv_weight, (1, 0, 2))
        core = bit_of("dp", 0)
        half = lax.dynamic_slice_in_dim(own, core * (features // 2), features // 2, 1)
        halves = [half]
        for bit in range(head.bit_length() - 1):
            halves = halves + [swap(part, "head", 1 << bit, head) for part in halves]
        weights = [own] + [double(part, 0, dp, 1) for part in halves[1:]]
        biases = jnp.stack([query_bias, value_bias]).astype(F32)
        bias_parts = [biases]
        for bit in range(head.bit_length() - 1):
            bias_parts = bias_parts + [swap(part, "head", 1 << bit, head) for part in bias_parts]
        out_parts = own_pieces(out_weight, head, 0)

        attended = jnp.broadcast_to(out_bias[None, :], tokens.shape)
        saved = []
        for group in range(head):
            q, k, v, ctx, lse, attended = attention_forward(
                inputs,
                weights[group],
                bias_parts[group][0:1],
                bias_parts[group][1:2],
                out_parts[group],
                attended,
            )
            saved.append((q, k, v, ctx, lse))

    inputs_wide = inputs.astype(F32)
    normed, normal_first, inverse_first = norm_forward(
        inputs_wide + attended, norm1_gain, norm1_bias
    )
    normed_low = normed.astype(BF)
    preact = dot_nn(normed_low, up_weight) + up_bias
    share = phi(preact)
    activated = (preact * share).astype(BF)
    slope = share + preact * jnp.exp(-0.5 * preact * preact) * (1.0 / math.sqrt(2.0 * math.pi))
    feedout = dot_nn(activated, down_weight) + down_bias
    result, normal_second, inverse_second = norm_forward(normed + feedout, norm2_gain, norm2_bias)
    grad_output = out_grad.astype(F32) * validity
    grad_second, gain_second_grad, bias_second_grad = norm_backward(
        grad_output, normal_second, inverse_second, norm2_gain
    )
    grad_feed = grad_second.astype(BF)
    down_bias_grad = jnp.sum(grad_feed, axis=0, dtype=F32)
    down_local = dot_tn(activated, grad_feed).astype(BF)
    squares = jnp.stack(
        [
            jnp.sum(validity * inputs_wide * inputs_wide),
            jnp.sum(validity * attended * attended),
            jnp.sum(validity * feedout * feedout),
            jnp.sum(validity),
        ]
    )
    if direct:
        vectors = [down_bias_grad, gain_second_grad, bias_second_grad]
        vectors += [
            jnp.sum(validity * inputs_wide * inputs_wide, axis=0),
            jnp.sum(validity * attended * attended, axis=0),
            jnp.sum(validity * feedout * feedout, axis=0),
            jnp.broadcast_to(jnp.sum(validity), (features,)),
        ]
        dx, weight_sum, sums, down_sum, up_sum, outw_sum = late_call(
            grad_feed,
            normed_low,
            slope,
            down_weight,
            up_weight,
            normal_first,
            inverse_first,
            grad_second,
            norm1_gain,
            inputs,
            weights,
            out_parts,
            ctx,
            q,
            k,
            v,
            lse,
            mask_column,
            vectors,
            down_local,
        )
        down_weight_grad, up_weight_grad, out_weight_grad, tokens_grad = final_call(
            down_sum, up_sum, outw_sum, dx, mask_column
        )
        weight_grad = jnp.transpose(weight_sum.reshape(3, width, features), (2, 0, 1))
        me = lax.axis_index("head")
        first_grad = lax.dynamic_slice(sums, (16 + me, 0), (1, width))[0]
        third_grad = lax.dynamic_slice(sums, (20 + me, 0), (1, width))[0]
        count = jnp.maximum(sums[13, 0], 1.0)
        stream_rms = jnp.sqrt(jnp.sum(sums[10:13], axis=1) / (count * features))
        return (
            result.astype(BF),
            tokens_grad,
            sums[15],
            weight_grad,
            first_grad,
            third_grad,
            out_weight_grad,
            sums[5],
            sums[3],
            sums[4],
            up_weight_grad,
            sums[6:10].reshape(-1),
            down_weight_grad,
            sums[0],
            sums[1],
            sums[2],
            stream_rms,
        )

    grad_preact = (dot_nt(grad_feed, down_weight) * slope).astype(BF)
    up_bias_grad = jnp.sum(grad_preact, axis=0, dtype=F32)
    up_local = dot_tn(normed_low, grad_preact).astype(BF)
    grad_normed = dot_nt(grad_preact, up_weight) + grad_second
    grad_first, gain_first_grad, bias_first_grad = norm_backward(
        grad_normed, normal_first, inverse_first, norm1_gain
    )
    grad_attended = grad_first.astype(BF)
    out_bias_grad = jnp.sum(grad_attended, axis=0, dtype=F32)
    early = [
        down_bias_grad,
        gain_second_grad,
        bias_second_grad,
        gain_first_grad,
        bias_first_grad,
        out_bias_grad,
        up_bias_grad,
        squares,
    ]
    down_weight_grad = all_reduce_matrix(down_local, dp, head, 0)
    up_weight_grad = all_reduce_matrix(up_local, dp, head, 1)
    early_sum = all_reduce_small(jnp.concatenate(early), dp, head)

    grad_inputs = grad_first
    weight_pieces = []
    out_pieces = []
    query_parts = []
    value_parts = []
    for group in range(head):
        q, k, v, ctx, lse = saved[group]
        weight_piece, out_piece, query_part, value_part, grad_inputs = attention_backward(
            inputs,
            weights[group],
            out_parts[group],
            q,
            k,
            v,
            ctx,
            lse,
            grad_attended,
            grad_inputs,
        )
        weight_pieces.append(reduce_plane(weight_piece, dp, 1))
        out_pieces.append(out_piece)
        query_parts.append(query_part[0])
        value_parts.append(value_part[0])

    weight_grad = gather_plane(
        [
            reduce_head([weight_pieces[group][part] for group in range(head)], head).astype(BF)
            for part in range(2)
        ],
        dp,
        1,
        F32,
    )
    weight_grad = jnp.transpose(weight_grad, (1, 0, 2))

    out_reduced = jnp.stack(out_pieces)
    for bit in range(dp.bit_length() - 1):
        out_reduced = halve(out_reduced, bit, dp, 1)
    out_piece = reduce_head([out_reduced[group] for group in range(head)], head).astype(BF)
    for bit in range(dp.bit_length() - 2, -1, -1):
        out_piece = double(out_piece, bit, dp, 0)
    out_weight_grad = absolute(gather_head(out_piece, head), 0).astype(F32)

    tokens_grad = jnp.where(masked, 0.0, grad_inputs)
    embedding_grad = jnp.sum(jnp.where(masked, grad_inputs, 0.0), axis=0)
    late = jnp.concatenate([embedding_grad, absolute(query_parts, 0), absolute(value_parts, 0)])
    late_sum = all_reduce_small(late, dp, head)
    embedding_grad = late_sum[:features]
    me = lax.axis_index("head")
    first_grad = lax.dynamic_slice_in_dim(late_sum, features + me * width, width)
    third_grad = lax.dynamic_slice_in_dim(late_sum, 2 * features + me * width, width)

    pieces = []
    offset = 0
    for part in early:
        pieces.append(lax.slice_in_dim(early_sum, offset, offset + part.shape[0]))
        offset += part.shape[0]
    (
        down_bias_grad,
        gain_second_grad,
        bias_second_grad,
        gain_first_grad,
        bias_first_grad,
        out_bias_grad,
        up_bias_grad,
        squares,
    ) = pieces
    count = jnp.maximum(squares[3], 1.0)
    stream_rms = jnp.sqrt(squares[:3] / (count * features))
    return (
        result.astype(BF),
        tokens_grad,
        embedding_grad,
        weight_grad,
        first_grad,
        third_grad,
        out_weight_grad,
        out_bias_grad,
        gain_first_grad,
        bias_first_grad,
        up_weight_grad,
        up_bias_grad,
        down_weight_grad,
        down_bias_grad,
        gain_second_grad,
        bias_second_grad,
        stream_rms,
    )


def solution(mesh):
    split = P(("dp", "head"), None)
    flat = P(("dp", "head"))
    placed = (split, flat, flat, P(), P(None, None, "head"), P("head"), P("head")) + (P(),) * 10
    placed = placed + (split,)
    outs = (split, split, P(), P(None, None, "head"), P("head"), P("head")) + (P(),) * 11
    return jax.shard_map(
        functools.partial(body, mesh.shape["dp"], mesh.shape["head"]),
        mesh=mesh,
        in_specs=placed,
        out_specs=outs,
        check_vma=False,
    )
```

```python
import functools
import math

import jax
import jax.numpy as jnp
from jax import lax
from jax.experimental import pallas as pl
from jax.experimental.pallas import tpu as pltpu
from jax.sharding import PartitionSpec as P

HEAD_DIM = 64
LEN = 512
EPS = 1e-12
BF = jnp.bfloat16
F32 = jnp.float32


def dot_nn(left, right):
    return lax.dot_general(left, right, (((1,), (0,)), ((), ())), preferred_element_type=F32)


def dot_nt(left, right):
    return lax.dot_general(left, right, (((1,), (1,)), ((), ())), preferred_element_type=F32)


def dot_tn(left, right):
    return lax.dot_general(left, right, (((0,), (0,)), ((), ())), preferred_element_type=F32)


def head_lanes(width, head):
    lanes = lax.broadcasted_iota(jnp.int32, (1, width), 1)
    return (lanes >= head * HEAD_DIM) & (lanes < (head + 1) * HEAD_DIM)


def forward_kernel(
    x_ref, w_ref, qb_ref, vb_ref, ow_ref, acc_ref, q_ref, k_ref, v_ref, ctx_ref, lse_ref, out_ref
):
    x = x_ref[...]
    width = w_ref.shape[2]
    heads = width // HEAD_DIM
    q = (dot_nn(x, w_ref[0]) + qb_ref[...]).astype(BF)
    k = dot_nn(x, w_ref[1]).astype(BF)
    v32 = dot_nn(x, w_ref[2]) + vb_ref[...]
    v = v32.astype(BF)
    q_ref[...] = q
    k_ref[...] = k
    v_ref[...] = v
    v_t = v.T
    q_scaled = q * jnp.asarray(0.125, BF)
    pieces = []
    for head in range(heads):
        k_head = jnp.where(head_lanes(width, head), k, jnp.zeros_like(k))
        scores = dot_nt(k_head, q_scaled)
        highest = jnp.max(scores, axis=0, keepdims=True)
        exponent = jnp.exp(scores - highest)
        totals = jnp.sum(exponent, axis=0, keepdims=True)
        probs = (exponent * (1.0 / totals)).astype(BF)
        pieces.append(dot_nn(v_t[head * HEAD_DIM : (head + 1) * HEAD_DIM], probs))
        lse_ref[0, head : head + 1, :] = highest + jnp.log(totals)
    ctx = jnp.concatenate(pieces, axis=0).T.astype(BF)
    ctx_ref[...] = ctx
    out_ref[...] = acc_ref[...] + dot_nn(ctx, ow_ref[...])


def backward_kernel(
    x_ref,
    w_ref,
    ow_ref,
    q_ref,
    k_ref,
    v_ref,
    ctx_ref,
    lse_ref,
    ga_ref,
    acc_ref,
    wg_ref,
    owg_ref,
    qbg_ref,
    vbg_ref,
    out_ref,
    wg_acc,
    owg_acc,
):
    row = pl.program_id(0)
    last = pl.num_programs(0) - 1
    width = w_ref.shape[2]
    heads = width // HEAD_DIM
    x = x_ref[...]
    ga = ga_ref[...]
    dctx = dot_nt(ga, ow_ref[...]).astype(BF)
    q = q_ref[...]
    k = k_ref[...]
    v = v_ref[...]
    k_t = k.T
    q_scaled = q * jnp.asarray(0.125, BF)
    dq_t = []
    dk = jnp.zeros(q.shape, F32)
    dv = jnp.zeros(q.shape, F32)
    for head in range(heads):
        mask = head_lanes(width, head)
        scores = dot_nt(jnp.where(mask, k, jnp.zeros_like(k)), q_scaled)
        probs = jnp.exp(scores - lse_ref[0, head : head + 1, :])
        dprobs = dot_nt(jnp.where(mask, v, jnp.zeros_like(v)), dctx)
        delta = jnp.sum(probs * dprobs, axis=0, keepdims=True)
        dscores = (probs * (dprobs - delta)).astype(BF)
        dv = jnp.where(mask, dot_nn(probs.astype(BF), dctx), dv)
        dk = jnp.where(mask, dot_nn(dscores, q_scaled), dk)
        dq_t.append(dot_nn(k_t[head * HEAD_DIM : (head + 1) * HEAD_DIM], dscores))
    dq32 = (jnp.concatenate(dq_t, axis=0) * 0.125).T
    dq = dq32.astype(BF)
    dk = dk.astype(BF)
    dv = dv.astype(BF)
    out_ref[...] = (
        acc_ref[...] + dot_nt(dq, w_ref[0]) + dot_nt(dk, w_ref[1]) + dot_nt(dv, w_ref[2])
    )

    @pl.when(row == 0)
    def _():
        wg_acc[...] = jnp.zeros_like(wg_acc)
        owg_acc[...] = jnp.zeros_like(owg_acc)
        qbg_ref[...] = jnp.zeros_like(qbg_ref)
        vbg_ref[...] = jnp.zeros_like(vbg_ref)

    wg_acc[0] += dot_tn(x, dq)
    wg_acc[1] += dot_tn(x, dk)
    wg_acc[2] += dot_tn(x, dv)
    owg_acc[...] += dot_tn(ctx_ref[...], ga)
    qbg_ref[...] += jnp.sum(dq.astype(F32), axis=0, keepdims=True)
    vbg_ref[...] += jnp.sum(dv.astype(F32), axis=0, keepdims=True)

    @pl.when(row == last)
    def _():
        wg_ref[...] = wg_acc[...].astype(BF)
        owg_ref[...] = owg_acc[...].astype(BF)


def by_row(block):
    rank = len(block)
    return pl.BlockSpec(block, lambda r: (r,) + (0,) * (rank - 1))


def fixed(block):
    rank = len(block)
    return pl.BlockSpec(block, lambda r: (0,) * rank)


def attention_forward(x, w, qb, vb, ow, acc):
    tokens, features = x.shape
    width = w.shape[2]
    rows = tokens // LEN
    flops = 2 * tokens * features * width * 4 + 4 * tokens * LEN * width
    return pl.pallas_call(
        forward_kernel,
        grid=(rows,),
        in_specs=[
            by_row((LEN, features)),
            fixed(w.shape),
            fixed((1, width)),
            fixed((1, width)),
            fixed((width, features)),
            by_row((LEN, features)),
        ],
        out_specs=[
            by_row((LEN, width)),
            by_row((LEN, width)),
            by_row((LEN, width)),
            by_row((LEN, width)),
            by_row((1, 8, LEN)),
            by_row((LEN, features)),
        ],
        out_shape=[jax.ShapeDtypeStruct((tokens, width), BF)] * 4
        + [
            jax.ShapeDtypeStruct((rows, 8, LEN), F32),
            jax.ShapeDtypeStruct((tokens, features), F32),
        ],
        compiler_params=pltpu.CompilerParams(
            dimension_semantics=("arbitrary",), vmem_limit_bytes=48 << 20
        ),
        cost_estimate=pl.CostEstimate(
            flops=4 * flops, bytes_accessed=12 << 20, transcendentals=tokens * LEN * 3
        ),
        name="attention_forward",
    )(x, w, qb, vb, ow, acc)


def attention_backward(x, w, ow, q, k, v, ctx, lse, ga, acc):
    tokens, features = x.shape
    width = w.shape[2]
    rows = tokens // LEN
    flops = 2 * tokens * features * width * 8 + 10 * tokens * LEN * width
    return pl.pallas_call(
        backward_kernel,
        grid=(rows,),
        in_specs=[
            by_row((LEN, features)),
            fixed(w.shape),
            fixed((width, features)),
            by_row((LEN, width)),
            by_row((LEN, width)),
            by_row((LEN, width)),
            by_row((LEN, width)),
            by_row((1, 8, LEN)),
            by_row((LEN, features)),
            by_row((LEN, features)),
        ],
        out_specs=[
            fixed(w.shape),
            fixed((width, features)),
            fixed((1, width)),
            fixed((1, width)),
            by_row((LEN, features)),
        ],
        out_shape=[
            jax.ShapeDtypeStruct(w.shape, BF),
            jax.ShapeDtypeStruct((width, features), BF),
            jax.ShapeDtypeStruct((1, width), F32),
            jax.ShapeDtypeStruct((1, width), F32),
            jax.ShapeDtypeStruct((tokens, features), F32),
        ],
        scratch_shapes=[pltpu.VMEM(w.shape, F32), pltpu.VMEM((width, features), F32)],
        compiler_params=pltpu.CompilerParams(
            dimension_semantics=("arbitrary",), vmem_limit_bytes=48 << 20
        ),
        cost_estimate=pl.CostEstimate(
            flops=4 * flops, bytes_accessed=16 << 20, transcendentals=tokens * LEN * 3
        ),
        name="attention_backward",
    )(x, w, ow, q, k, v, ctx, lse, ga, acc)


MESH = pl.DeviceIdType.MESH


class Place:
    def __init__(self):
        self.dp = lax.axis_index("dp")
        self.h = lax.axis_index("head")
        self.c = self.dp & 1
        self.x = (self.dp >> 1) & 1
        self.y = (self.dp >> 2) & 1

    def core(self):
        return (self.dp ^ 1, self.h)

    def side(self, axis):
        return (self.dp ^ (2 if axis == "x" else 4), self.h)

    def up(self, offset):
        return (self.dp, self.h ^ offset)


def remote(src, dst, send, recv, where):
    return pltpu.make_async_remote_copy(
        src_ref=src,
        dst_ref=dst,
        send_sem=send,
        recv_sem=recv,
        device_id=where,
        device_id_type=MESH,
    )


def greet(friends):
    barrier = pltpu.get_barrier_semaphore()
    for friend in friends:
        pl.semaphore_signal(barrier, inc=1, device_id=friend, device_id_type=MESH)
    pl.semaphore_wait(barrier, len(friends))


def early_kernel(
    tokens_ref,
    mask_ref,
    embed_ref,
    own_ref,
    qb_ref,
    vb_ref,
    ow_ref,
    ob_ref,
    q_ref,
    k_ref,
    v_ref,
    ctx_ref,
    lse_ref,
    out_ref,
    x_out,
    w_out,
    w_all,
    b_all,
    send,
    recv,
    local,
):
    step = pl.program_id(0)
    group, row = step // 2, step % 2
    place = Place()
    width = w_all.shape[2]
    heads = width // HEAD_DIM
    half, quarter = width // 2, width // 4

    def half_of(g):
        return w_all.at[g, :, pl.ds(pl.multiple_of(place.c * half, half), half), :]

    def quarter_rows(g):
        side = place.x if g == 1 else place.y
        return pl.ds(pl.multiple_of(place.c * half + side * quarter, quarter), quarter)

    def quarter_of(g):
        return w_all.at[g, :, quarter_rows(g), :]

    load = pltpu.make_async_copy(own_ref, w_all.at[0], local.at[0])

    def direct(g):
        src = own_ref.at[:, quarter_rows(g), :]
        return remote(src, quarter_of(g), send.at[0, g], recv.at[0, g], place.up(g))

    relay = remote(quarter_of(2), quarter_of(3), send.at[0, 3], recv.at[0, 3], place.up(1))

    def beside(g):
        where = place.side("x" if g == 1 else "y")
        return remote(quarter_of(g), quarter_of(g), send.at[3, g], recv.at[3, g], where)

    def cross(g):
        return remote(half_of(g), half_of(g), send.at[1, g], recv.at[1, g], place.core())

    def bias(g):
        return remote(b_all.at[0], b_all.at[g], send.at[2, g], recv.at[2, g], place.up(g))

    def store(g):
        return pltpu.make_async_copy(w_all.at[g], w_out.at[g], local.at[2 + g])

    @pl.when(step == 0)
    def _():
        greet(
            [place.core(), place.side("x"), place.side("y")] + [place.up(o) for o in range(1, 4)]
        )
        direct(1).start()
        direct(2).start()
        load.start()
        b_all[0] = jnp.zeros(b_all.shape[1:], F32)
        b_all[0, 0:1, :] = qb_ref[...].astype(F32).reshape(1, width)
        b_all[0, 1:2, :] = vb_ref[...].astype(F32).reshape(1, width)
        load.wait()
        store(0).start()

    @pl.when(step == 1)
    def _():
        for g in range(1, 4):
            bias(g).start()

    for g in range(1, 4):

        @pl.when(step == 2 * g)
        def _():
            cross(g).wait()
            bias(g).wait()
            store(g).start()

    embed = embed_ref[...].astype(F32).reshape(1, tokens_ref.shape[1])
    x = jnp.where(mask_ref[...] == 1.0, embed, tokens_ref[...].astype(F32))
    x = x.astype(BF)

    @pl.when(step < 2)
    def _():
        x_out[...] = x

    q = (dot_nt(x, w_all[group, 0]) + b_all[group, 0:1, :]).astype(BF)
    k = dot_nt(x, w_all[group, 1]).astype(BF)
    v = (dot_nt(x, w_all[group, 2]) + b_all[group, 1:2, :]).astype(BF)
    q_ref[0] = q
    k_ref[0] = k
    v_ref[0] = v
    v_t = v.T
    q_scaled = q * jnp.asarray(0.125, BF)
    pieces = []
    for head in range(heads):
        k_head = jnp.where(head_lanes(width, head), k, jnp.zeros_like(k))
        scores = dot_nt(k_head, q_scaled)
        highest = jnp.max(scores, axis=0, keepdims=True)
        exponent = jnp.exp(scores - highest)
        totals = jnp.sum(exponent, axis=0, keepdims=True)
        probs = (exponent * (1.0 / totals)).astype(BF)
        pieces.append(dot_nn(v_t[head * HEAD_DIM : (head + 1) * HEAD_DIM], probs))
        lse_ref[0, 0, head : head + 1, :] = highest + jnp.log(totals)
    ctx = jnp.concatenate(pieces, axis=0).T.astype(BF)
    ctx_ref[0] = ctx
    result = dot_nn(ctx, ow_ref[place.h ^ group])
    spot = pl.ds(pl.multiple_of(row * LEN, LEN), LEN)

    @pl.when(group == 0)
    def _():
        out_ref[spot, :] = result + ob_ref[...].reshape(1, result.shape[1])

    @pl.when(group > 0)
    def _():
        out_ref[spot, :] = out_ref[spot, :] + result

    @pl.when(step == 1)
    def _():
        direct(1).wait()
        beside(1).start()
        direct(2).wait()
        relay.start()
        beside(2).start()
        beside(1).wait()
        cross(1).start()

    @pl.when(step == 2)
    def _():
        relay.wait()
        beside(3).start()
        beside(2).wait()
        cross(2).start()

    @pl.when(step == 4)
    def _():
        beside(3).wait()
        cross(3).start()

    @pl.when(step == 7)
    def _():
        for g in range(4):
            store(g).wait()


def early_call(x, mask, embed, own, qb, vb, ow, ob):
    tokens, features = x.shape
    width = own.shape[1]
    groups = features // width
    rows = tokens // LEN
    hbm = pl.BlockSpec(memory_space=pl.ANY)
    per_head = pl.BlockSpec((1, LEN, width), lambda s: (s // 2, s % 2, 0))
    stacked = jax.ShapeDtypeStruct((groups, tokens, width), BF)
    dma = pltpu.SemaphoreType.DMA
    return pl.pallas_call(
        early_kernel,
        grid=(groups * rows,),
        in_specs=[
            pl.BlockSpec((LEN, features), lambda s: (s % 2, 0)),
            pl.BlockSpec((LEN, 1), lambda s: (s % 2, 0)),
            pl.BlockSpec((features,), lambda s: (0,)),
            hbm,
            pl.BlockSpec((width,), lambda s: (0,)),
            pl.BlockSpec((width,), lambda s: (0,)),
            pl.BlockSpec((groups, width, features), lambda s: (0, 0, 0)),
            pl.BlockSpec((features,), lambda s: (0,)),
        ],
        out_specs=[
            per_head,
            per_head,
            per_head,
            per_head,
            pl.BlockSpec((1, 1, 8, LEN), lambda s: (s // 2, s % 2, 0, 0)),
            pl.BlockSpec((tokens, features), lambda s: (0, 0)),
            pl.BlockSpec((LEN, features), lambda s: (jnp.minimum(s, 1), 0)),
            hbm,
        ],
        out_shape=[
            stacked,
            stacked,
            stacked,
            stacked,
            jax.ShapeDtypeStruct((groups, rows, 8, LEN), F32),
            jax.ShapeDtypeStruct((tokens, features), F32),
            jax.ShapeDtypeStruct((tokens, features), BF),
            jax.ShapeDtypeStruct((groups,) + own.shape, BF),
        ],
        scratch_shapes=[
            pltpu.VMEM((groups,) + own.shape, BF),
            pltpu.VMEM((groups, 8, width), F32),
            dma((4, 4)),
            dma((4, 4)),
            dma((6,)),
        ],
        compiler_params=pltpu.CompilerParams(
            dimension_semantics=("arbitrary",),
            vmem_limit_bytes=56 << 20,
            collective_id=0,
            has_side_effects=True,
        ),
        name="early_kernel",
    )(x, mask, embed, own, qb, vb, ow, ob)


LANES = 384
CHUNK = 1024
PIECE = CHUNK // 64
SPACING = 3
DOWN_EVERY = 1
UP_EVERY = 4
UP_FIRST = 6
BLOCK = 256


def add_into(target, source):
    target[...] = (target[...].astype(F32) + source[...].astype(F32)).astype(BF)


class MatrixSum:
    COPIES = 16

    def __init__(self, place, parts, keep, first, second, third, fourth, full, send, recv, local):
        self.place = place
        self.parts = parts
        self.keep, self.first, self.second = keep, first, second
        self.third, self.fourth, self.full = third, fourth, full
        self.send, self.recv, self.local = send, recv, local

    def copy(self, i, slot, src, dst, where):
        return remote(src, dst, self.send.at[i, slot], self.recv.at[i, slot], where)

    def fetch(self, i, source, index):
        return pltpu.make_async_copy(
            source.at[index, self.place.c], self.keep.at[i], self.local.at[i]
        )

    def copies(self, phase, i, source=None, index=None):
        p = self.place
        keep, full = self.keep, self.full
        both = self.parts == 2
        out = []
        if phase == 1:
            out.append(self.copy(i, 0, source.at[index, 1 - p.c], self.first.at[i], p.core()))
        if phase == 2:
            src = keep.at[i, 0, 1 - p.x]
            out.append(self.copy(i, 1, src, self.second.at[i, 0], p.side("x")))
            if both:
                src = keep.at[i, 1, :, 1 - p.y]
                out.append(self.copy(i, 2, src, self.second.at[i, 1], p.side("y")))
        if phase == 3:
            src = keep.at[i, 0, p.x, 1 - p.y]
            out.append(self.copy(i, 3, src, self.third.at[i, 0], p.side("y")))
            if both:
                src = keep.at[i, 1, 1 - p.x, p.y]
                out.append(self.copy(i, 4, src, self.third.at[i, 1], p.side("x")))
        if phase == 4:
            for o in range(1, 4):
                src = keep.at[i, :, p.x, p.y, p.h ^ o]
                out.append(self.copy(i, 4 + o, src, self.fourth.at[i, o - 1], p.up(o)))
        if phase == 5:
            spot = full.at[i, p.c, :, p.x, p.y, p.h]
            for o in range(1, 4):
                out.append(self.copy(i, 7 + o, spot, spot, p.up(o)))
        if phase == 6:
            spot = full.at[i, p.c, 0, p.x, p.y]
            out.append(self.copy(i, 11, spot, spot, p.side("y")))
            if both:
                spot = full.at[i, p.c, 1, p.x, p.y]
                out.append(self.copy(i, 12, spot, spot, p.side("x")))
        if phase == 7:
            spot = full.at[i, p.c, 0, p.x]
            out.append(self.copy(i, 13, spot, spot, p.side("x")))
            if both:
                spot = full.at[i, p.c, 1, :, p.y]
                out.append(self.copy(i, 14, spot, spot, p.side("y")))
        if phase == 8:
            spot = full.at[i, p.c]
            out.append(self.copy(i, 15, spot, spot, p.core()))
        return out

    def begin(self, i, source, index):
        self.fetch(i, source, index).start()
        for one in self.copies(1, i, source, index):
            one.start()

    def advance(self, phase, i, source=None, index=None):
        p = self.place
        if phase == 2:
            self.fetch(i, source, index).wait()
        for one in self.copies(phase - 1, i, source, index):
            one.wait()
        if phase == 2:
            add_into(self.keep.at[i], self.first.at[i])
        if phase == 3:
            add_into(self.keep.at[i, 0, p.x], self.second.at[i, 0])
            if self.parts == 2:
                add_into(self.keep.at[i, 1, :, p.y], self.second.at[i, 1])
        if phase == 4:
            for part in range(self.parts):
                add_into(self.keep.at[i, part, p.x, p.y], self.third.at[i, part])
        if phase == 5:
            total = self.keep[i, :, p.x, p.y, p.h].astype(F32)
            for o in range(3):
                total = total + self.fourth[i, o].astype(F32)
            self.full[i, p.c, :, p.x, p.y, p.h] = total.astype(BF)
        if phase <= 8:
            for one in self.copies(phase, i):
                one.start()


class GroupSum:
    COPIES = 11

    def __init__(self, place, own, first, second, third, fourth, full, send, recv):
        self.place = place
        self.own, self.first, self.second = own, first, second
        self.third, self.fourth, self.full = third, fourth, full
        self.send, self.recv = send, recv

    def copy(self, g, slot, src, dst, where):
        return remote(src, dst, self.send.at[g, slot], self.recv.at[g, slot], where)

    def copies(self, phase, g):
        p, own, full = self.place, self.own, self.full
        x, y = p.side("x"), p.side("y")
        if phase == 1:
            return [self.copy(g, 0, own.at[g, 1 - p.c], self.first.at[g], p.core())]
        if phase == 2:
            return [
                self.copy(g, 1, own.at[g, p.c, 0, 1 - p.x], self.second.at[g, 0], x),
                self.copy(g, 2, own.at[g, p.c, 1, :, 1 - p.y], self.second.at[g, 1], y),
            ]
        if phase == 3:
            return [
                self.copy(g, 3, own.at[g, p.c, 0, p.x, 1 - p.y], self.third.at[g, 0], y),
                self.copy(g, 4, own.at[g, p.c, 1, 1 - p.x, p.y], self.third.at[g, 1], x),
            ]
        if phase == 4 and g > 0:
            return [
                self.copy(g, 5, own.at[g, p.c, :, p.x, p.y], self.fourth.at[g - 1], p.up(g))
            ]
        if phase == 6:
            spots = full.at[p.c, 0, p.x, p.y], full.at[p.c, 1, p.x, p.y]
            return [self.copy(0, 6, spots[0], spots[0], y), self.copy(0, 7, spots[1], spots[1], x)]
        if phase == 7:
            spots = full.at[p.c, 0, p.x], full.at[p.c, 1, :, p.y]
            return [self.copy(0, 8, spots[0], spots[0], x), self.copy(0, 9, spots[1], spots[1], y)]
        if phase == 8:
            spot = full.at[p.c]
            return [self.copy(0, 10, spot, spot, p.core())]
        return []

    def begin(self, g):
        for one in self.copies(1, g):
            one.start()

    def advance(self, phase, g):
        p, own = self.place, self.own
        if phase == 6:
            for group in range(own.shape[0]):
                for one in self.copies(4, group):
                    one.wait()
            total = own[0, p.c, :, p.x, p.y].astype(F32)
            for o in range(3):
                total = total + self.fourth[o].astype(F32)
            self.full[p.c, :, p.x, p.y] = total.astype(BF)
        else:
            for one in self.copies(phase - 1, g):
                one.wait()
        if phase == 2:
            add_into(own.at[g, p.c], self.first.at[g])
        if phase == 3:
            add_into(own.at[g, p.c, 0, p.x], self.second.at[g, 0])
            add_into(own.at[g, p.c, 1, :, p.y], self.second.at[g, 1])
        if phase == 4:
            add_into(own.at[g, p.c, 0, p.x, p.y], self.third.at[g, 0])
            add_into(own.at[g, p.c, 1, p.x, p.y], self.third.at[g, 1])
        for one in self.copies(phase, g):
            one.start()


class Stages:
    def __init__(self, tokens, ff, count, heads):
        rows = tokens // LEN
        self.blocks = ff // BLOCK
        self.norms = self.blocks + tokens // BLOCK
        self.outer = self.norms + count
        self.per_group = 2 * rows
        self.end = self.outer + count * self.per_group
        self.half = ff // CHUNK
        self.outw_first = self.outer + 1


def late_kernel(
    plan,
    gf_ref,
    nl_hbm,
    slope_ref,
    dw_ref,
    uw_ref,
    xh_ref,
    inv_ref,
    gs_ref,
    gain_ref,
    x_hbm,
    w_ref,
    ow_ref,
    ctx_ref,
    q_ref,
    k_ref,
    v_ref,
    lse_ref,
    mask_ref,
    early_0,
    early_1,
    early_2,
    early_3,
    early_4,
    early_5,
    early_6,
    down_ref,
    vec_ref,
    dx_out,
    wg_out,
    down_out,
    up_out,
    outw_out,
    up_ref,
    outw_ref,
    dx,
    rows_ref,
    ga_all,
    dpre,
    stage_w,
    stage_o,
    wg_acc,
    dctx,
    k_t,
    dq_t,
    dk_acc,
    dv_acc,
    stage_up,
    vec,
    vec_in,
    ff_keep,
    ff_1,
    ff_2,
    ff_3,
    ff_4,
    ff_full,
    ow_keep,
    ow_1,
    ow_2,
    ow_3,
    ow_4,
    ow_full,
    qk_own,
    qk_1,
    qk_2,
    qk_3,
    qk_4,
    qk_full,
    ff_send,
    ff_recv,
    ff_local,
    ow_send,
    ow_recv,
    ow_local,
    qk_send,
    qk_recv,
    vec_send,
    vec_recv,
    store_sem,
    block_sem,
    outer_sem,
    last_sem,
    rows_sem,
):
    step = pl.program_id(0)
    place = Place()
    half = plan.half
    chunks = 2 * half
    count = qk_own.shape[0]
    width = q_ref.shape[2]
    heads = width // HEAD_DIM
    feed = MatrixSum(
        place, 2, ff_keep, ff_1, ff_2, ff_3, ff_4, ff_full, ff_send, ff_recv, ff_local
    )
    outer = MatrixSum(
        place, 1, ow_keep, ow_1, ow_2, ow_3, ow_4, ow_full, ow_send, ow_recv, ow_local
    )
    groups = GroupSum(place, qk_own, qk_1, qk_2, qk_3, qk_4, qk_full, qk_send, qk_recv)
    tail = plan.end
    end = max(
        tail + 8,
        plan.outw_first + 8 * SPACING + 1,
        UP_FIRST + UP_EVERY * (half - 1) + 8 * SPACING + 1,
    )

    nl_load = pltpu.make_async_copy(nl_hbm, rows_ref, rows_sem.at[0])
    x_load = pltpu.make_async_copy(x_hbm, rows_ref, rows_sem.at[1])

    @pl.when(step == 0)
    def _():
        nl_load.start()
        greet(
            [place.core(), place.side("x"), place.side("y")] + [place.up(o) for o in range(1, 4)]
        )
        nl_load.wait()
        vec[...] = jnp.zeros_like(vec)
        rows = (early_0, 0), (early_1, 1), (early_2, 2)
        rows += (early_3, 10), (early_4, 11), (early_5, 12), (early_6, 13)
        for ref, index in rows:
            vec[0, index : index + 1, :] = ref[...].reshape(1, vec.shape[2])

    def down_store(i):
        return pltpu.make_async_copy(ff_full.at[i], down_out.at[i], store_sem.at[i, 0])

    def up_store(i, part):
        spot = pl.ds(pl.multiple_of((2 * i + part) * (CHUNK // 2), CHUNK // 2), CHUNK // 2)
        return pltpu.make_async_copy(stage_up, up_out.at[:, spot], store_sem.at[half + i, part])

    def outw_store():
        return pltpu.make_async_copy(ow_full.at[0], outw_out.at[0], store_sem.at[chunks, 0])

    def tick(t, start, stop):
        span = 8 * SPACING

        def window(first, last, run):
            if start <= last and stop > first:

                @pl.when((t >= first) & (t <= last))
                def _():
                    run()

        def each(first, every, number, run):
            for phase in range(9, 0, -1):
                behind = SPACING * (phase - 1)
                if stop - behind <= first or start - behind > first + every * (number - 1):
                    continue
                at = t - behind - first
                index = at // every

                @pl.when((at >= 0) & (index < number) & (at % every == 0))
                def _():
                    run(phase, index)

        def down_step(phase, i):
            if phase == 1:
                feed.begin(i, down_ref, i)
                return
            feed.advance(phase, i, down_ref, i)
            if phase == 9:
                down_store(i).start()

        def up_step(phase, i):
            if phase == 1:
                feed.begin(half + i, up_ref, i)
                return
            feed.advance(phase, half + i, up_ref, i)
            if phase == 9:

                @pl.when(i > 0)
                def _():
                    up_store(i - 1, 1).wait()

                for c in range(2):
                    if c == 1:
                        up_store(i, 0).wait()
                    block = ff_full[half + i, c].reshape(CHUNK // 2, 2 * LANES)
                    stage_up[...] = block.T
                    up_store(i, c).start()

        def outw_step(phase, i):
            if phase == 1:
                outer.begin(0, outw_ref, 0)
                return
            outer.advance(phase, 0, outw_ref, 0)
            if phase == 9:
                outw_store().start()

        def group_steps():
            for place_of in range(count):
                g = (place_of + 1) % count
                base = plan.outer + plan.per_group * (place_of + 1)
                steps = ((4, 5), (3, 3), (2, 1), (1, 0))
                if place_of == count - 1:
                    steps = ((9, 7), (8, 6), (7, 5), (6, 4), (4, 3), (3, 2), (2, 1), (1, 0))
                for phase, later in steps:
                    if not start <= base + later < stop:
                        continue

                    @pl.when(t == base + later)
                    def _():
                        if phase == 1:
                            groups.begin(g)
                        else:
                            groups.advance(phase, g)

        first, last = 0, DOWN_EVERY * (half - 1) + span
        window(first, last, lambda: each(0, DOWN_EVERY, half, down_step))
        first, last = UP_FIRST, UP_FIRST + UP_EVERY * (half - 1) + span
        window(first, last, lambda: each(UP_FIRST, UP_EVERY, half, up_step))
        first, last = plan.outw_first, plan.outw_first + span
        window(first, last, lambda: each(plan.outw_first, 1, 1, outw_step))
        window(plan.outer + plan.per_group, tail + 8, group_steps)

    tick(step, 0, tail)


    def block_copy(b):
        per_chunk = CHUNK // BLOCK
        spot = up_ref.at[b // per_chunk, (b % per_chunk) // 2, b % 2]
        return pltpu.make_async_copy(stage_w.at[b % 2], spot, block_sem.at[b])

    @pl.when(step < plan.blocks)
    def _():
        grad = dot_nt(gf_ref[...], dw_ref[...]) * slope_ref[...]
        dpre[...] = grad.astype(BF)

        @pl.when(step > 1)
        def _():
            block_copy(step - 2).wait()

        part = dot_tn(dpre[...], rows_ref[...]).astype(BF)
        stage_w[step % 2] = part.reshape(stage_w.shape[1:])
        block_copy(step).start()
        per_row = rows_ref.shape[1] // BLOCK
        spot = pl.ds(pl.multiple_of((step % per_row) * BLOCK, BLOCK), BLOCK)
        vec[0, pl.ds(6 + step // per_row, 1), spot] = jnp.sum(
            dpre[...].astype(F32), axis=0, keepdims=True
        )
        for r in range(0, dx.shape[0], BLOCK):
            part = dot_nt(dpre[r : r + BLOCK], uw_ref[...])

            @pl.when(step == 0)
            def _():
                dx[r : r + BLOCK] = part

            @pl.when(step > 0)
            def _():
                dx[r : r + BLOCK] = dx[r : r + BLOCK] + part


    @pl.when((step >= plan.blocks) & (step < plan.norms))
    def _():
        @pl.when(step == plan.blocks)
        def _():
            block_copy(plan.blocks - 2).wait()
            block_copy(plan.blocks - 1).wait()
            x_load.start()

        rows = pl.ds(pl.multiple_of((step - plan.blocks) * BLOCK, BLOCK), BLOCK)
        upstream = dx[rows, :] + gs_ref[...]
        normal = xh_ref[...]
        scaled = upstream * gain_ref[...].reshape(1, upstream.shape[1])
        mean = jnp.mean(scaled, axis=1, keepdims=True)
        along = jnp.mean(scaled * normal, axis=1, keepdims=True)
        hidden = inv_ref[...] * (scaled - mean - normal * along)
        low = hidden.astype(BF)
        dx[rows, :] = hidden
        ga_all[rows, :] = low
        vec[0, 3:4, :] += jnp.sum(upstream * normal, axis=0, keepdims=True)
        vec[0, 4:5, :] += jnp.sum(upstream, axis=0, keepdims=True)
        vec[0, 5:6, :] += jnp.sum(low.astype(F32), axis=0, keepdims=True)


    def outer_copy(g):
        spot = place.h ^ g
        return pltpu.make_async_copy(
            stage_o, outw_ref.at[0, spot >> 1, 0, spot & 1], outer_sem.at[g]
        )

    @pl.when((step >= plan.norms) & (step < plan.outer))
    def _():
        g = step - plan.norms

        @pl.when(g > 0)
        def _():
            outer_copy(g - 1).wait()

        part = dot_tn(ctx_ref[0], ga_all[...])
        stage_o[...] = part.astype(BF).reshape(stage_o.shape)
        outer_copy(g).start()

    @pl.when(step == plan.outer)
    def _():
        outer_copy(count - 1).wait()
        x_load.wait()


    def dx_copy(r):
        spot = pl.ds(pl.multiple_of(r * LEN, LEN), LEN)
        return pltpu.make_async_copy(dx.at[spot], dx_out.at[spot], last_sem.at[r])

    @pl.when(step >= plan.outer)
    def _():
        at = step - plan.outer
        part = at % 2
        row = (at // 2) % 2
        turn = at // plan.per_group
        group = (turn + 1) % count
        mine = pl.ds(pl.multiple_of(row * LEN, LEN), LEN)
        q = q_ref[0]
        k = k_ref[0]
        v = v_ref[0]

        @pl.when(part == 0)
        def _():
            dctx[...] = dot_nt(ga_all[mine, :], ow_ref[place.h ^ group]).astype(BF)
            k_t[...] = k.T

        q_scaled = q * jnp.asarray(0.125, BF)

        def one_head(head, carry):
            mask = head_lanes(width, head)
            spot = pl.ds(pl.multiple_of(head * HEAD_DIM, HEAD_DIM), HEAD_DIM)
            scores = dot_nt(jnp.where(mask, k, jnp.zeros_like(k)), q_scaled)
            probs = jnp.exp(scores - lse_ref[0, 0, pl.ds(head, 1), :])
            dprobs = dot_nt(jnp.where(mask, v, jnp.zeros_like(v)), dctx[...])
            delta = jnp.sum(probs * dprobs, axis=0, keepdims=True)
            dscores = (probs * (dprobs - delta)).astype(BF)
            dv_acc[...] = jnp.where(mask, dot_nn(probs.astype(BF), dctx[...]), dv_acc[...])
            dk_acc[...] = jnp.where(mask, dot_nn(dscores, q_scaled), dk_acc[...])
            dq_t[spot, :] = dot_nn(k_t[spot, :], dscores)
            return carry

        split = heads // 2 + 1
        lax.fori_loop(part * split, split + part * (heads - split), one_head, 0)

        @pl.when(part == 1)
        def _():
            x = rows_ref[mine, :]
            dq = (dq_t[...] * 0.125).T.astype(BF)
            dk = dk_acc[...].astype(BF)
            dv = dv_acc[...].astype(BF)
            delta = dot_nn(dq, w_ref[0, 0]) + dot_nn(dk, w_ref[0, 1]) + dot_nn(dv, w_ref[0, 2])
            dx[mine, :] = dx[mine, :] + delta

            @pl.when(row == 0)
            def _():
                wg_acc[...] = jnp.zeros_like(wg_acc)

            for index, grad in enumerate((dq, dk, dv)):
                wg_acc[index * width : (index + 1) * width] += dot_tn(grad, x)
            spot = place.h ^ group
            vec[0, pl.ds(16 + spot, 1), 0:width] += jnp.sum(
                dq.astype(F32), axis=0, keepdims=True
            )
            vec[0, pl.ds(20 + spot, 1), 0:width] += jnp.sum(
                dv.astype(F32), axis=0, keepdims=True
            )

            @pl.when(row == 1)
            def _():
                shape = qk_own.shape[2:]
                for zl in range(2):
                    block = wg_acc[:, zl * LANES : (zl + 1) * LANES].astype(BF)
                    qk_own[group, zl] = block.reshape(shape)

            @pl.when(turn == count - 1)
            def _():
                total = jnp.where(mask_ref[...] == 1.0, dx[mine, :], 0.0)
                vec[0, 15:16, :] += jnp.sum(total, axis=0, keepdims=True)
                dx_copy(row).start()

    @pl.when(step == plan.end - 1)
    def _():
        def vec_copy(k):
            if k < 3:
                where = (place.dp ^ (1 << k), place.h)
            else:
                where = (place.dp, place.h ^ (1 << (k - 3)))
            return remote(vec.at[k], vec_in.at[k], vec_send.at[k], vec_recv.at[k], where)

        @pl.loop(tail, end)
        def _(t):
            tick(t, tail, end)
            for k in range(6):

                @pl.when(t == tail + k)
                def _():
                    if k > 0:
                        vec_copy(k - 1).wait()
                        vec[k] = vec[k - 1] + vec_in[k - 1]
                    if k < 5:
                        vec_copy(k).start()

        vec_ref[...] = vec[5]
        for c in range(2):
            block = qk_full[c].reshape(wg_acc.shape[0], LANES)
            wg_acc[:, c * LANES : (c + 1) * LANES] = block.astype(F32)
        wg_copy = pltpu.make_async_copy(wg_acc, wg_out, last_sem.at[2])
        wg_copy.start()
        for i in range(half):
            down_store(i).wait()
        up_store(half - 1, 1).wait()
        outw_store().wait()
        for r in range(2):
            dx_copy(r).wait()
        wg_copy.wait()


def late_call(
    gf, nl, slope, dw, uw, xh, inv, gs, gain, x, w, ow, ctx, q, k, v, lse, mask, early, down
):
    tokens, features = x.shape
    count, _, width, _ = w.shape
    ff = down.shape[0]
    heads = width // HEAD_DIM
    plan = Stages(tokens, ff, count, heads)
    chunks = 2 * plan.half
    chunked = (plan.half, 2, 2, 2, 2, 4, PIECE, features)
    squared = (1, 2, 1, 2, 2, 4, features // 32, features)
    hbm = pl.BlockSpec(memory_space=pl.ANY)
    once = pl.Buffered(1)

    def whole(shape):
        return pl.BlockSpec(shape, lambda s: (0,) * len(shape), pipeline_mode=once)

    def block_at(s):
        return jnp.minimum(s, plan.blocks - 1)

    def norm_at(s):
        return jnp.clip(s - plan.blocks, 0, tokens // BLOCK - 1)

    def head_at(s):
        at = jnp.clip(s - plan.outer, 0, plan.end - plan.outer - 1)
        return (at // plan.per_group + 1) % count, (at // 2) % 2

    def per_head(s):
        group, row = head_at(s)
        return group, row, 0

    in_specs = [
        whole(gf.shape),
        hbm,
        pl.BlockSpec((tokens, BLOCK), lambda s: (0, block_at(s))),
        pl.BlockSpec((BLOCK, features), lambda s: (block_at(s), 0)),
        pl.BlockSpec((features, BLOCK), lambda s: (0, block_at(s))),
        pl.BlockSpec((BLOCK, features), lambda s: (norm_at(s), 0)),
        pl.BlockSpec((BLOCK, 1), lambda s: (norm_at(s), 0), pipeline_mode=once),
        pl.BlockSpec((BLOCK, features), lambda s: (norm_at(s), 0)),
        whole(gain.shape),
        hbm,
        pl.BlockSpec((1, 3, width, features), lambda s: (head_at(s)[0], 0, 0, 0)),
        whole(ow.shape),
        pl.BlockSpec(
            (1, tokens, width),
            lambda s: (jnp.clip(s - plan.norms, 0, count - 1), 0, 0),
            pipeline_mode=once,
        ),
        pl.BlockSpec((1, LEN, width), per_head),
        pl.BlockSpec((1, LEN, width), per_head),
        pl.BlockSpec((1, LEN, width), per_head),
        pl.BlockSpec((1, 1, 8, LEN), lambda s: head_at(s) + (0, 0)),
        pl.BlockSpec((LEN, 1), lambda s: (head_at(s)[1], 0)),
    ]
    in_specs += [whole(one.shape) for one in early]
    in_specs += [hbm]
    out_specs = [pl.BlockSpec((24, features), lambda s: (0, 0))] + [hbm] * 7
    out_shape = [
        jax.ShapeDtypeStruct((24, features), F32),
        jax.ShapeDtypeStruct((tokens, features), F32),
        jax.ShapeDtypeStruct((3 * width, features), F32),
        jax.ShapeDtypeStruct(chunked, BF),
        jax.ShapeDtypeStruct((features, ff), BF),
        jax.ShapeDtypeStruct(squared, BF),
        jax.ShapeDtypeStruct(chunked, BF),
        jax.ShapeDtypeStruct(squared, BF),
    ]

    def sum_buffers(n, parts, rows):
        block = (rows, features)
        return [
            pltpu.VMEM((n, parts, 2, 2, 4) + block, BF),
            pltpu.VMEM((n, parts, 2, 2, 4) + block, BF),
            pltpu.VMEM((n, parts, 2, 4) + block, BF),
            pltpu.VMEM((n, parts, 4) + block, BF),
            pltpu.VMEM((n, 3, parts) + block, BF),
            pltpu.VMEM((n, 2, parts, 2, 2, 4) + block, BF),
        ]

    qrows = 3 * width // 8
    quarter = (2, 2, 2, qrows, LANES)
    scratch = [
        pltpu.VMEM((tokens, features), F32),
        pltpu.VMEM((tokens, features), BF),
        pltpu.VMEM((tokens, features), BF),
        pltpu.VMEM((tokens, BLOCK), BF),
        pltpu.VMEM((2, 2, 2, 4, PIECE, features), BF),
        pltpu.VMEM((2, 4, width // 8, features), BF),
        pltpu.VMEM((3 * width, features), F32),
        pltpu.VMEM((LEN, width), BF),
        pltpu.VMEM((width, LEN), BF),
        pltpu.VMEM((width, LEN), F32),
        pltpu.VMEM((LEN, width), F32),
        pltpu.VMEM((LEN, width), F32),
        pltpu.VMEM((features, CHUNK // 2), BF),
        pltpu.VMEM((6, 24, features), F32),
        pltpu.VMEM((5, 24, features), F32),
    ]
    scratch += sum_buffers(chunks, 2, PIECE)
    scratch += sum_buffers(1, 1, features // 32)
    scratch += [
        pltpu.VMEM((count, 2) + quarter, BF),
        pltpu.VMEM((count,) + quarter, BF),
        pltpu.VMEM((count, 2, 2, qrows, LANES), BF),
        pltpu.VMEM((count, 2, qrows, LANES), BF),
        pltpu.VMEM((3, 2, qrows, LANES), BF),
        pltpu.VMEM((2,) + quarter, BF),
    ]
    dma = pltpu.SemaphoreType.DMA
    scratch += [
        dma((chunks, MatrixSum.COPIES)),
        dma((chunks, MatrixSum.COPIES)),
        dma((chunks,)),
        dma((1, MatrixSum.COPIES)),
        dma((1, MatrixSum.COPIES)),
        dma((1,)),
        dma((count, GroupSum.COPIES)),
        dma((count, GroupSum.COPIES)),
        dma((5,)),
        dma((5,)),
        dma((chunks + 1, 2)),
        dma((plan.blocks,)),
        dma((count,)),
        dma((3,)),
        dma((2,)),
    ]
    results = pl.pallas_call(
        functools.partial(late_kernel, plan),
        grid=(plan.end,),
        in_specs=in_specs,
        out_specs=out_specs,
        out_shape=out_shape,
        scratch_shapes=scratch,
        compiler_params=pltpu.CompilerParams(
            dimension_semantics=("arbitrary",),
            vmem_limit_bytes=67043328,
            collective_id=1,
            has_side_effects=True,
        ),
        name="late_kernel",
    )(
        gf,
        nl,
        slope,
        dw,
        uw,
        xh,
        inv,
        gs,
        gain,
        x,
        w,
        ow,
        ctx,
        q,
        k,
        v,
        lse,
        mask,
        *early,
        down.reshape(chunked),
    )
    sums, dx, wg, down_sum, up_sum, outw_sum = results[:6]
    return (
        dx,
        wg,
        sums,
        down_sum.reshape(ff, features),
        up_sum,
        outw_sum.reshape(features, features),
    )


def final_kernel(down_ref, up_ref, outw_ref, dx_ref, mask_ref, down_out, up_out, outw_out, dx_out):
    down_out[...] = down_ref[...].astype(F32)
    up_out[...] = up_ref[...].astype(F32)
    outw_out[...] = outw_ref[...].astype(F32)
    dx_out[...] = jnp.where(mask_ref[...] == 1.0, 0.0, dx_ref[...])


def final_call(down, up, outw, dx, mask):
    steps = 8
    arrays = (down, up, outw, dx)

    def spec(shape):
        return pl.BlockSpec((shape[0] // steps, shape[1]), lambda s: (s, 0))

    return pl.pallas_call(
        final_kernel,
        grid=(steps,),
        in_specs=[spec(one.shape) for one in arrays + (mask,)],
        out_specs=[spec(one.shape) for one in arrays],
        out_shape=[jax.ShapeDtypeStruct(one.shape, F32) for one in arrays],
        compiler_params=pltpu.CompilerParams(
            dimension_semantics=("arbitrary",), vmem_limit_bytes=63 << 20
        ),
        name="final_kernel",
    )(down, up, outw, dx, mask)


def swap(value, axis, mask, size):
    return lax.ppermute(value, axis, [(i, i ^ mask) for i in range(size)])


def bit_of(axis, bit):
    return (lax.axis_index(axis) >> bit) & 1


def joined(mine, other, upper, dim, kind=None):
    low = jnp.where(upper == 1, other, mine)
    high = jnp.where(upper == 1, mine, other)
    if kind is not None:
        low, high = low.astype(kind), high.astype(kind)
    return jnp.concatenate([low, high], axis=dim)


def halve(value, bit, size, dim):
    half = value.shape[dim] // 2
    mine = bit_of("dp", bit)
    sent = lax.dynamic_slice_in_dim(value, (1 - mine) * half, half, dim)
    kept = lax.dynamic_slice_in_dim(value, mine * half, half, dim)
    received = swap(sent, "dp", 1 << bit, size)
    return (kept.astype(F32) + received.astype(F32)).astype(BF)


def double(value, bit, size, dim, kind=None):
    return joined(value, swap(value, "dp", 1 << bit, size), bit_of("dp", bit), dim, kind)


def plane_orders(size):
    bits = size.bit_length() - 1
    rest = list(range(1, bits))
    return rest, rest[::-1]


def reduce_plane(value, size, dim):
    value = halve(value, 0, size, dim)
    half = value.shape[dim] // 2
    parts = []
    for index, order in enumerate(plane_orders(size)):
        part = lax.slice_in_dim(value, index * half, (index + 1) * half, axis=dim)
        for bit in order:
            part = halve(part, bit, size, dim)
        parts.append(part)
    return parts


def gather_plane(parts, size, dim, kind=None):
    done = []
    for part, order in zip(parts, plane_orders(size)):
        for bit in order[::-1]:
            part = double(part, bit, size, dim)
        done.append(part)
    return double(jnp.concatenate(done, axis=dim), 0, size, dim, kind)


def reduce_head(pieces, size):
    total = pieces[0].astype(F32)
    for offset in range(1, size):
        total = total + swap(pieces[offset], "head", offset, size).astype(F32)
    return total


def gather_head(piece, size):
    return [piece] + [swap(piece, "head", offset, size) for offset in range(1, size)]


def absolute(pieces, dim):
    count = len(pieces)
    bit = 0
    while (1 << bit) < count:
        upper = bit_of("head", bit)
        step = 1 << bit
        pieces = [
            jnp.where(upper == 1, pieces[index ^ step], pieces[index]) for index in range(count)
        ]
        bit += 1
    return jnp.concatenate(pieces, axis=dim)


def own_pieces(value, size, dim):
    width = value.shape[dim] // size
    me = lax.axis_index("head")
    return [
        lax.dynamic_slice_in_dim(value, (me ^ offset) * width, width, dim)
        for offset in range(size)
    ]


def all_reduce_matrix(value, dp, head, head_dim):
    parts = []
    for part in reduce_plane(value, dp, 0):
        piece = reduce_head(own_pieces(part, head, head_dim), head).astype(BF)
        parts.append(absolute(gather_head(piece, head), head_dim))
    return gather_plane(parts, dp, 0, F32)


def all_reduce_small(vector, dp, head):
    bit = 1
    while bit < dp:
        vector = vector + swap(vector, "dp", bit, dp)
        bit *= 2
    bit = 1
    while bit < head:
        vector = vector + swap(vector, "head", bit, head)
        bit *= 2
    return vector


def norm_forward(hidden, gain, bias):
    center = hidden - jnp.mean(hidden, axis=-1, keepdims=True)
    inverse = lax.rsqrt(jnp.mean(center * center, axis=-1, keepdims=True) + EPS)
    normal = center * inverse
    return (normal * gain + bias, normal, inverse)


def norm_backward(upstream, normal, inverse, gain):
    gain_grad = jnp.sum(upstream * normal, axis=0)
    bias_grad = jnp.sum(upstream, axis=0)
    scaled = upstream * gain
    hidden_grad = inverse * (
        scaled
        - jnp.mean(scaled, axis=-1, keepdims=True)
        - normal * jnp.mean(scaled * normal, axis=-1, keepdims=True)
    )
    return (hidden_grad, gain_grad, bias_grad)


def phi(values):
    return 0.5 * (1.0 + jax.scipy.special.erf(values * (1.0 / math.sqrt(2.0))))


def body(
    dp,
    head,
    tokens,
    span_mask,
    valid_mask,
    mask_embedding,
    qkv_weight,
    query_bias,
    value_bias,
    out_weight,
    out_bias,
    norm1_gain,
    norm1_bias,
    up_weight,
    up_bias,
    down_weight,
    down_bias,
    norm2_gain,
    norm2_bias,
    out_grad,
):
    features = tokens.shape[1]
    width = qkv_weight.shape[2]
    masked = (span_mask == 1)[:, None]
    validity = valid_mask.astype(F32)[:, None]
    direct = dp == 8 and head == 4 and features == 2 * LANES and tokens.shape[0] == 2 * LEN
    if direct:
        mask_column = (span_mask == 1).astype(F32)[:, None]
        out_parts = out_weight.reshape(head, width, features)
        q, k, v, ctx, lse, attended, inputs, weights = early_call(
            tokens,
            mask_column,
            mask_embedding,
            jnp.transpose(qkv_weight, (1, 2, 0)),
            query_bias,
            value_bias,
            out_parts,
            out_bias,
        )
    else:
        inputs = jnp.where(masked, mask_embedding[None, :], tokens)
        own = jnp.transpose(qkv_weight, (1, 0, 2))
        core = bit_of("dp", 0)
        half = lax.dynamic_slice_in_dim(own, core * (features // 2), features // 2, 1)
        halves = [half]
        for bit in range(head.bit_length() - 1):
            halves = halves + [swap(part, "head", 1 << bit, head) for part in halves]
        weights = [own] + [double(part, 0, dp, 1) for part in halves[1:]]
        biases = jnp.stack([query_bias, value_bias]).astype(F32)
        bias_parts = [biases]
        for bit in range(head.bit_length() - 1):
            bias_parts = bias_parts + [swap(part, "head", 1 << bit, head) for part in bias_parts]
        out_parts = own_pieces(out_weight, head, 0)

        attended = jnp.broadcast_to(out_bias[None, :], tokens.shape)
        saved = []
        for group in range(head):
            q, k, v, ctx, lse, attended = attention_forward(
                inputs,
                weights[group],
                bias_parts[group][0:1],
                bias_parts[group][1:2],
                out_parts[group],
                attended,
            )
            saved.append((q, k, v, ctx, lse))

    inputs_wide = inputs.astype(F32)
    normed, normal_first, inverse_first = norm_forward(
        inputs_wide + attended, norm1_gain, norm1_bias
    )
    normed_low = normed.astype(BF)
    preact = dot_nn(normed_low, up_weight) + up_bias
    share = phi(preact)
    activated = (preact * share).astype(BF)
    slope = share + preact * jnp.exp(-0.5 * preact * preact) * (1.0 / math.sqrt(2.0 * math.pi))
    feedout = dot_nn(activated, down_weight) + down_bias
    result, normal_second, inverse_second = norm_forward(normed + feedout, norm2_gain, norm2_bias)
    grad_output = out_grad.astype(F32) * validity
    grad_second, gain_second_grad, bias_second_grad = norm_backward(
        grad_output, normal_second, inverse_second, norm2_gain
    )
    grad_feed = grad_second.astype(BF)
    down_bias_grad = jnp.sum(grad_feed, axis=0, dtype=F32)
    down_local = dot_tn(activated, grad_feed).astype(BF)
    squares = jnp.stack(
        [
            jnp.sum(validity * inputs_wide * inputs_wide),
            jnp.sum(validity * attended * attended),
            jnp.sum(validity * feedout * feedout),
            jnp.sum(validity),
        ]
    )
    if direct:
        vectors = [down_bias_grad, gain_second_grad, bias_second_grad]
        vectors += [
            jnp.sum(validity * inputs_wide * inputs_wide, axis=0),
            jnp.sum(validity * attended * attended, axis=0),
            jnp.sum(validity * feedout * feedout, axis=0),
            jnp.broadcast_to(jnp.sum(validity), (features,)),
        ]
        dx, weight_sum, sums, down_sum, up_sum, outw_sum = late_call(
            grad_feed,
            normed_low,
            slope,
            down_weight,
            up_weight,
            normal_first,
            inverse_first,
            grad_second,
            norm1_gain,
            inputs,
            weights,
            out_parts,
            ctx,
            q,
            k,
            v,
            lse,
            mask_column,
            vectors,
            down_local,
        )
        down_weight_grad, up_weight_grad, out_weight_grad, tokens_grad = final_call(
            down_sum, up_sum, outw_sum, dx, mask_column
        )
        weight_grad = jnp.transpose(weight_sum.reshape(3, width, features), (2, 0, 1))
        me = lax.axis_index("head")
        first_grad = lax.dynamic_slice(sums, (16 + me, 0), (1, width))[0]
        third_grad = lax.dynamic_slice(sums, (20 + me, 0), (1, width))[0]
        count = jnp.maximum(sums[13, 0], 1.0)
        stream_rms = jnp.sqrt(jnp.sum(sums[10:13], axis=1) / (count * features))
        return (
            result.astype(BF),
            tokens_grad,
            sums[15],
            weight_grad,
            first_grad,
            third_grad,
            out_weight_grad,
            sums[5],
            sums[3],
            sums[4],
            up_weight_grad,
            sums[6:10].reshape(-1),
            down_weight_grad,
            sums[0],
            sums[1],
            sums[2],
            stream_rms,
        )

    grad_preact = (dot_nt(grad_feed, down_weight) * slope).astype(BF)
    up_bias_grad = jnp.sum(grad_preact, axis=0, dtype=F32)
    up_local = dot_tn(normed_low, grad_preact).astype(BF)
    grad_normed = dot_nt(grad_preact, up_weight) + grad_second
    grad_first, gain_first_grad, bias_first_grad = norm_backward(
        grad_normed, normal_first, inverse_first, norm1_gain
    )
    grad_attended = grad_first.astype(BF)
    out_bias_grad = jnp.sum(grad_attended, axis=0, dtype=F32)
    early = [
        down_bias_grad,
        gain_second_grad,
        bias_second_grad,
        gain_first_grad,
        bias_first_grad,
        out_bias_grad,
        up_bias_grad,
        squares,
    ]
    down_weight_grad = all_reduce_matrix(down_local, dp, head, 0)
    up_weight_grad = all_reduce_matrix(up_local, dp, head, 1)
    early_sum = all_reduce_small(jnp.concatenate(early), dp, head)

    grad_inputs = grad_first
    weight_pieces = []
    out_pieces = []
    query_parts = []
    value_parts = []
    for group in range(head):
        q, k, v, ctx, lse = saved[group]
        weight_piece, out_piece, query_part, value_part, grad_inputs = attention_backward(
            inputs,
            weights[group],
            out_parts[group],
            q,
            k,
            v,
            ctx,
            lse,
            grad_attended,
            grad_inputs,
        )
        weight_pieces.append(reduce_plane(weight_piece, dp, 1))
        out_pieces.append(out_piece)
        query_parts.append(query_part[0])
        value_parts.append(value_part[0])

    weight_grad = gather_plane(
        [
            reduce_head([weight_pieces[group][part] for group in range(head)], head).astype(BF)
            for part in range(2)
        ],
        dp,
        1,
        F32,
    )
    weight_grad = jnp.transpose(weight_grad, (1, 0, 2))

    out_reduced = jnp.stack(out_pieces)
    for bit in range(dp.bit_length() - 1):
        out_reduced = halve(out_reduced, bit, dp, 1)
    out_piece = reduce_head([out_reduced[group] for group in range(head)], head).astype(BF)
    for bit in range(dp.bit_length() - 2, -1, -1):
        out_piece = double(out_piece, bit, dp, 0)
    out_weight_grad = absolute(gather_head(out_piece, head), 0).astype(F32)

    tokens_grad = jnp.where(masked, 0.0, grad_inputs)
    embedding_grad = jnp.sum(jnp.where(masked, grad_inputs, 0.0), axis=0)
    late = jnp.concatenate([embedding_grad, absolute(query_parts, 0), absolute(value_parts, 0)])
    late_sum = all_reduce_small(late, dp, head)
    embedding_grad = late_sum[:features]
    me = lax.axis_index("head")
    first_grad = lax.dynamic_slice_in_dim(late_sum, features + me * width, width)
    third_grad = lax.dynamic_slice_in_dim(late_sum, 2 * features + me * width, width)

    pieces = []
    offset = 0
    for part in early:
        pieces.append(lax.slice_in_dim(early_sum, offset, offset + part.shape[0]))
        offset += part.shape[0]
    (
        down_bias_grad,
        gain_second_grad,
        bias_second_grad,
        gain_first_grad,
        bias_first_grad,
        out_bias_grad,
        up_bias_grad,
        squares,
    ) = pieces
    count = jnp.maximum(squares[3], 1.0)
    stream_rms = jnp.sqrt(squares[:3] / (count * features))
    return (
        result.astype(BF),
        tokens_grad,
        embedding_grad,
        weight_grad,
        first_grad,
        third_grad,
        out_weight_grad,
        out_bias_grad,
        gain_first_grad,
        bias_first_grad,
        up_weight_grad,
        up_bias_grad,
        down_weight_grad,
        down_bias_grad,
        gain_second_grad,
        bias_second_grad,
        stream_rms,
    )


def solution(mesh):
    split = P(("dp", "head"), None)
    flat = P(("dp", "head"))
    placed = (split, flat, flat, P(), P(None, None, "head"), P("head"), P("head")) + (P(),) * 10
    placed = placed + (split,)
    outs = (split, split, P(), P(None, None, "head"), P("head"), P("head")) + (P(),) * 11
    return jax.shard_map(
        functools.partial(body, mesh.shape["dp"], mesh.shape["head"]),
        mesh=mesh,
        in_specs=placed,
        out_specs=outs,
        check_vma=False,
    )
```
